256 devices in a mesh: blk: 32 (over x, z_hi, core), grp: 8 (over y, z_lo).
Axes of the slice: x: 4, y: 4, z: 8 (z_hi: 4, z_lo: 2; z = z_hi * 2 + z_lo), core: 2. Of those that a mesh axis runs over, the one named last changes fastest.
Arguments:
- residents: bfloat16 [512, 32, 1024], P(('blk', 'grp')), may hold values from -6 to 6
- travellers: bfloat16 [64, 32, 1024], P('blk'), may hold values from -6 to 6
- pair_list: int32 [256, 4, 2, 3], P(('blk', 'grp')), may hold values from 0 to 1, as said below
Outputs:
- resident_exchange: float32 [512, 32, 1024], P(('blk', 'grp'))
- traveller_exchange: float32 [64, 32, 1024], P('blk', 'grp')
The draws below stay inside these ranges and needn't reach their ends.
Inputs may be any that keep to these rules, and one draw needn't show every extreme that they name: `pair_list`: entry 0 is a resident index below 2, entry 1 a traveller index below 2, entry 2 is 0 or 1; the number of active slots differs from device to device.
All inputs are finite; a program needn't handle non-finite values.
Results may differ from the reference program's by a relative error of at most 0.0003.
Values may be sent and summed in bfloat16 or wider, within the bound.
A program may use at most 64 MiB of HBM per device.

```python
import jax
import jax.numpy as jnp
from jax import lax

BOX = 32
R_DEV = 2
TRAV = 2
STEPS = 4
PAIRS = 2
RESIDENTS = 512
TRAVELLERS = 64
N_BLK = 32
N_GRP = 8


def draw_pair_list(key, part):
    keys = jax.random.split(jax.random.fold_in(key, 17), 4)
    shape = (N_BLK * N_GRP, STEPS, PAIRS)
    res_index = jax.random.randint(keys[0], shape, 0, R_DEV)
    trav_index = jax.random.randint(keys[1], shape, 0, TRAV)
    device_load = jax.random.randint(keys[2], (N_BLK * N_GRP, 1, 1), 1, PAIRS + 1)
    tickets = jax.random.randint(keys[3], shape, 0, PAIRS)
    active = (tickets < device_load).astype(jnp.int32)
    return jnp.stack([res_index, trav_index, active], axis=-1).astype(jnp.int32)


def level_of(own_key, shape, pieces, smallest, top_value):
    loudness, own = 1.0, jax.random.fold_in(own_key, 6)
    for dim, blocks in pieces:
        steps = jnp.exp(jax.random.uniform(jax.random.fold_in(own, dim), (blocks,), jnp.float32, smallest / len(pieces), top_value / len(pieces)))
        loudness = loudness * jnp.repeat(steps, shape[dim] // blocks).reshape([-1 if axis == dim else 1 for axis in range(len(shape))])
    return loudness


def gaussian(stream_key, extent, width, limit, shards=(), kind=jnp.bfloat16):
    values = jax.random.normal(stream_key, extent, jnp.float32) * width
    if len(shards) > 0:
        values = level_of(stream_key, extent, shards, -0.22, 0.18) * values
    return jnp.clip(values, min=-limit, max=limit).astype(kind)


def setup_inputs(seed: int = 0) -> dict:
    key_of = jax.random.split(jax.random.key(seed), 4)
    return {
        "residents": gaussian(key_of[0], (RESIDENTS, BOX, BOX * BOX), 1.0, 6.0, ((0, 256),)),
        "travellers": gaussian(key_of[1], (TRAVELLERS, BOX, BOX * BOX), 1.0, 6.0, ((0, 32),)),
        "pair_list": draw_pair_list(jax.random.fold_in(key_of[3], 71), 0),
    }


def sine_table(size):
    index = jnp.arange(size, dtype=jnp.float32) + 1.0
    return jnp.sqrt(2.0 / (size + 1)) * jnp.sin(jnp.pi * jnp.outer(index, index) / (size + 1))

def inverse_eigen(size):
    index = jnp.arange(size, dtype=jnp.float32) + 1.0
    eigen = 2.0 - 2.0 * jnp.cos(jnp.pi * index / (size + 1))
    total = eigen[:, None, None] + eigen[None, :, None] + eigen[None, None, :]
    return 1.0 / total

def transform(field, table):
    high = lax.Precision.HIGHEST
    field = jnp.einsum('ai,ijk->ajk', table, field, precision=high)
    field = jnp.einsum('bj,ajk->abk', table, field, precision=high)
    return jnp.einsum('ck,abk->abc', table, field, precision=high)

def reference(residents, travellers, pair_list):
    table = sine_table(BOX)
    inverse = inverse_eigen(BOX)
    per_device = STEPS * PAIRS
    count = N_BLK * N_GRP * per_device

    def visit(entry, totals):
        res_total, trav_total = totals
        device = entry // per_device
        arrival = entry // PAIRS % STEPS + 1
        slot = entry % PAIRS
        block = device // N_GRP
        source = (block - arrival + N_BLK) % N_BLK
        row = pair_list[device, arrival - 1, slot]
        res_row = (device * R_DEV + row[0]).astype(jnp.int32)
        trav_row = (source * TRAV + row[1]).astype(jnp.int32)
        active = row[2].astype(jnp.float32)
        resident = lax.dynamic_index_in_dim(residents, res_row, 0, False).astype(jnp.float32).reshape(BOX, BOX, BOX)
        traveller = lax.dynamic_index_in_dim(travellers, trav_row, 0, False).astype(jnp.float32).reshape(BOX, BOX, BOX)
        potential = transform(transform(resident * traveller, table) * inverse, table)
        res_add = (active * potential * traveller).reshape(1, BOX, BOX * BOX)
        trav_add = (active * potential * resident).reshape(1, BOX, BOX * BOX)
        res_old = lax.dynamic_index_in_dim(res_total, res_row, 0, True)
        res_total = lax.dynamic_update_index_in_dim(res_total, res_old + res_add, res_row, 0)
        trav_old = lax.dynamic_index_in_dim(trav_total, trav_row, 0, True)
        trav_total = lax.dynamic_update_index_in_dim(trav_total, trav_old + trav_add, trav_row, 0)
        return (res_total, trav_total)
    start = (jnp.zeros(residents.shape, jnp.float32), jnp.zeros(travellers.shape, jnp.float32))
    res_total, trav_total = lax.fori_loop(0, count, visit, start)
    return (res_total, trav_total)
```

```python
import functools

import jax
import jax.numpy as jnp
import numpy as np
from jax import lax
from jax.experimental import pallas as pl
from jax.experimental.pallas import tpu as pltpu
from jax.sharding import PartitionSpec as P

MESH = pl.DeviceIdType.MESH
F32, BF16, I16 = jnp.float32, jnp.bfloat16, jnp.int16
TOP = 32767.0


def tables(edge):
    half = edge // 2
    index = np.arange(edge, dtype=np.float64) + 1.0
    sine = np.sqrt(2.0 / (edge + 1)) * np.sin(np.pi * np.outer(index, index) / (edge + 1))
    eigen = 2.0 - 2.0 * np.cos(np.pi * index / (edge + 1))
    perm = np.zeros((2, 256, 256))
    for b8 in range(8):
        for c in range(edge):
            rc, cc = (0, c) if c < half else (1, edge - 1 - c)
            perm[0, b8 * edge + c, rc * 128 + b8 * half + cc] = 1.0
            perm[1, b8 * edge + c, rc * 128 + (7 - b8) * half + cc] = 1.0
    perms = np.concatenate([perm, perm.transpose(0, 2, 1)])
    planes, scales = [], []
    for pb in range(2):
        for pc in range(2):
            planes.append(np.kron(sine[pb::2, :half].T, sine[pc::2, :half].T))
            scales.append(
                1.0
                / (
                    eigen[:, None, None]
                    + eigen[None, pb::2, None]
                    + eigen[None, None, pc::2]
                ).reshape(edge, half * half)
            )
    planes = np.stack(planes)
    both = np.stack([planes, planes.transpose(0, 2, 1)]).astype(np.float32)
    high = both.astype(jnp.bfloat16)
    low = (both - high.astype(np.float32)).astype(jnp.bfloat16)
    weights = np.stack([high, low], axis=2)
    small = np.kron(np.eye(2), sine).astype(np.float32)
    small_high = small.astype(jnp.bfloat16)
    small_low = (small - small_high.astype(np.float32)).astype(jnp.bfloat16)
    rows = np.concatenate([small_high, small_high, small_low, small_low], axis=1)
    return (
        perms.astype(jnp.bfloat16),
        weights,
        rows,
        np.stack(scales).astype(np.float32),
    )


def dot(a, b):
    return jnp.dot(a, b, preferred_element_type=F32)


def split(x):
    high = x.astype(BF16)
    return high, (x - high.astype(F32)).astype(BF16)


def permuted(x, perm_ref):
    halves = []
    for rb in range(2):
        parts = [[None, None], [None, None]]
        for n in range(2):
            m = n if rb == 0 else 3 - n
            y = dot(x[:, m * 256 : (m + 1) * 256], perm_ref[rb])
            parts[0][n], parts[1][n] = y[:, :128], y[:, 128:]
        halves.append(jnp.concatenate(parts[0] + parts[1], axis=1))
    return halves


def restored(halves, perm_ref):
    rows = halves[0].shape[0]
    groups = [None] * 4
    for rb in range(2):
        for n in range(2):
            m = n if rb == 0 else 3 - n
            x = jnp.concatenate(
                [
                    halves[rb][:, n * 128 : (n + 1) * 128],
                    halves[rb][:, 256 + n * 128 : 256 + (n + 1) * 128],
                ],
                axis=1,
            )
            y = dot(jnp.concatenate(split(x), axis=0), perm_ref[2 + rb])
            groups[m] = y[:rows] + y[rows:]
    return jnp.concatenate(groups, axis=1)


def plane(g, weight_ref, way):
    out = []
    for p in range(4):
        high, low = split(g[p])
        rows = high.shape[0]
        a = dot(jnp.concatenate([high, low], axis=0), weight_ref[way, p, 0])
        out.append(a[:rows] + a[rows:] + dot(high, weight_ref[way, p, 1]))
    return out


def along_rows(g, rows):
    out = []
    for p in range(4):
        high, low = split(g[p])
        out.append(dot(rows, jnp.concatenate([high, low, high, low], axis=0)))
    return out


def peak(tiles):
    tiles = [jnp.abs(t) for t in tiles]
    while len(tiles) > 1:
        tiles = [
            jnp.maximum(tiles[i], tiles[i + 1]) if i + 1 < len(tiles) else tiles[i]
            for i in range(0, len(tiles), 2)
        ]
    return jnp.maximum(tiles[0], 1e-30)


def lane_tiles(x):
    return [x[:, j * 128 : (j + 1) * 128] for j in range(x.shape[1] // 128)]


def coded(x, wide):
    return jnp.round(x * wide).astype(jnp.int32)


def spread(tile, times):
    return jnp.concatenate([tile] * times, axis=1)


def kernel(
    res_hbm,
    trav_hbm,
    pair_ref,
    perm_hbm,
    weight_hbm,
    rows_hbm,
    scale_hbm,
    res_out,
    trav_out,
    res_in,
    trav_in,
    perm_ref,
    weight_ref,
    rows_ref,
    scale_ref,
    load_sem,
    mine,
    tbuf,
    ubuf,
    res_acc,
    ycode,
    yscale,
    yown,
    yget,
    ygets,
    hcode,
    hscale,
    hget,
    hgets,
    z_send,
    d_send,
    f_send,
    t_recv,
    y_send,
    ys_send,
    y_recv,
    ys_recv,
    h_send,
    hs_send,
    h_recv,
    hs_recv,
):
    n_blk = lax.axis_size("blk")
    blk, grp = lax.axis_index("blk"), lax.axis_index("grp")
    core = lax.rem(blk, 2)
    y, lo = grp // 2, lax.rem(grp, 2)

    def around(b):
        return lax.rem(b + n_blk, n_blk)

    loads = [
        pltpu.make_async_copy(src, dst, load_sem.at[j])
        for j, (src, dst) in enumerate(
            (
                (trav_hbm, trav_in),
                (perm_hbm, perm_ref),
                (res_hbm, res_in),
                (rows_hbm, rows_ref),
                (scale_hbm, scale_ref),
                (weight_hbm, weight_ref),
            )
        )
    ]
    for load in loads:
        load.start()

    barrier = pltpu.get_barrier_semaphore()
    count = 0
    for d in range(1, 4):
        for other in range(2):
            to = (blk - core + other, lax.rem(y + d, 4) * 2 + lo)
            pl.semaphore_signal(barrier, inc=1, device_id=to, device_id_type=MESH)
            count += 1
    for s in (-4, -3, -2, -1, 1, 2, 3, 4):
        for z in range(2):
            to = (around(blk + s), y * 2 + z)
            pl.semaphore_signal(barrier, inc=1, device_id=to, device_id_type=MESH)
            count += 1

    loads[0].wait()
    loads[1].wait()
    own = [h.reshape(2, 4, 8, 512) for h in permuted(trav_in[...].reshape(64, 1024), perm_ref)]
    for q in range(4):
        for t in range(2):
            mine[q, t] = jnp.concatenate([own[0][t, q], own[1][t, q]], axis=0).astype(BF16)

    pl.semaphore_wait(barrier, count)

    def remote(src, dst, send, recv, to):
        return pltpu.make_async_remote_copy(
            src_ref=src, dst_ref=dst, send_sem=send, recv_sem=recv, device_id=to, device_id_type=MESH
        )

    hops = []
    for near in range(2):
        slot = near * 2 + core
        hop = remote(
            mine.at[y],
            tbuf.at[slot, y],
            z_send.at[near],
            t_recv.at[slot, y],
            (around(blk + (2 if near else 4)), y * 2 + 1 - lo),
        )
        hop.start()
        hops.append(hop)

    def across(q):
        return remote(mine.at[q], tbuf.at[0, q], d_send.at[q], t_recv.at[0, q], (blk - core + 1, grp))

    @pl.when(core == 0)
    def _():
        for q in range(4):
            across(q).start()

    loads[2].wait()
    for rb, h in enumerate(permuted(res_in[...].reshape(64, 1024), perm_ref)):
        for r in range(2):
            ubuf[r, rb] = h[r * 32 : (r + 1) * 32]
    res_acc[...] = jnp.zeros_like(res_acc)

    def forward(near, d, swap):
        slot = near * 2 + core
        to_core = 1 - core if swap else core
        return remote(
            tbuf.at[slot, y],
            tbuf.at[slot, y],
            f_send.at[near, d, int(swap)],
            t_recv.at[slot, y],
            (blk - core + to_core, lax.rem(y + d, 4) * 2 + lo),
        )

    for near in range(2):
        hops[near].wait_recv()
        for d in range(1, 4):
            forward(near, d, False).start()
        if near:
            for d in range(4):
                forward(near, d, True).start()
        else:

            @pl.when(core == 1)
            def _():
                for d in range(4):
                    forward(0, d, True).start()

    for load in loads[3:]:
        load.wait()

    def arrived(slot, q):
        remote(tbuf.at[slot, q], tbuf.at[slot, q], z_send.at[0], t_recv.at[slot, q], (blk, grp)).wait_recv()

    def y_copies(i, d):
        to = (blk, lax.rem(y + d, 4) * 2 + lo)
        q = lax.rem(y + d, 4)
        return (
            remote(ycode.at[i, q], yget.at[i, d - 1], y_send.at[i, d - 1], y_recv.at[i, d - 1], to),
            remote(yscale.at[i], ygets.at[i, d - 1], ys_send.at[i, d - 1], ys_recv.at[i, d - 1], to),
        )

    def h_copies(i, z):
        s = lax.rem(3 - i + core, 4)
        to = (around(blk - 1 - s), y * 2 + z)
        at = s * 2 + lo
        return (
            remote(hcode.at[i, z], hget.at[at], h_send.at[i, z], h_recv.at[at], to),
            remote(hscale.at[i], hgets.at[at], hs_send.at[i, z], hs_recv.at[at], to),
        )

    def solve(i):
        s = lax.rem(3 - i + core, 4)
        pick = [[pair_ref[0, s, p, e] for e in range(3)] for p in range(2)]
        both = []
        for t in range(2):
            wide = tbuf[i, :, t].astype(F32).reshape(4, 2, 8, 512)
            both.append([wide[:, rb].reshape(32, 512) for rb in range(2)])
        u, w = [], []
        for p in range(2):
            u.append([ubuf[pick[p][0], rb] for rb in range(2)])
            second = pick[p][1] == 1
            w.append([jnp.where(second, both[1][rb], both[0][rb]) for rb in range(2)])
        d = [jnp.concatenate([u[p][rb] * w[p][rb] for p in range(2)], axis=0) for rb in range(2)]
        g = []
        for e in (d[0] + d[1], d[0] - d[1]):
            g += [e[:, :256] + e[:, 256:], e[:, :256] - e[:, 256:]]
        rows = rows_ref[...]
        g = along_rows(plane(g, weight_ref, 0), rows)
        g = [
            (m.reshape(2, 32, 256) * scale_ref[p][None]).reshape(64, 256)
            for p, m in enumerate(g)
        ]
        g = plane(along_rows(g, rows), weight_ref, 1)
        pot = []
        for e, o in (
            (g[0] + g[2], g[1] + g[3]),
            (g[0] - g[2], g[1] - g[3]),
        ):
            pot.append(jnp.concatenate([e + o, e - o], axis=1))

        def factor(p, e, value):
            return jnp.where(pick[p][e] == value, pick[p][2], 0).astype(F32)

        terms = [[None, None], [None, None]]
        for rb in range(2):
            v = [pot[rb][p * 32 : (p + 1) * 32] for p in range(2)]
            vw = [v[p] * w[p][rb] for p in range(2)]
            vu = [v[p] * u[p][rb] for p in range(2)]
            for j in range(2):
                res_acc[j, rb] += vw[0] * factor(0, 0, j) + vw[1] * factor(1, 0, j)
                terms[j][rb] = vu[0] * factor(0, 1, j) + vu[1] * factor(1, 1, j)
        top = peak([t for j in range(2) for rb in range(2) for a in range(4) for t in lane_tiles(terms[j][rb][a * 8 : (a + 1) * 8])])
        yscale[i] = top * (1.0 / TOP)
        wide = spread(TOP / top, 4)[None]
        for j in range(2):
            parts = []
            for rb in range(2):
                t = terms[j][rb].reshape(4, 8, 512)
                parts.append(coded(t, wide))
                for q in range(4):
                    yown[i, q, j, rb] = t[q]
            for q in range(4):
                ycode[i, q, j] = jnp.concatenate([parts[0][q], parts[1][q]], axis=0).astype(I16)

    def gather(i):
        sums = [[yown[i, y, j, rb] for rb in range(2)] for j in range(2)]
        for d in range(1, 4):
            for copy in y_copies(i, d):
                copy.wait_recv()
            scale = spread(ygets[i, d - 1], 4)
            for j in range(2):
                code = yget[i, d - 1, j].astype(jnp.int32).astype(F32)
                for rb in range(2):
                    sums[j][rb] += code[rb * 8 : (rb + 1) * 8] * scale
        first = lax.broadcasted_iota(jnp.int32, (8, 512), 0) < 4
        out = [
            [jnp.where(first, sums[0][rb], pltpu.roll(sums[1][rb], 4, 0)) for rb in range(2)],
            [jnp.where(first, pltpu.roll(sums[0][rb], 4, 0), sums[1][rb]) for rb in range(2)],
        ]
        top = peak([t for z in range(2) for rb in range(2) for t in lane_tiles(out[z][rb])])
        hscale[i] = top * (1.0 / TOP)
        wide = spread(TOP / top, 4)
        for z in range(2):
            hcode[i, z] = jnp.concatenate([coded(out[z][rb], wide) for rb in range(2)], axis=0).astype(I16)
            for copy in h_copies(i, z):
                copy.start()

    def step(i, carry):
        for d in range(1, 4):
            arrived(i, lax.rem(y + d, 4))

        @pl.when(lax.rem(i, 2) != core)
        def _():
            arrived(i, y)

        solve(i)
        for d in range(1, 4):
            for copy in y_copies(i, d):
                copy.start()

        @pl.when(i > 0)
        def _():
            gather(i - 1)

        return carry

    lax.fori_loop(0, 4, step, 0)

    for r in range(2):
        res_out[r] = restored([res_acc[r, rb] for rb in range(2)], perm_ref)
    gather(3)

    total = [jnp.zeros((8, 512), F32) for _ in range(2)]
    for at in range(8):
        remote(hcode.at[0, 0], hget.at[at], h_send.at[0, 0], h_recv.at[at], (blk, grp)).wait_recv()
        remote(hscale.at[0], hgets.at[at], hs_send.at[0, 0], hs_recv.at[at], (blk, grp)).wait_recv()
        code = hget[at].astype(jnp.int32).astype(F32)
        scale = spread(hgets[at], 4)
        for rb in range(2):
            total[rb] += code[rb * 8 : (rb + 1) * 8] * scale
    trav_out[...] = restored(total, perm_ref).reshape(2, 4, 1024)

    for near in range(2):
        hops[near].wait_send()
        for d in range(1, 4):
            forward(near, d, False).wait_send()
    for d in range(4):
        forward(1, d, True).wait_send()

    @pl.when(core == 1)
    def _():
        for d in range(4):
            forward(0, d, True).wait_send()

    @pl.when(core == 0)
    def _():
        for q in range(4):
            across(q).wait_send()

    for i in range(4):
        for d in range(1, 4):
            for copy in y_copies(i, d):
                copy.wait_send()
        for z in range(2):
            for copy in h_copies(i, z):
                copy.wait_send()


def local(residents, travellers, pair_list):
    consts = tables(32)
    hbm = pl.BlockSpec(memory_space=pltpu.HBM)
    vmem = pl.BlockSpec(memory_space=pltpu.VMEM)
    dma = pltpu.SemaphoreType.DMA
    return pl.pallas_call(
        kernel,
        out_shape=(
            jax.ShapeDtypeStruct((2, 32, 1024), F32),
            jax.ShapeDtypeStruct((2, 4, 1024), F32),
        ),
        in_specs=[hbm, hbm, pl.BlockSpec(memory_space=pltpu.SMEM), hbm, hbm, hbm, hbm],
        out_specs=(vmem, vmem),
        scratch_shapes=[
            pltpu.VMEM((2, 32, 1024), BF16),
            pltpu.VMEM((2, 32, 1024), BF16),
            pltpu.VMEM((4, 256, 256), BF16),
            pltpu.VMEM((2, 4, 2, 256, 256), BF16),
            pltpu.VMEM((64, 256), BF16),
            pltpu.VMEM((4, 32, 256), F32),
            dma((6,)),
            pltpu.VMEM((4, 2, 16, 512), BF16),
            pltpu.VMEM((4, 4, 2, 16, 512), BF16),
            pltpu.VMEM((2, 2, 32, 512), F32),
            pltpu.VMEM((2, 2, 32, 512), F32),
            pltpu.VMEM((4, 4, 2, 16, 512), I16),
            pltpu.VMEM((4, 8, 128), F32),
            pltpu.VMEM((4, 4, 2, 2, 8, 512), F32),
            pltpu.VMEM((4, 3, 2, 16, 512), I16),
            pltpu.VMEM((4, 3, 8, 128), F32),
            pltpu.VMEM((4, 2, 16, 512), I16),
            pltpu.VMEM((4, 8, 128), F32),
            pltpu.VMEM((8, 16, 512), I16),
            pltpu.VMEM((8, 8, 128), F32),
            dma((2,)),
            dma((4,)),
            dma((2, 4, 2)),
            dma((4, 4)),
            dma((4, 3)),
            dma((4, 3)),
            dma((4, 3)),
            dma((4, 3)),
            dma((4, 2)),
            dma((4, 2)),
            dma((8,)),
            dma((8,)),
        ],
        compiler_params=pltpu.CompilerParams(collective_id=0, has_side_effects=True),
    )(residents, travellers, pair_list, *[jnp.asarray(c) for c in consts])


def solution(mesh):
    return jax.shard_map(
        local,
        mesh=mesh,
        in_specs=(
            P(("blk", "grp"), None, None),
            P("blk", None, None),
            P(("blk", "grp"), None, None, None),
        ),
        out_specs=(P(("blk", "grp"), None, None), P("blk", "grp", None)),
        check_vma=False,
    )
```

```python
import functools

import jax
import jax.numpy as jnp
import numpy as np
from jax import lax
from jax.experimental import pallas as pl
from jax.experimental.pallas import tpu as pltpu
from jax.sharding import PartitionSpec as P

MESH = pl.DeviceIdType.MESH
F32, BF16, I16 = jnp.float32, jnp.bfloat16, jnp.int16
TOP = 32767.0


def tables(edge):
    half = edge // 2
    index = np.arange(edge, dtype=np.float64) + 1.0
    sine = np.sqrt(2.0 / (edge + 1)) * np.sin(np.pi * np.outer(index, index) / (edge + 1))
    eigen = 2.0 - 2.0 * np.cos(np.pi * index / (edge + 1))
    perm = np.zeros((2, 256, 256))
    for b8 in range(8):
        for c in range(edge):
            rc, cc = (0, c) if c < half else (1, edge - 1 - c)
            perm[0, b8 * edge + c, rc * 128 + b8 * half + cc] = 1.0
            perm[1, b8 * edge + c, rc * 128 + (7 - b8) * half + cc] = 1.0
    perms = np.concatenate([perm, perm.transpose(0, 2, 1)])
    planes, scales = [], []
    for pb in range(2):
        for pc in range(2):
            planes.append(np.kron(sine[pb::2, :half].T, sine[pc::2, :half].T))
            scales.append(
                1.0
                / (
                    eigen[:, None, None]
                    + eigen[None, pb::2, None]
                    + eigen[None, None, pc::2]
                ).reshape(edge, half * half)
            )
    planes = np.stack(planes)
    both = np.stack([planes, planes.transpose(0, 2, 1)]).astype(np.float32)
    high = both.astype(jnp.bfloat16)
    low = (both - high.astype(np.float32)).astype(jnp.bfloat16)
    weights = np.stack([high, low], axis=2)
    small = np.kron(np.eye(2), sine).astype(np.float32)
    small_high = small.astype(jnp.bfloat16)
    small_low = (small - small_high.astype(np.float32)).astype(jnp.bfloat16)
    rows = np.concatenate([small_high, small_high, small_low, small_low], axis=1)
    return (
        perms.astype(jnp.bfloat16),
        weights,
        rows,
        np.stack(scales).astype(np.float32),
    )


def dot(a, b):
    return jnp.dot(a, b, preferred_element_type=F32)


def split(x):
    high = x.astype(BF16)
    return high, (x - high.astype(F32)).astype(BF16)


def permuted(x, perm_ref):
    halves = []
    for rb in range(2):
        parts = [[None, None], [None, None]]
        for n in range(2):
            m = n if rb == 0 else 3 - n
            y = dot(x[:, m * 256 : (m + 1) * 256], perm_ref[rb])
            parts[0][n], parts[1][n] = y[:, :128], y[:, 128:]
        halves.append(jnp.concatenate(parts[0] + parts[1], axis=1))
    return halves


def restored(halves, perm_ref):
    rows = halves[0].shape[0]
    groups = [None] * 4
    for rb in range(2):
        for n in range(2):
            m = n if rb == 0 else 3 - n
            x = jnp.concatenate(
                [
                    halves[rb][:, n * 128 : (n + 1) * 128],
                    halves[rb][:, 256 + n * 128 : 256 + (n + 1) * 128],
                ],
                axis=1,
            )
            y = dot(jnp.concatenate(split(x), axis=0), perm_ref[2 + rb])
            groups[m] = y[:rows] + y[rows:]
    return jnp.concatenate(groups, axis=1)


def plane(g, weight_ref, way):
    out = []
    for p in range(4):
        high, low = split(g[p])
        rows = high.shape[0]
        a = dot(jnp.concatenate([high, low], axis=0), weight_ref[way, p, 0])
        out.append(a[:rows] + a[rows:] + dot(high, weight_ref[way, p, 1]))
    return out


def along_rows(g, rows):
    out = []
    for p in range(4):
        high, low = split(g[p])
        out.append(dot(rows, jnp.concatenate([high, low, high, low], axis=0)))
    return out


def peak(tiles):
    tiles = [jnp.abs(t) for t in tiles]
    while len(tiles) > 1:
        tiles = [
            jnp.maximum(tiles[i], tiles[i + 1]) if i + 1 < len(tiles) else tiles[i]
            for i in range(0, len(tiles), 2)
        ]
    return jnp.maximum(tiles[0], 1e-30)


def lane_tiles(x):
    return [x[:, j * 128 : (j + 1) * 128] for j in range(x.shape[1] // 128)]


def coded(x, wide):
    return jnp.round(x * wide).astype(jnp.int32)


def spread(tile, times):
    return jnp.concatenate([tile] * times, axis=1)


def kernel(
    res_hbm,
    trav_hbm,
    pair_hbm,
    perm_hbm,
    weight_hbm,
    rows_hbm,
    scale_hbm,
    res_out,
    trav_out,
    res_in,
    trav_in,
    pair_ref,
    perm_ref,
    weight_ref,
    rows_ref,
    scale_ref,
    load_sem,
    mine,
    tbuf,
    ubuf,
    res_acc,
    half,
    other,
    ysum,
    ycode,
    yscale,
    yget,
    ygets,
    hcode,
    hscale,
    hget,
    hgets,
    total,
    res_done,
    trav_done,
    out_sem,
    z_send,
    f_send,
    t_recv,
    x_send,
    x_recv,
    c_send,
    c_recv,
    y_send,
    ys_send,
    y_recv,
    ys_recv,
    h_send,
    hs_send,
    h_recv,
    hs_recv,
):
    n_blk = lax.axis_size("blk")
    blk, grp = lax.axis_index("blk"), lax.axis_index("grp")
    core = lax.rem(blk, 2)
    first = blk - core
    y, lo = grp // 2, lax.rem(grp, 2)
    partner = (first + 1 - core, grp)
    across_z = y * 2 + 1 - lo

    def around(b):
        return lax.rem(b + n_blk, n_blk)

    def y_peer(d):
        return lax.rem(y + d, 4)

    def remote(src, dst, send, recv, to):
        return pltpu.make_async_remote_copy(
            src_ref=src, dst_ref=dst, send_sem=send, recv_sem=recv, device_id=to, device_id_type=MESH
        )

    loads = [
        pltpu.make_async_copy(src, dst, load_sem.at[j])
        for j, (src, dst) in enumerate(
            (
                (trav_hbm, trav_in),
                (perm_hbm, perm_ref),
                (res_hbm, res_in),
                (pair_hbm, pair_ref),
                (rows_hbm, rows_ref),
                (scale_hbm, scale_ref),
                (weight_hbm, weight_ref),
            )
        )
    ]
    for load in loads:
        load.start()

    barrier = pltpu.get_barrier_semaphore()
    near_by = [(first + c, y_peer(d) * 2 + lo) for d in range(1, 4) for c in range(2)]
    near_by += [partner, (blk, across_z)]
    senders = [(around(blk - 4), across_z), (around(blk - 2), across_z)]
    for to in senders + near_by:
        pl.semaphore_signal(barrier, inc=1, device_id=to, device_id_type=MESH)

    loads[0].wait()
    loads[1].wait()
    own = [h.reshape(2, 4, 8, 512) for h in permuted(trav_in[...].reshape(64, 1024), perm_ref)]
    for q in range(4):
        for t in range(2):
            mine[q, t] = jnp.concatenate([own[0][t, q], own[1][t, q]], axis=0).astype(BF16)

    pl.semaphore_wait(barrier, len(senders) + len(near_by))

    hops = []
    for near in range(2):
        slot = near * 2 + core
        hop = remote(
            mine.at[y],
            tbuf.at[slot, y],
            z_send.at[near],
            t_recv.at[slot, y],
            (around(blk + (2 if near else 4)), across_z),
        )
        hop.start()
        hops.append(hop)

    def to_partner(slot, src):
        return remote(src, tbuf.at[slot], x_send.at[slot], x_recv.at[slot], partner)

    @pl.when(core == 0)
    def _():
        to_partner(0, mine).start()

    loads[2].wait()
    for rb, h in enumerate(permuted(res_in[...].reshape(64, 1024), perm_ref)):
        for r in range(2):
            ubuf[r, rb] = h[r * 32 : (r + 1) * 32]
    res_acc[...] = jnp.zeros_like(res_acc)

    def forward(near, d):
        slot = near * 2 + core
        return remote(
            tbuf.at[slot, y],
            tbuf.at[slot, y],
            f_send.at[near, d - 1],
            t_recv.at[slot, y],
            (blk, y_peer(d) * 2 + lo),
        )

    for near in range(2):
        hops[near].wait_recv()
        for d in range(1, 4):
            forward(near, d).start()

    for load in loads[3:]:
        load.wait()

    def to_other(i):
        return remote(half.at[i, 1 - core], other.at[i], c_send.at[i], c_recv.at[i], partner)

    def y_copies(e, d):
        to = (blk, y_peer(d) * 2 + lo)
        return (
            remote(ycode.at[e, y_peer(d)], yget.at[e, d - 1], y_send.at[e, d - 1], y_recv.at[e, d - 1], to),
            remote(
                yscale.at[e, pl.ds(0, 1)],
                ygets.at[e, d - 1, pl.ds(0, 1)],
                ys_send.at[e, d - 1],
                ys_recv.at[e, d - 1],
                to,
            ),
        )

    def h_copies(e):
        to = (around(first - 4 + e), y * 2 + core)
        at = (5 - e) // 2 * 2 + lo
        return (
            remote(hcode.at[e], hget.at[at], h_send.at[e], h_recv.at[at], to),
            remote(hscale.at[e, pl.ds(0, 1)], hgets.at[at, pl.ds(0, 1)], hs_send.at[e], hs_recv.at[at], to),
        )

    def solve(i):
        s = lax.rem(3 - i + core, 4)
        pick = [[pair_ref[0, e, p, s] for e in range(3)] for p in range(2)]
        both = []
        for t in range(2):
            wide = tbuf[i, :, t].astype(F32).reshape(4, 2, 8, 512)
            both.append([wide[:, rb].reshape(32, 512) for rb in range(2)])
        u, w = [], []
        for p in range(2):
            u.append([ubuf[pick[p][0], rb] for rb in range(2)])
            second = pick[p][1] == 1
            w.append([jnp.where(second, both[1][rb], both[0][rb]) for rb in range(2)])
        d = [jnp.concatenate([u[p][rb] * w[p][rb] for p in range(2)], axis=0) for rb in range(2)]
        g = []
        for e in (d[0] + d[1], d[0] - d[1]):
            g += [e[:, :256] + e[:, 256:], e[:, :256] - e[:, 256:]]
        rows = rows_ref[...]
        g = along_rows(plane(g, weight_ref, 0), rows)
        g = [
            (m.reshape(2, 32, 256) * scale_ref[p][None]).reshape(64, 256)
            for p, m in enumerate(g)
        ]
        g = plane(along_rows(g, rows), weight_ref, 1)
        pot = []
        for e, o in (
            (g[0] + g[2], g[1] + g[3]),
            (g[0] - g[2], g[1] - g[3]),
        ):
            pot.append(jnp.concatenate([e + o, e - o], axis=1))

        def factor(p, e, value):
            return jnp.where(pick[p][e] == value, pick[p][2], 0).astype(F32)

        upper = lax.broadcasted_iota(jnp.int32, (4, 8, 512), 1) < 4
        for rb in range(2):
            v = [pot[rb][p * 32 : (p + 1) * 32] for p in range(2)]
            vw = [v[p] * w[p][rb] for p in range(2)]
            vu = [v[p] * u[p][rb] for p in range(2)]
            terms = []
            for j in range(2):
                res_acc[j, rb] += vw[0] * factor(0, 0, j) + vw[1] * factor(1, 0, j)
                terms.append((vu[0] * factor(0, 1, j) + vu[1] * factor(1, 1, j)).reshape(4, 8, 512))
            half[i, 0, :, rb] = jnp.where(upper, terms[0], pltpu.roll(terms[1], 4, 1))
            half[i, 1, :, rb] = jnp.where(upper, pltpu.roll(terms[0], 4, 1), terms[1])

    def one_row(tiles):
        top = jnp.max(peak(tiles), axis=0, keepdims=True)
        return top, jnp.broadcast_to(TOP / top, (8, 128))

    def over_y(e, value):
        ysum[e] = value
        top, wide = one_row([t for q in range(4) for rb in range(2) for t in lane_tiles(value[q, rb])])
        yscale[e, pl.ds(0, 1)] = top * (1.0 / TOP)
        wide = spread(wide, 4)
        for q in range(4):
            ycode[e, q] = jnp.concatenate([coded(value[q, rb], wide) for rb in range(2)], axis=0).astype(I16)
        for d in range(1, 4):
            for copy in y_copies(e, d):
                copy.start()

    def widened(code_ref, scale_row):
        code = code_ref[...].astype(jnp.int32).astype(F32)
        scale = spread(jnp.broadcast_to(scale_row, (8, 128)), 4)
        return [code[rb * 8 : (rb + 1) * 8] * scale for rb in range(2)]

    def homeward(e):
        sums = [ysum[e, y, rb] for rb in range(2)]
        for d in range(1, 4):
            for copy in y_copies(e, d):
                copy.wait_recv()
            for rb, part in enumerate(widened(yget.at[e, d - 1], ygets[e, d - 1, pl.ds(0, 1)])):
                sums[rb] += part
        top, wide = one_row([t for rb in range(2) for t in lane_tiles(sums[rb])])
        hscale[e, pl.ds(0, 1)] = top * (1.0 / TOP)
        wide = spread(wide, 4)
        hcode[e] = jnp.concatenate([coded(sums[rb], wide) for rb in range(2)], axis=0).astype(I16)

    stays = jnp.logical_and(core == 0, lo == 0)

    def step(i, carry):
        @pl.when(i < 2)
        def _():
            slot = i * 2 + core
            for d in range(1, 4):
                q = y_peer(d)
                remote(mine.at[q], tbuf.at[slot, q], z_send.at[0], t_recv.at[slot, q], partner).wait_recv()

            @pl.when(slot > 0)
            def _():
                to_partner(slot, tbuf.at[slot]).start()

        @pl.when(lax.rem(i, 2) != core)
        def _():
            to_partner(i, mine).wait_recv()

        solve(i)
        to_other(i).start()

        @pl.when(i == 0)
        def _():
            over_y(4 * core, half[0, core])

        @pl.when(i == 1)
        def _():
            to_other(0).wait_recv()
            over_y(4 - 4 * core, other[0])

        @pl.when(i > 1)
        def _():
            to_other(i - 1).wait_recv()
            over_y(i - 1, half[i - 1, core] + other[i - 1])

        return carry

    lax.fori_loop(0, 4, step, 0)

    to_other(3).wait_recv()
    over_y(3, half[3, core] + other[3])
    for r in range(2):
        res_done[r] = restored([res_acc[r, rb] for rb in range(2)], perm_ref)
    outs = [
        pltpu.make_async_copy(res_done, res_out, out_sem.at[0]),
        pltpu.make_async_copy(trav_done, trav_out, out_sem.at[1]),
    ]
    outs[0].start()

    def send_home(e, carry):
        homeward(e)
        for copy in h_copies(e):
            copy.start()
        return carry

    lax.fori_loop(0, 4, send_home, 0)
    homeward(4)

    @pl.when(stays)
    def _():
        hget[0] = hcode[4]
        hgets[0, pl.ds(0, 1)] = hscale[4, pl.ds(0, 1)]

    @pl.when(jnp.logical_not(stays))
    def _():
        for copy in h_copies(4):
            copy.start()

    def from_home(at):
        return (
            remote(hcode.at[0], hget.at[at], h_send.at[0], h_recv.at[at], partner),
            remote(hscale.at[0, pl.ds(0, 1)], hgets.at[at, pl.ds(0, 1)], hs_send.at[0], hs_recv.at[at], partner),
        )

    def take(at):
        for rb, part in enumerate(widened(hget.at[at], hgets[at, pl.ds(0, 1)])):
            total[rb] += part

    total[...] = jnp.zeros_like(total)
    for at in range(2, 6):
        for copy in from_home(at):
            copy.wait_recv()
        take(at)

    @pl.when(core == 0)
    def _():
        for at in range(2):
            if at:
                for copy in from_home(at):
                    copy.wait_recv()
            else:

                @pl.when(lo > 0)
                def _():
                    for copy in from_home(0):
                        copy.wait_recv()

            take(at)

    trav_done[...] = restored([total[rb] for rb in range(2)], perm_ref).reshape(2, 4, 1024)
    outs[1].start()

    for near in range(2):
        hops[near].wait_send()
        for d in range(1, 4):
            forward(near, d).wait_send()
    to_partner(2 + core, mine).wait_send()
    to_partner(core, mine).wait_send()
    for i in range(4):
        to_other(i).wait_send()
    for e in range(5):
        for d in range(1, 4):
            for copy in y_copies(e, d):
                copy.wait_send()
        if e < 4:
            for copy in h_copies(e):
                copy.wait_send()

    @pl.when(jnp.logical_not(stays))
    def _():
        for copy in h_copies(4):
            copy.wait_send()

    for out in outs:
        out.wait()


def local(residents, travellers, pair_list):
    consts = tables(32)
    hbm = pl.BlockSpec(memory_space=pltpu.HBM)
    dma = pltpu.SemaphoreType.DMA
    return pl.pallas_call(
        kernel,
        out_shape=(
            jax.ShapeDtypeStruct((2, 32, 1024), F32),
            jax.ShapeDtypeStruct((2, 4, 1024), F32),
        ),
        in_specs=[hbm] * 7,
        out_specs=(hbm, hbm),
        scratch_shapes=[
            pltpu.VMEM((2, 32, 1024), BF16),
            pltpu.VMEM((2, 32, 1024), BF16),
            pltpu.SMEM((1, 3, 2, 4), jnp.int32),
            pltpu.VMEM((4, 256, 256), BF16),
            pltpu.VMEM((2, 4, 2, 256, 256), BF16),
            pltpu.VMEM((64, 256), BF16),
            pltpu.VMEM((4, 32, 256), F32),
            dma((7,)),
            pltpu.VMEM((4, 2, 16, 512), BF16),
            pltpu.VMEM((4, 4, 2, 16, 512), BF16),
            pltpu.VMEM((2, 2, 32, 512), F32),
            pltpu.VMEM((2, 2, 32, 512), F32),
            pltpu.VMEM((4, 2, 4, 2, 8, 512), F32),
            pltpu.VMEM((4, 4, 2, 8, 512), F32),
            pltpu.VMEM((5, 4, 2, 8, 512), F32),
            pltpu.VMEM((5, 4, 16, 512), I16),
            pltpu.VMEM((5, 8, 128), F32),
            pltpu.VMEM((5, 3, 16, 512), I16),
            pltpu.VMEM((5, 3, 8, 128), F32),
            pltpu.VMEM((5, 16, 512), I16),
            pltpu.VMEM((5, 8, 128), F32),
            pltpu.VMEM((6, 16, 512), I16),
            pltpu.VMEM((6, 8, 128), F32),
            pltpu.VMEM((2, 8, 512), F32),
            pltpu.VMEM((2, 32, 1024), F32),
            pltpu.VMEM((2, 4, 1024), F32),
            dma((2,)),
            dma((2,)),
            dma((2, 3)),
            dma((4, 4)),
            dma((4,)),
            dma((4,)),
            dma((4,)),
            dma((4,)),
            dma((5, 3)),
            dma((5, 3)),
            dma((5, 3)),
            dma((5, 3)),
            dma((5,)),
            dma((5,)),
            dma((6,)),
            dma((6,)),
        ],
        compiler_params=pltpu.CompilerParams(
            collective_id=0, has_side_effects=True
        ),
    )(residents, travellers, pair_list.transpose(0, 3, 2, 1), *[jnp.asarray(c) for c in consts])


def solution(mesh):
    return jax.shard_map(
        local,
        mesh=mesh,
        in_specs=(
            P(("blk", "grp"), None, None),
            P("blk", None, None),
            P(("blk", "grp"), None, None, None),
        ),
        out_specs=(P(("blk", "grp"), None, None), P("blk", "grp", None)),
        check_vma=False,
    )
```

```python
import functools

import jax
import jax.numpy as jnp
import numpy as np
from jax import lax
from jax.experimental import pallas as pl
from jax.experimental.pallas import tpu as pltpu
from jax.sharding import PartitionSpec as P

MESH = pl.DeviceIdType.MESH
F32, BF16, I16 = jnp.float32, jnp.bfloat16, jnp.int16
TOP = 32767.0


def tables(edge):
    half = edge // 2
    index = np.arange(edge, dtype=np.float64) + 1.0
    sine = np.sqrt(2.0 / (edge + 1)) * np.sin(np.pi * np.outer(index, index) / (edge + 1))
    eigen = 2.0 - 2.0 * np.cos(np.pi * index / (edge + 1))
    perm = np.zeros((2, 256, 256))
    for b8 in range(8):
        for c in range(edge):
            rc, cc = (0, c) if c < half else (1, edge - 1 - c)
            perm[0, b8 * edge + c, rc * 128 + b8 * half + cc] = 1.0
            perm[1, b8 * edge + c, rc * 128 + (7 - b8) * half + cc] = 1.0
    perms = np.concatenate([perm, perm.transpose(0, 2, 1)])
    planes, scales = [], []
    for pb in range(2):
        for pc in range(2):
            planes.append(np.kron(sine[pb::2, :half].T, sine[pc::2, :half].T))
            scales.append(
                1.0
                / (
                    eigen[:, None, None]
                    + eigen[None, pb::2, None]
                    + eigen[None, None, pc::2]
                ).reshape(edge, half * half)
            )
    planes = np.stack(planes)
    both = np.stack([planes, planes.transpose(0, 2, 1)]).astype(np.float32)
    high = both.astype(jnp.bfloat16)
    low = (both - high.astype(np.float32)).astype(jnp.bfloat16)
    weights = np.stack([high, low], axis=2)
    small = np.kron(np.eye(2), sine).astype(np.float32)
    small_high = small.astype(jnp.bfloat16)
    small_low = (small - small_high.astype(np.float32)).astype(jnp.bfloat16)
    rows = np.concatenate([small_high, small_high, small_low, small_low], axis=1)
    return (
        perms.astype(jnp.bfloat16),
        weights,
        rows,
        np.stack(scales).astype(np.float32),
    )


def dot(a, b):
    return jnp.dot(a, b, preferred_element_type=F32)


def split(x):
    high = x.astype(BF16)
    return high, (x - high.astype(F32)).astype(BF16)


def permuted(x, perm_ref):
    halves = []
    for rb in range(2):
        parts = [[None, None], [None, None]]
        for n in range(2):
            m = n if rb == 0 else 3 - n
            y = dot(x[:, m * 256 : (m + 1) * 256], perm_ref[rb])
            parts[0][n], parts[1][n] = y[:, :128], y[:, 128:]
        halves.append(jnp.concatenate(parts[0] + parts[1], axis=1))
    return halves


def restored(halves, perm_ref):
    rows = halves[0].shape[0]
    groups = [None] * 4
    for rb in range(2):
        for n in range(2):
            m = n if rb == 0 else 3 - n
            x = jnp.concatenate(
                [
                    halves[rb][:, n * 128 : (n + 1) * 128],
                    halves[rb][:, 256 + n * 128 : 256 + (n + 1) * 128],
                ],
                axis=1,
            )
            y = dot(jnp.concatenate(split(x), axis=0), perm_ref[2 + rb])
            groups[m] = y[:rows] + y[rows:]
    return jnp.concatenate(groups, axis=1)


def plane(g, weight_ref, way):
    out = []
    for p in range(4):
        high, low = split(g[p])
        rows = high.shape[0]
        a = dot(jnp.concatenate([high, low], axis=0), weight_ref[way, p, 0])
        out.append(a[:rows] + a[rows:] + dot(high, weight_ref[way, p, 1]))
    return out


def along_rows(g, rows):
    out = []
    for p in range(4):
        high, low = split(g[p])
        out.append(dot(rows, jnp.concatenate([high, low, high, low], axis=0)))
    return out


def peak(tiles):
    tiles = [jnp.abs(t) for t in tiles]
    while len(tiles) > 1:
        tiles = [
            jnp.maximum(tiles[i], tiles[i + 1]) if i + 1 < len(tiles) else tiles[i]
            for i in range(0, len(tiles), 2)
        ]
    return jnp.maximum(tiles[0], 1e-30)


def lane_tiles(x):
    return [x[:, j * 128 : (j + 1) * 128] for j in range(x.shape[1] // 128)]


def coded(x, wide):
    return jnp.round(x * wide).astype(jnp.int32)


def spread(tile, times):
    return jnp.concatenate([tile] * times, axis=1)


def kernel(
    res_hbm,
    trav_hbm,
    pair_hbm,
    perm_hbm,
    weight_hbm,
    rows_hbm,
    scale_hbm,
    res_out,
    trav_out,
    res_in,
    trav_in,
    pair_ref,
    perm_ref,
    weight_ref,
    rows_ref,
    scale_ref,
    load_sem,
    mine,
    tbuf,
    ubuf,
    res_acc,
    terms,
    other,
    ysum,
    ycode,
    yscale,
    yget,
    ygets,
    hcode,
    hscale,
    hget,
    hgets,
    total,
    z_send,
    f_send,
    t_recv,
    x_send,
    x_recv,
    c_send,
    c_recv,
    y_send,
    ys_send,
    y_recv,
    ys_recv,
    h_send,
    hs_send,
    h_recv,
    hs_recv,
):
    n_blk = lax.axis_size("blk")
    blk, grp = lax.axis_index("blk"), lax.axis_index("grp")
    core = lax.rem(blk, 2)
    first = blk - core
    y, lo = grp // 2, lax.rem(grp, 2)
    partner = (first + 1 - core, grp)
    across_z = y * 2 + 1 - lo

    def around(b):
        return lax.rem(b + n_blk, n_blk)

    def y_peer(d):
        return lax.rem(y + d, 4)

    def remote(src, dst, send, recv, to):
        return pltpu.make_async_remote_copy(
            src_ref=src, dst_ref=dst, send_sem=send, recv_sem=recv, device_id=to, device_id_type=MESH
        )

    loads = [
        pltpu.make_async_copy(src, dst, load_sem.at[j])
        for j, (src, dst) in enumerate(
            (
                (trav_hbm, trav_in),
                (perm_hbm, perm_ref),
                (res_hbm, res_in),
                (pair_hbm, pair_ref),
                (rows_hbm, rows_ref),
                (scale_hbm, scale_ref),
                (weight_hbm, weight_ref),
            )
        )
    ]
    for load in loads:
        load.start()

    barrier = pltpu.get_barrier_semaphore()
    near_by = [(blk, y_peer(d) * 2 + lo) for d in range(1, 4)] + [partner, (blk, across_z)]
    senders = [(around(blk - 4), across_z), (around(blk - 2), grp)]
    for to in senders + near_by:
        pl.semaphore_signal(barrier, inc=1, device_id=to, device_id_type=MESH)

    loads[0].wait()
    loads[1].wait()
    own = [h.reshape(2, 4, 8, 512) for h in permuted(trav_in[...].reshape(64, 1024), perm_ref)]
    for q in range(4):
        for t in range(2):
            mine[q, t] = jnp.concatenate([own[0][t, q], own[1][t, q]], axis=0).astype(BF16)

    pl.semaphore_wait(barrier, len(senders) + len(near_by))

    hops = []
    for near in range(2):
        slot = near * 2 + core
        hop = remote(
            mine.at[y],
            tbuf.at[slot, y],
            z_send.at[near],
            t_recv.at[slot, y],
            (around(blk + 2), grp) if near else (around(blk + 4), across_z),
        )
        hop.start()
        hops.append(hop)

    def to_partner(slot, src):
        return remote(src, tbuf.at[slot], x_send.at[slot], x_recv.at[slot], partner)

    @pl.when(core == 0)
    def _():
        to_partner(0, mine).start()

    loads[2].wait()
    for rb, h in enumerate(permuted(res_in[...].reshape(64, 1024), perm_ref)):
        for r in range(2):
            ubuf[r, rb] = h[r * 32 : (r + 1) * 32]
    res_acc[...] = jnp.zeros_like(res_acc)

    def forward(near, d):
        slot = near * 2 + core
        return remote(
            tbuf.at[slot, y],
            tbuf.at[slot, y],
            f_send.at[near, d - 1],
            t_recv.at[slot, y],
            (blk, y_peer(d) * 2 + lo),
        )

    for load in loads[3:]:
        load.wait()

    def to_other(slot):
        return remote(terms.at[slot], other.at[slot], c_send.at[slot], c_recv.at[slot], partner)

    def y_copies(e, d):
        to = (blk, y_peer(d) * 2 + lo)
        return (
            remote(ycode.at[e, y_peer(d)], yget.at[e, d - 1], y_send.at[e, d - 1], y_recv.at[e, d - 1], to),
            remote(
                yscale.at[e, pl.ds(0, 1)],
                ygets.at[e, d - 1, pl.ds(0, 1)],
                ys_send.at[e, d - 1],
                ys_recv.at[e, d - 1],
                to,
            ),
        )

    def h_copies(e):
        at = (5 - e) // 2 * 2 + lo
        copies = []
        for z in range(2):
            to = (around(first - 4 + e), y * 2 + z)
            copies += [
                remote(hcode.at[e, z], hget.at[at], h_send.at[e, z], h_recv.at[at], to),
                remote(hscale.at[e, pl.ds(0, 1)], hgets.at[at, pl.ds(0, 1)], hs_send.at[e, z], hs_recv.at[at], to),
            ]
        return copies

    def solve(i):
        s = lax.rem(3 - i + core, 4)
        pick = [[pair_ref[0, e, p, s] for e in range(3)] for p in range(2)]
        both = []
        for t in range(2):
            wide = tbuf[i, :, t].astype(F32).reshape(4, 2, 8, 512)
            both.append([wide[:, rb].reshape(32, 512) for rb in range(2)])
        u, w = [], []
        for p in range(2):
            u.append([ubuf[pick[p][0], rb] for rb in range(2)])
            second = pick[p][1] == 1
            w.append([jnp.where(second, both[1][rb], both[0][rb]) for rb in range(2)])
        d = [jnp.concatenate([u[p][rb] * w[p][rb] for p in range(2)], axis=0) for rb in range(2)]
        g = []
        for e in (d[0] + d[1], d[0] - d[1]):
            g += [e[:, :256] + e[:, 256:], e[:, :256] - e[:, 256:]]
        rows = rows_ref[...]
        g = along_rows(plane(g, weight_ref, 0), rows)
        g = [
            (m.reshape(2, 32, 256) * scale_ref[p][None]).reshape(64, 256)
            for p, m in enumerate(g)
        ]
        g = plane(along_rows(g, rows), weight_ref, 1)
        pot = []
        for e, o in (
            (g[0] + g[2], g[1] + g[3]),
            (g[0] - g[2], g[1] - g[3]),
        ):
            pot.append(jnp.concatenate([e + o, e - o], axis=1))

        def factor(p, e, value):
            return jnp.where(pick[p][e] == value, pick[p][2], 0).astype(F32)

        for rb in range(2):
            v = [pot[rb][p * 32 : (p + 1) * 32] for p in range(2)]
            vw = [v[p] * w[p][rb] for p in range(2)]
            vu = [v[p] * u[p][rb] for p in range(2)]
            for j in range(2):
                res_acc[j, rb] += vw[0] * factor(0, 0, j) + vw[1] * factor(1, 0, j)
                terms[i, :, j, rb] = (vu[0] * factor(0, 1, j) + vu[1] * factor(1, 1, j)).reshape(4, 8, 512)

    def one_row(tiles):
        top = jnp.max(peak(tiles), axis=0, keepdims=True)
        return top, jnp.broadcast_to(TOP / top, (8, 128))

    def over_y(e, value):
        ysum[e] = value
        parts = [(q, t, rb) for q in range(4) for t in range(2) for rb in range(2)]
        top, wide = one_row([x for at in parts for x in lane_tiles(value[at])])
        yscale[e, pl.ds(0, 1)] = top * (1.0 / TOP)
        wide = spread(wide, 4)
        for q in range(4):
            for t in range(2):
                ycode[e, q, t] = jnp.concatenate([coded(value[q, t, rb], wide) for rb in range(2)], axis=0).astype(I16)
        for d in range(1, 4):
            for copy in y_copies(e, d):
                copy.start()

    def widened(code_ref, scale_row):
        code = code_ref[...].astype(jnp.int32).astype(F32)
        scale = spread(jnp.broadcast_to(scale_row, (8, 128)), 4)
        return [code[rb * 8 : (rb + 1) * 8] * scale for rb in range(2)]

    def homeward(e):
        sums = [[ysum[e, y, t, rb] for rb in range(2)] for t in range(2)]
        for d in range(1, 4):
            for copy in y_copies(e, d):
                copy.wait_recv()
            for t in range(2):
                for rb, part in enumerate(widened(yget.at[e, d - 1, t], ygets[e, d - 1, pl.ds(0, 1)])):
                    sums[t][rb] += part
        upper = lax.broadcasted_iota(jnp.int32, (8, 512), 0) < 4
        rows = [
            [jnp.where(upper, sums[0][rb], pltpu.roll(sums[1][rb], 4, 0)) for rb in range(2)],
            [jnp.where(upper, pltpu.roll(sums[0][rb], 4, 0), sums[1][rb]) for rb in range(2)],
        ]
        top, wide = one_row([x for z in range(2) for rb in range(2) for x in lane_tiles(rows[z][rb])])
        hscale[e, pl.ds(0, 1)] = top * (1.0 / TOP)
        wide = spread(wide, 4)
        for z in range(2):
            hcode[e, z] = jnp.concatenate([coded(rows[z][rb], wide) for rb in range(2)], axis=0).astype(I16)
        for copy in h_copies(e):
            copy.start()

    def slot_at(i):
        return (1 - core) * (lax.rem(2 * i, 3) + i // 3 * 3) + core * (i + i // 2 - i // 3 * 2)

    def entry_of(slot):
        return slot + 4 * core * (1 - (slot + 3) // 4)

    def step(i, carry):
        slot = slot_at(i)

        @pl.when(i == core)
        def _():
            for near in range(2):
                hops[near].wait_recv()
                for d in range(1, 4):
                    forward(near, d).start()

        own = jnp.logical_or(i == core, i == core + 1)

        @pl.when(own)
        def _():
            for d in range(1, 4):
                q = y_peer(d)
                remote(mine.at[q], tbuf.at[slot, q], z_send.at[0], t_recv.at[slot, q], partner).wait_recv()

            @pl.when(slot > 0)
            def _():
                to_partner(slot, tbuf.at[slot]).start()

        @pl.when(jnp.logical_not(own))
        def _():
            to_partner(slot, mine).wait_recv()

        solve(slot)
        gives = jnp.logical_or(i == 1, jnp.logical_and(i == 2, core == 1))

        @pl.when(gives)
        def _():
            to_other(slot).start()

        @pl.when(i == 0)
        def _():
            over_y(4 * core, terms[0])

        @pl.when(jnp.logical_and(i > 0, jnp.logical_not(gives)))
        def _():
            to_other(slot).wait_recv()
            over_y(slot, terms[slot] + other[slot])

        return carry

    lax.fori_loop(0, 4, step, 0)

    for r in range(2):
        res_out[r] = restored([res_acc[r, rb] for rb in range(2)], perm_ref)

    def entry_at(j):
        return (1 - core) * (j + j // 2) + core * (4 - 2 * j)

    def send_home(j, carry):
        @pl.when(j < 3 - core)
        def _():
            homeward(entry_at(j))

        return carry

    lax.fori_loop(0, 3, send_home, 0)

    def from_home(at):
        return (
            remote(hcode.at[0, 0], hget.at[at], h_send.at[0, 0], h_recv.at[at], partner),
            remote(hscale.at[0, pl.ds(0, 1)], hgets.at[at, pl.ds(0, 1)], hs_send.at[0, 0], hs_recv.at[at], partner),
        )

    def take(at):
        for rb, part in enumerate(widened(hget.at[at], hgets[at, pl.ds(0, 1)])):
            total[rb] += part

    total[...] = jnp.zeros_like(total)
    for at in range(2, 6):
        for copy in from_home(at):
            copy.wait_recv()
        take(at)

    @pl.when(core == 0)
    def _():
        for at in range(2):
            for copy in from_home(at):
                copy.wait_recv()
            take(at)

    trav_out[...] = restored([total[rb] for rb in range(2)], perm_ref).reshape(2, 4, 1024)

    for near in range(2):
        hops[near].wait_send()
        for d in range(1, 4):
            forward(near, d).wait_send()
    to_partner(2 + core, mine).wait_send()
    to_partner(core, mine).wait_send()
    to_other(2 - core).wait_send()

    @pl.when(core == 1)
    def _():
        to_other(3).wait_send()

    def sent(j, carry):
        @pl.when(j < 3 - core)
        def _():
            for d in range(1, 4):
                for copy in y_copies(entry_at(j), d):
                    copy.wait_send()
            for copy in h_copies(entry_at(j)):
                copy.wait_send()

        return carry

    lax.fori_loop(0, 3, sent, 0)


def store(res_ref, trav_ref, res_out, trav_out, sem):
    copies = [
        pltpu.make_async_copy(res_ref, res_out, sem.at[0]),
        pltpu.make_async_copy(trav_ref, trav_out, sem.at[1]),
    ]
    for copy in copies:
        copy.start()
    for copy in copies:
        copy.wait()


def local(residents, travellers, pair_list):
    consts = tables(32)
    hbm = pl.BlockSpec(memory_space=pltpu.HBM)
    vmem = pl.BlockSpec(memory_space=pltpu.VMEM)
    dma = pltpu.SemaphoreType.DMA
    done = pl.pallas_call(
        kernel,
        out_shape=(pltpu.VMEM((2, 32, 1024), F32), pltpu.VMEM((2, 4, 1024), F32)),
        in_specs=[hbm] * 7,
        out_specs=(vmem, vmem),
        scratch_shapes=[
            pltpu.VMEM((2, 32, 1024), BF16),
            pltpu.VMEM((2, 32, 1024), BF16),
            pltpu.SMEM((1, 3, 2, 4), jnp.int32),
            pltpu.VMEM((4, 256, 256), BF16),
            pltpu.VMEM((2, 4, 2, 256, 256), BF16),
            pltpu.VMEM((64, 256), BF16),
            pltpu.VMEM((4, 32, 256), F32),
            dma((7,)),
            pltpu.VMEM((4, 2, 16, 512), BF16),
            pltpu.VMEM((4, 4, 2, 16, 512), BF16),
            pltpu.VMEM((2, 2, 32, 512), F32),
            pltpu.VMEM((2, 2, 32, 512), F32),
            pltpu.VMEM((4, 4, 2, 2, 8, 512), F32),
            pltpu.VMEM((4, 4, 2, 2, 8, 512), F32),
            pltpu.VMEM((5, 4, 2, 2, 8, 512), F32),
            pltpu.VMEM((5, 4, 2, 16, 512), I16),
            pltpu.VMEM((5, 8, 128), F32),
            pltpu.VMEM((5, 3, 2, 16, 512), I16),
            pltpu.VMEM((5, 3, 8, 128), F32),
            pltpu.VMEM((5, 2, 16, 512), I16),
            pltpu.VMEM((5, 8, 128), F32),
            pltpu.VMEM((6, 16, 512), I16),
            pltpu.VMEM((6, 8, 128), F32),
            pltpu.VMEM((2, 8, 512), F32),
            dma((2,)),
            dma((2, 3)),
            dma((4, 4)),
            dma((4,)),
            dma((4,)),
            dma((4,)),
            dma((4,)),
            dma((5, 3)),
            dma((5, 3)),
            dma((5, 3)),
            dma((5, 3)),
            dma((5, 2)),
            dma((5, 2)),
            dma((6,)),
            dma((6,)),
        ],
        compiler_params=pltpu.CompilerParams(
            collective_id=0, has_side_effects=True
        ),
    )(residents, travellers, pair_list.transpose(0, 3, 2, 1), *[jnp.asarray(c) for c in consts])
    return pl.pallas_call(
        store,
        out_shape=(
            jax.ShapeDtypeStruct((2, 32, 1024), F32),
            jax.ShapeDtypeStruct((2, 4, 1024), F32),
        ),
        in_specs=[vmem] * 2,
        out_specs=(hbm, hbm),
        scratch_shapes=[dma((2,))],
        compiler_params=pltpu.CompilerParams(vmem_limit_bytes=2**20),
    )(*done)


def solution(mesh):
    return jax.shard_map(
        local,
        mesh=mesh,
        in_specs=(
            P(("blk", "grp"), None, None),
            P("blk", None, None),
            P(("blk", "grp"), None, None, None),
        ),
        out_specs=(P(("blk", "grp"), None, None), P("blk", "grp", None)),
        check_vma=False,
    )
```

```python
import functools

import jax
import jax.numpy as jnp
import numpy as np
from jax import lax
from jax.experimental import pallas as pl
from jax.experimental.pallas import tpu as pltpu
from jax.sharding import PartitionSpec as P

MESH = pl.DeviceIdType.MESH
F32, BF16, I16 = jnp.float32, jnp.bfloat16, jnp.int16
TOP = 32767.0


def tables(edge):
    half = edge // 2
    index = np.arange(edge, dtype=np.float64) + 1.0
    sine = np.sqrt(2.0 / (edge + 1)) * np.sin(np.pi * np.outer(index, index) / (edge + 1))
    eigen = 2.0 - 2.0 * np.cos(np.pi * index / (edge + 1))
    perm = np.zeros((2, 256, 256))
    for b8 in range(8):
        for c in range(edge):
            rc, cc = (0, c) if c < half else (1, edge - 1 - c)
            perm[0, b8 * edge + c, rc * 128 + b8 * half + cc] = 1.0
            perm[1, b8 * edge + c, rc * 128 + (7 - b8) * half + cc] = 1.0
    perms = np.concatenate([perm, perm.transpose(0, 2, 1)])
    planes, scales = [], []
    for pb in range(2):
        for pc in range(2):
            planes.append(np.kron(sine[pb::2, :half].T, sine[pc::2, :half].T))
            scales.append(
                1.0
                / (
                    eigen[:, None, None]
                    + eigen[None, pb::2, None]
                    + eigen[None, None, pc::2]
                ).reshape(edge, half * half)
            )
    planes = np.stack(planes)
    both = np.stack([planes, planes.transpose(0, 2, 1)]).astype(np.float32)
    high = both.astype(jnp.bfloat16)
    low = (both - high.astype(np.float32)).astype(jnp.bfloat16)
    weights = np.stack([high, low], axis=2)
    small = np.kron(np.eye(2), sine).astype(np.float32)
    small_high = small.astype(jnp.bfloat16)
    small_low = (small - small_high.astype(np.float32)).astype(jnp.bfloat16)
    rows = np.concatenate([small_high, small_high, small_low, small_low], axis=1)
    return (
        perms.astype(jnp.bfloat16),
        weights,
        rows,
        np.stack(scales).astype(np.float32),
    )


def dot(a, b):
    return jnp.dot(a, b, preferred_element_type=F32)


def split(x):
    high = x.astype(BF16)
    return high, (x - high.astype(F32)).astype(BF16)


def permuted(x, perm_ref):
    halves = []
    for rb in range(2):
        parts = [[None, None], [None, None]]
        for n in range(2):
            m = n if rb == 0 else 3 - n
            y = dot(x[:, m * 256 : (m + 1) * 256], perm_ref[rb])
            parts[0][n], parts[1][n] = y[:, :128], y[:, 128:]
        halves.append(jnp.concatenate(parts[0] + parts[1], axis=1))
    return halves


def restored(halves, perm_ref):
    rows = halves[0].shape[0]
    groups = [None] * 4
    for rb in range(2):
        for n in range(2):
            m = n if rb == 0 else 3 - n
            x = jnp.concatenate(
                [
                    halves[rb][:, n * 128 : (n + 1) * 128],
                    halves[rb][:, 256 + n * 128 : 256 + (n + 1) * 128],
                ],
                axis=1,
            )
            y = dot(jnp.concatenate(split(x), axis=0), perm_ref[2 + rb])
            groups[m] = y[:rows] + y[rows:]
    return jnp.concatenate(groups, axis=1)


def plane(g, weight_ref, way):
    out = []
    for p in range(4):
        high, low = split(g[p])
        rows = high.shape[0]
        a = dot(jnp.concatenate([high, low], axis=0), weight_ref[way, p, 0])
        out.append(a[:rows] + a[rows:] + dot(high, weight_ref[way, p, 1]))
    return out


def along_rows(g, rows):
    out = []
    for p in range(4):
        high, low = split(g[p])
        out.append(dot(rows, jnp.concatenate([high, low, high, low], axis=0)))
    return out


def peak(tiles):
    tiles = [jnp.abs(t) for t in tiles]
    while len(tiles) > 1:
        tiles = [
            jnp.maximum(tiles[i], tiles[i + 1]) if i + 1 < len(tiles) else tiles[i]
            for i in range(0, len(tiles), 2)
        ]
    return jnp.maximum(tiles[0], 1e-30)


def lane_tiles(x):
    return [x[:, j * 128 : (j + 1) * 128] for j in range(x.shape[1] // 128)]


def coded(x, wide):
    return jnp.round(x * wide).astype(jnp.int32)


def spread(tile, times):
    return jnp.concatenate([tile] * times, axis=1)


def kernel(
    res_hbm,
    trav_hbm,
    pair_hbm,
    perm_hbm,
    weight_hbm,
    rows_hbm,
    scale_hbm,
    res_out,
    trav_out,
    res_in,
    trav_in,
    pair_ref,
    perm_ref,
    weight_ref,
    rows_ref,
    scale_ref,
    load_sem,
    mine,
    tbuf,
    ubuf,
    res_acc,
    terms,
    other,
    ycode,
    yscale,
    yget,
    ygets,
    hcode,
    hscale,
    hget,
    hgets,
    total,
    z_send,
    f_send,
    t_recv,
    x_send,
    x_recv,
    c_send,
    c_recv,
    y_send,
    ys_send,
    y_recv,
    ys_recv,
    h_send,
    hs_send,
    h_recv,
    hs_recv,
):
    n_blk = lax.axis_size("blk")
    blk, grp = lax.axis_index("blk"), lax.axis_index("grp")
    core = lax.rem(blk, 2)
    first = blk - core
    y, lo = grp // 2, lax.rem(grp, 2)
    partner = (first + 1 - core, grp)
    across_z = y * 2 + 1 - lo

    def around(b):
        return lax.rem(b + n_blk, n_blk)

    def y_peer(d):
        return lax.rem(y + d, 4)

    def remote(src, dst, send, recv, to):
        return pltpu.make_async_remote_copy(
            src_ref=src, dst_ref=dst, send_sem=send, recv_sem=recv, device_id=to, device_id_type=MESH
        )

    loads = [
        pltpu.make_async_copy(src, dst, load_sem.at[j])
        for j, (src, dst) in enumerate(
            (
                (trav_hbm, trav_in),
                (perm_hbm, perm_ref),
                (res_hbm, res_in),
                (pair_hbm, pair_ref),
                (rows_hbm, rows_ref),
                (scale_hbm, scale_ref),
                (weight_hbm, weight_ref),
            )
        )
    ]
    for load in loads:
        load.start()

    barrier = pltpu.get_barrier_semaphore()

    def arrive(to):
        pl.semaphore_signal(barrier, inc=1, device_id=to, device_id_type=MESH)

    arrive(partner)
    arrive((blk, across_z))

    @pl.when(core == 1)
    def _():
        for c in range(2):
            arrive((around(first - 4 + c), across_z))
            arrive((around(first - 2 + c), grp))
            for d in range(1, 4):
                arrive((first + c, y_peer(d) * 2 + lo))

    loads[0].wait()
    loads[1].wait()
    own = [h.reshape(2, 4, 8, 512) for h in permuted(trav_in[...].reshape(64, 1024), perm_ref)]
    for q in range(4):
        for t in range(2):
            mine[q, t] = jnp.concatenate([own[0][t, q], own[1][t, q]], axis=0).astype(BF16)

    pl.semaphore_wait(barrier, 7)

    hops = []
    for near in range(2):
        slot = near * 2 + core
        hop = remote(
            mine.at[y],
            tbuf.at[slot, y],
            z_send.at[near],
            t_recv.at[slot, y],
            (around(first + 3), grp) if near else (around(first + 5), across_z),
        )
        hop.start()
        hops.append(hop)

    def to_partner(slot, src):
        return remote(src, tbuf.at[slot], x_send.at[slot], x_recv.at[slot], partner)

    @pl.when(core == 0)
    def _():
        to_partner(4, mine).start()

    loads[2].wait()
    for rb, h in enumerate(permuted(res_in[...].reshape(64, 1024), perm_ref)):
        for r in range(2):
            ubuf[r, rb] = h[r * 32 : (r + 1) * 32]
    res_acc[...] = jnp.zeros_like(res_acc)

    for e in (0, 4):
        other[e] = jnp.zeros((4, 2, 2, 8, 512), F32)

    def quarter(slot, q):
        return remote(mine.at[q], tbuf.at[slot, q], z_send.at[0], t_recv.at[slot, q], partner)

    def forward(slot, d):
        return remote(
            tbuf.at[slot, y],
            tbuf.at[slot, y],
            f_send.at[slot, d - 1],
            t_recv.at[slot, y],
            (blk, y_peer(d) * 2 + lo),
        )

    for load in loads[3:]:
        load.wait()

    def to_other(slot):
        return remote(terms.at[slot], other.at[slot], c_send.at[slot], c_recv.at[slot], partner)

    def y_copies(e, d):
        to = (first + 1, y_peer(d) * 2 + lo)
        return (
            remote(ycode.at[e, y_peer(d)], yget.at[e, d], y_send.at[e, d], y_recv.at[e, d], to),
            remote(
                yscale.at[e, pl.ds(0, 1)],
                ygets.at[e, d, pl.ds(0, 1)],
                ys_send.at[e, d],
                ys_recv.at[e, d],
                to,
            ),
        )

    def h_copies(e):
        at = (5 - e) // 2 * 2 + lo
        copies = []
        for z in range(2):
            to = (around(first - 4 + e), y * 2 + z)
            copies += [
                remote(hcode.at[e, z], hget.at[at], h_send.at[e, z], h_recv.at[at], to),
                remote(hscale.at[e, pl.ds(0, 1)], hgets.at[at, pl.ds(0, 1)], hs_send.at[e, z], hs_recv.at[at], to),
            ]
        return copies

    def solve(i):
        s = lax.rem(3 - i + core, 4)
        pick = [[pair_ref[0, e, p, s] for e in range(3)] for p in range(2)]
        both = []
        for t in range(2):
            wide = tbuf[i, :, t].astype(F32).reshape(4, 2, 8, 512)
            both.append([wide[:, rb].reshape(32, 512) for rb in range(2)])
        u, w = [], []
        for p in range(2):
            u.append([ubuf[pick[p][0], rb] for rb in range(2)])
            second = pick[p][1] == 1
            w.append([jnp.where(second, both[1][rb], both[0][rb]) for rb in range(2)])
        d = [jnp.concatenate([u[p][rb] * w[p][rb] for p in range(2)], axis=0) for rb in range(2)]
        g = []
        for e in (d[0] + d[1], d[0] - d[1]):
            g += [e[:, :256] + e[:, 256:], e[:, :256] - e[:, 256:]]
        rows = rows_ref[...]
        g = along_rows(plane(g, weight_ref, 0), rows)
        g = [
            (m.reshape(2, 32, 256) * scale_ref[p][None]).reshape(64, 256)
            for p, m in enumerate(g)
        ]
        g = plane(along_rows(g, rows), weight_ref, 1)
        pot = []
        for e, o in (
            (g[0] + g[2], g[1] + g[3]),
            (g[0] - g[2], g[1] - g[3]),
        ):
            pot.append(jnp.concatenate([e + o, e - o], axis=1))

        def factor(p, e, value):
            return jnp.where(pick[p][e] == value, pick[p][2], 0).astype(F32)

        for rb in range(2):
            v = [pot[rb][p * 32 : (p + 1) * 32] for p in range(2)]
            vw = [v[p] * w[p][rb] for p in range(2)]
            vu = [v[p] * u[p][rb] for p in range(2)]
            for j in range(2):
                res_acc[j, rb] += vw[0] * factor(0, 0, j) + vw[1] * factor(1, 0, j)
                terms[i, :, j, rb] = (vu[0] * factor(0, 1, j) + vu[1] * factor(1, 1, j)).reshape(4, 8, 512)

    def one_row(tiles):
        top = jnp.max(peak(tiles), axis=0, keepdims=True)
        return top, jnp.broadcast_to(TOP / top, (8, 128))

    def over_y(e, value):
        parts = [(q, t, rb) for q in range(4) for t in range(2) for rb in range(2)]
        top, wide = one_row([x for at in parts for x in lane_tiles(value[at])])
        yscale[e, pl.ds(0, 1)] = top * (1.0 / TOP)
        wide = spread(wide, 4)
        for q in range(4):
            for t in range(2):
                ycode[e, q, t] = jnp.concatenate([coded(value[q, t, rb], wide) for rb in range(2)], axis=0).astype(I16)
        for d in range(1, 4):
            for copy in y_copies(e, d):
                copy.start()

        @pl.when(core == 0)
        def _():
            for copy in y_copies(e, 0):
                copy.start()

        @pl.when(core == 1)
        def _():
            yget[4, 0] = ycode[4, y]
            ygets[4, 0, pl.ds(0, 1)] = yscale[4, pl.ds(0, 1)]

    def widened(code_ref, scale_row):
        code = code_ref[...].astype(jnp.int32).astype(F32)
        scale = spread(jnp.broadcast_to(scale_row, (8, 128)), 4)
        return [code[rb * 8 : (rb + 1) * 8] * scale for rb in range(2)]

    def homeward(e):
        @pl.when(e < 4)
        def _():
            for copy in y_copies(e, 0):
                copy.wait_recv()

        sums = [widened(yget.at[e, 0, t], ygets[e, 0, pl.ds(0, 1)]) for t in range(2)]
        for d in range(1, 4):
            for copy in y_copies(e, d):
                copy.wait_recv()
            for t in range(2):
                for rb, part in enumerate(widened(yget.at[e, d, t], ygets[e, d, pl.ds(0, 1)])):
                    sums[t][rb] += part
        upper = lax.broadcasted_iota(jnp.int32, (8, 512), 0) < 4
        rows = [
            [jnp.where(upper, sums[0][rb], pltpu.roll(sums[1][rb], 4, 0)) for rb in range(2)],
            [jnp.where(upper, pltpu.roll(sums[0][rb], 4, 0), sums[1][rb]) for rb in range(2)],
        ]
        top, wide = one_row([x for z in range(2) for rb in range(2) for x in lane_tiles(rows[z][rb])])
        hscale[e, pl.ds(0, 1)] = top * (1.0 / TOP)
        wide = spread(wide, 4)
        for z in range(2):
            hcode[e, z] = jnp.concatenate([coded(rows[z][rb], wide) for rb in range(2)], axis=0).astype(I16)
        for copy in h_copies(e):
            copy.start()

    def first_order(i):
        return (1 - i // 2) * (1 - i) + i // 2 * i

    def spread_slots(slots):
        for slot in slots:
            for d in range(1, 4):
                quarter(slot, y_peer(d)).wait_recv()
            to_partner(slot, tbuf.at[slot]).start()

    def step(i, carry):
        slot = (1 - core) * first_order(i) + core * (i + 4 * (1 - (i + 3) // 4))

        @pl.when(jnp.logical_and(core == 1, i == 1))
        def _():
            for s in (1, 0, 3, 2):
                quarter(s, y).wait_recv()
                for d in range(1, 4):
                    forward(s, d).start()
            spread_slots((1, 0))

        @pl.when(jnp.logical_and(core == 1, i == 2))
        def _():
            spread_slots((2, 3))

        takes = jnp.logical_or(core == 0, i == 0)

        @pl.when(takes)
        def _():
            to_partner(slot, mine).wait_recv()

        solve(slot)

        @pl.when(jnp.logical_not(takes))
        def _():
            to_other(slot).start()

        @pl.when(jnp.logical_and(core == 0, slot > 0))
        def _():
            to_other(slot).wait_recv()

        @pl.when(takes)
        def _():
            over_y(slot, terms[slot] + other[slot])

        return carry

    lax.fori_loop(0, 4, step, 0)

    for r in range(2):
        res_out[r] = restored([res_acc[r, rb] for rb in range(2)], perm_ref)

    def entry_at(j):
        later = (j + 4) // 5
        return 4 * (1 - later) + later * first_order(j - later)

    def send_home(j, carry):
        homeward(entry_at(j))
        return carry

    @pl.when(core == 1)
    def _():
        lax.fori_loop(0, 5, send_home, 0)

    def from_home(at):
        return (
            remote(hcode.at[0, 0], hget.at[at], h_send.at[0, 0], h_recv.at[at], partner),
            remote(hscale.at[0, pl.ds(0, 1)], hgets.at[at, pl.ds(0, 1)], hs_send.at[0, 0], hs_recv.at[at], partner),
        )

    def take(at):
        for rb, part in enumerate(widened(hget.at[at], hgets[at, pl.ds(0, 1)])):
            total[rb] += part

    total[...] = jnp.zeros_like(total)
    for at in range(2, 6):
        for copy in from_home(at):
            copy.wait_recv()
        take(at)

    @pl.when(core == 0)
    def _():
        for at in range(2):
            for copy in from_home(at):
                copy.wait_recv()
            take(at)

    trav_out[...] = restored([total[rb] for rb in range(2)], perm_ref).reshape(2, 4, 1024)

    for near in range(2):
        hops[near].wait_send()
    for d in range(1, 4):
        for copy in y_copies(4 * core, d):
            copy.wait_send()

    @pl.when(core == 0)
    def _():
        to_partner(4, mine).wait_send()
        for e in range(4):
            for d in range(4):
                if e == 0 and d > 0:
                    continue
                for copy in y_copies(e, d):
                    copy.wait_send()

    @pl.when(core == 1)
    def _():
        for slot in range(4):
            for d in range(1, 4):
                forward(slot, d).wait_send()
            to_partner(slot, mine).wait_send()
            if slot:
                to_other(slot).wait_send()
        for e in range(5):
            for copy in h_copies(e):
                copy.wait_send()


def store(res_ref, trav_ref, res_out, trav_out, sem):
    copies = [
        pltpu.make_async_copy(res_ref, res_out, sem.at[0]),
        pltpu.make_async_copy(trav_ref, trav_out, sem.at[1]),
    ]
    for copy in copies:
        copy.start()
    for copy in copies:
        copy.wait()


def local(residents, travellers, pair_list):
    consts = tables(32)
    hbm = pl.BlockSpec(memory_space=pltpu.HBM)
    vmem = pl.BlockSpec(memory_space=pltpu.VMEM)
    dma = pltpu.SemaphoreType.DMA
    done = pl.pallas_call(
        kernel,
        out_shape=(pltpu.VMEM((2, 32, 1024), F32), pltpu.VMEM((2, 4, 1024), F32)),
        in_specs=[hbm] * 7,
        out_specs=(vmem, vmem),
        scratch_shapes=[
            pltpu.VMEM((2, 32, 1024), BF16),
            pltpu.VMEM((2, 32, 1024), BF16),
            pltpu.SMEM((1, 3, 2, 4), jnp.int32),
            pltpu.VMEM((4, 256, 256), BF16),
            pltpu.VMEM((2, 4, 2, 256, 256), BF16),
            pltpu.VMEM((64, 256), BF16),
            pltpu.VMEM((4, 32, 256), F32),
            dma((7,)),
            pltpu.VMEM((4, 2, 16, 512), BF16),
            pltpu.VMEM((5, 4, 2, 16, 512), BF16),
            pltpu.VMEM((2, 2, 32, 512), F32),
            pltpu.VMEM((2, 2, 32, 512), F32),
            pltpu.VMEM((5, 4, 2, 2, 8, 512), F32),
            pltpu.VMEM((5, 4, 2, 2, 8, 512), F32),
            pltpu.VMEM((5, 4, 2, 16, 512), I16),
            pltpu.VMEM((5, 8, 128), F32),
            pltpu.VMEM((5, 4, 2, 16, 512), I16),
            pltpu.VMEM((5, 4, 8, 128), F32),
            pltpu.VMEM((5, 2, 16, 512), I16),
            pltpu.VMEM((5, 8, 128), F32),
            pltpu.VMEM((6, 16, 512), I16),
            pltpu.VMEM((6, 8, 128), F32),
            pltpu.VMEM((2, 8, 512), F32),
            dma((2,)),
            dma((4, 3)),
            dma((4, 4)),
            dma((5,)),
            dma((5,)),
            dma((4,)),
            dma((4,)),
            dma((5, 4)),
            dma((5, 4)),
            dma((5, 4)),
            dma((5, 4)),
            dma((5, 2)),
            dma((5, 2)),
            dma((6,)),
            dma((6,)),
        ],
        compiler_params=pltpu.CompilerParams(
            collective_id=0, has_side_effects=True
        ),
    )(residents, travellers, pair_list.transpose(0, 3, 2, 1), *[jnp.asarray(c) for c in consts])
    return pl.pallas_call(
        store,
        out_shape=(
            jax.ShapeDtypeStruct((2, 32, 1024), F32),
            jax.ShapeDtypeStruct((2, 4, 1024), F32),
        ),
        in_specs=[vmem] * 2,
        out_specs=(hbm, hbm),
        scratch_shapes=[dma((2,))],
        compiler_params=pltpu.CompilerParams(vmem_limit_bytes=2**20),
    )(*done)


def solution(mesh):
    return jax.shard_map(
        local,
        mesh=mesh,
        in_specs=(
            P(("blk", "grp"), None, None),
            P("blk", None, None),
            P(("blk", "grp"), None, None, None),
        ),
        out_specs=(P(("blk", "grp"), None, None), P("blk", "grp", None)),
        check_vma=False,
    )
```

```python
import functools

import jax
import jax.numpy as jnp
import numpy as np
from jax import lax
from jax.experimental import pallas as pl
from jax.experimental.pallas import tpu as pltpu
from jax.sharding import PartitionSpec as P

MESH = pl.DeviceIdType.MESH
F32, BF16, I16 = jnp.float32, jnp.bfloat16, jnp.int16
TOP = 32767.0


def tables(edge):
    half = edge // 2
    index = np.arange(edge, dtype=np.float64) + 1.0
    sine = np.sqrt(2.0 / (edge + 1)) * np.sin(np.pi * np.outer(index, index) / (edge + 1))
    eigen = 2.0 - 2.0 * np.cos(np.pi * index / (edge + 1))
    perm = np.zeros((2, 256, 256))
    for b8 in range(8):
        for c in range(edge):
            rc, cc = (0, c) if c < half else (1, edge - 1 - c)
            perm[0, b8 * edge + c, rc * 128 + b8 * half + cc] = 1.0
            perm[1, b8 * edge + c, rc * 128 + (7 - b8) * half + cc] = 1.0
    perms = np.concatenate([perm, perm.transpose(0, 2, 1)])
    planes, scales = [], []
    for pb in range(2):
        for pc in range(2):
            planes.append(np.kron(sine[pb::2, :half].T, sine[pc::2, :half].T))
            scales.append(
                1.0
                / (
                    eigen[:, None, None]
                    + eigen[None, pb::2, None]
                    + eigen[None, None, pc::2]
                ).reshape(edge, half * half)
            )
    planes = np.stack(planes)
    both = np.stack([planes, planes.transpose(0, 2, 1)]).astype(np.float32)
    high = both.astype(jnp.bfloat16)
    low = (both - high.astype(np.float32)).astype(jnp.bfloat16)
    weights = np.stack([high, low], axis=2)
    small = np.kron(np.eye(4), sine).astype(np.float32)
    small_high = small.astype(jnp.bfloat16)
    small_low = (small - small_high.astype(np.float32)).astype(jnp.bfloat16)
    rows = np.concatenate([small_high, small_high, small_low], axis=1)
    return (
        perms.astype(jnp.bfloat16),
        weights,
        rows,
        np.stack(scales).astype(np.float32),
    )


def dot(a, b):
    return jnp.dot(a, b, preferred_element_type=F32)


def split(x):
    high = x.astype(BF16)
    return high, (x - high.astype(F32)).astype(BF16)


def permuted(x, perm_ref):
    halves = []
    for rb in range(2):
        parts = [[None, None], [None, None]]
        for n in range(2):
            m = n if rb == 0 else 3 - n
            y = dot(x[:, m * 256 : (m + 1) * 256], perm_ref[rb])
            parts[0][n], parts[1][n] = y[:, :128], y[:, 128:]
        halves.append(jnp.concatenate(parts[0] + parts[1], axis=1))
    return halves


def restored(halves, perm_ref):
    rows = halves[0].shape[0]
    groups = [None] * 4
    for rb in range(2):
        for n in range(2):
            m = n if rb == 0 else 3 - n
            x = jnp.concatenate(
                [
                    halves[rb][:, n * 128 : (n + 1) * 128],
                    halves[rb][:, 256 + n * 128 : 256 + (n + 1) * 128],
                ],
                axis=1,
            )
            y = dot(jnp.concatenate(split(x), axis=0), perm_ref[2 + rb])
            groups[m] = y[:rows] + y[rows:]
    return jnp.concatenate(groups, axis=1)


def plane(g, weight_ref, way):
    out = []
    for p in range(4):
        high, low = split(g[p])
        rows = high.shape[0]
        a = dot(jnp.concatenate([high, low], axis=0), weight_ref[way, p, 0])
        out.append(a[:rows] + a[rows:] + dot(high, weight_ref[way, p, 1]))
    return out


def along_rows(g, rows):
    out = []
    for p in range(4):
        high, low = split(g[p])
        out.append(dot(rows, jnp.concatenate([high, low, high], axis=0)))
    return out


def peak(tiles):
    tiles = [jnp.abs(t) for t in tiles]
    while len(tiles) > 1:
        tiles = [
            jnp.maximum(tiles[i], tiles[i + 1]) if i + 1 < len(tiles) else tiles[i]
            for i in range(0, len(tiles), 2)
        ]
    return jnp.maximum(tiles[0], 1e-30)


def lane_tiles(x):
    return [x[:, j * 128 : (j + 1) * 128] for j in range(x.shape[1] // 128)]


def coded(x, wide):
    return jnp.round(x * wide).astype(jnp.int32)


def spread(tile, times):
    return jnp.concatenate([tile] * times, axis=1)


def kernel(
    res_hbm,
    trav_hbm,
    pair_hbm,
    perm_hbm,
    weight_hbm,
    rows_hbm,
    scale_hbm,
    res_out,
    trav_out,
    res_in,
    trav_in,
    pair_ref,
    perm_ref,
    weight_ref,
    rows_ref,
    scale_ref,
    load_sem,
    mine,
    tbuf,
    ubuf,
    res_acc,
    terms,
    other,
    ycode,
    yscale,
    yget,
    ygets,
    hcode,
    hscale,
    hget,
    hgets,
    total,
    z_send,
    f_send,
    t_recv,
    x_send,
    x_recv,
    c_send,
    c_recv,
    y_send,
    ys_send,
    y_recv,
    ys_recv,
    h_send,
    hs_send,
    h_recv,
    hs_recv,
):
    n_blk = lax.axis_size("blk")
    blk, grp = lax.axis_index("blk"), lax.axis_index("grp")
    core = lax.rem(blk, 2)
    first = blk - core
    y, lo = grp // 2, lax.rem(grp, 2)
    partner = (first + 1 - core, grp)
    across_z = y * 2 + 1 - lo

    def around(b):
        return lax.rem(b + n_blk, n_blk)

    def y_peer(d):
        return lax.rem(y + d, 4)

    def remote(src, dst, send, recv, to):
        return pltpu.make_async_remote_copy(
            src_ref=src, dst_ref=dst, send_sem=send, recv_sem=recv, device_id=to, device_id_type=MESH
        )

    loads = [
        pltpu.make_async_copy(src, dst, load_sem.at[j])
        for j, (src, dst) in enumerate(
            (
                (trav_hbm, trav_in),
                (perm_hbm, perm_ref),
                (res_hbm, res_in),
                (pair_hbm, pair_ref),
                (rows_hbm, rows_ref),
                (scale_hbm, scale_ref),
                (weight_hbm, weight_ref),
            )
        )
    ]
    for load in loads:
        load.start()

    barrier = pltpu.get_barrier_semaphore()

    def arrive(to):
        pl.semaphore_signal(barrier, inc=1, device_id=to, device_id_type=MESH)

    arrive(partner)
    arrive((blk, across_z))

    @pl.when(core == 1)
    def _():
        for c in range(2):
            arrive((around(first - 4 + c), across_z))
            arrive((around(first - 2 + c), grp))
            for d in range(1, 4):
                arrive((first + c, y_peer(d) * 2 + lo))

    loads[0].wait()
    loads[1].wait()
    own = [h.reshape(2, 4, 8, 512) for h in permuted(trav_in[...].reshape(64, 1024), perm_ref)]
    for q in range(4):
        for t in range(2):
            mine[q, t] = jnp.concatenate([own[0][t, q], own[1][t, q]], axis=0).astype(BF16)

    pl.semaphore_wait(barrier, 7)

    far = remote(mine.at[y], tbuf.at[core, y], z_send.at[0], t_recv.at[core, y], (around(first + 5), across_z))
    far.start()

    def near(c):
        src = mine.at[y] if c else tbuf.at[4, y]
        return remote(src, tbuf.at[2 + c, y], z_send.at[1 + c], t_recv.at[2 + c, y], (around(first + 3), grp))

    def to_partner(slot, src):
        return remote(src, tbuf.at[slot], x_send.at[slot], x_recv.at[slot], partner)

    @pl.when(core == 0)
    def _():
        to_partner(4, mine).start()

    loads[2].wait()
    for rb, h in enumerate(permuted(res_in[...].reshape(64, 1024), perm_ref)):
        for r in range(2):
            ubuf[r, rb] = h[r * 32 : (r + 1) * 32]
    res_acc[...] = jnp.zeros_like(res_acc)

    other[0] = jnp.zeros((4, 2, 2, 8, 512), F32)

    def quarter(slot, q):
        return remote(mine.at[q], tbuf.at[slot, q], z_send.at[0], t_recv.at[slot, q], partner)

    def forward(slot, d):
        return remote(
            tbuf.at[slot, y],
            tbuf.at[slot, y],
            f_send.at[slot, d - 1],
            t_recv.at[slot, y],
            (blk, y_peer(d) * 2 + lo),
        )

    for load in loads[3:]:
        load.wait()

    def to_other(slot):
        return remote(terms.at[slot], other.at[slot], c_send.at[slot], c_recv.at[slot], partner)

    def y_copies(e, d):
        to = (first + 1, y_peer(d) * 2 + lo)
        return (
            remote(ycode.at[e, y_peer(d)], yget.at[e, d], y_send.at[e, d], y_recv.at[e, d], to),
            remote(
                yscale.at[e, pl.ds(0, 1)],
                ygets.at[e, d, pl.ds(0, 1)],
                ys_send.at[e, d],
                ys_recv.at[e, d],
                to,
            ),
        )

    def h_copies(e):
        at = (5 - e) // 2 * 2 + lo
        copies = []
        for z in range(2):
            to = (around(first - 4 + e), y * 2 + z)
            copies += [
                remote(hcode.at[e, z], hget.at[at], h_send.at[e, z], h_recv.at[at], to),
                remote(hscale.at[e, pl.ds(0, 1)], hgets.at[at, pl.ds(0, 1)], hs_send.at[e, z], hs_recv.at[at], to),
            ]
        return copies

    def solve(slots):
        u, w, factors = [], [], []
        for slot in slots:
            s = lax.rem(3 - slot + core, 4)
            both = []
            for t in range(2):
                wide = tbuf[slot, :, t].astype(F32).reshape(4, 2, 8, 512)
                both.append([wide[:, rb].reshape(32, 512) for rb in range(2)])
            for p in range(2):
                r, t, active = (pair_ref[0, e, p, s] for e in range(3))
                u.append([ubuf[r, rb] for rb in range(2)])
                w.append([jnp.where(t == 1, both[1][rb], both[0][rb]) for rb in range(2)])
                factors.append([[jnp.where(e == j, active, 0).astype(F32) for j in range(2)] for e in (r, t)])
        d = [jnp.concatenate([u[f][rb] * w[f][rb] for f in range(4)], axis=0) for rb in range(2)]
        g = []
        for e in (d[0] + d[1], d[0] - d[1]):
            g += [e[:, :256] + e[:, 256:], e[:, :256] - e[:, 256:]]
        rows = rows_ref[...]
        g = along_rows(plane(g, weight_ref, 0), rows)
        g = [
            (m.reshape(4, 32, 256) * scale_ref[p][None]).reshape(128, 256)
            for p, m in enumerate(g)
        ]
        g = plane(along_rows(g, rows), weight_ref, 1)
        pot = []
        for e, o in (
            (g[0] + g[2], g[1] + g[3]),
            (g[0] - g[2], g[1] - g[3]),
        ):
            pot.append(jnp.concatenate([e + o, e - o], axis=1))
        for rb in range(2):
            v = [pot[rb][f * 32 : (f + 1) * 32] for f in range(4)]
            vw = [v[f] * w[f][rb] for f in range(4)]
            vu = [v[f] * u[f][rb] for f in range(4)]
            for j in range(2):
                ours = [vw[f] * factors[f][0][j] for f in range(4)]
                res_acc[j, rb] += (ours[0] + ours[1]) + (ours[2] + ours[3])
                for k, slot in enumerate(slots):
                    f = 2 * k
                    theirs = vu[f] * factors[f][1][j] + vu[f + 1] * factors[f + 1][1][j]
                    terms[slot, :, j, rb] = theirs.reshape(4, 8, 512)

    def one_row(tiles):
        top = jnp.max(peak(tiles), axis=0, keepdims=True)
        return top, jnp.broadcast_to(TOP / top, (8, 128))

    def over_y(e, value):
        parts = [(q, t, rb) for q in range(4) for t in range(2) for rb in range(2)]
        top, wide = one_row([x for at in parts for x in lane_tiles(value[at])])
        yscale[e, pl.ds(0, 1)] = top * (1.0 / TOP)
        wide = spread(wide, 4)
        for q in range(4):
            for t in range(2):
                ycode[e, q, t] = jnp.concatenate([coded(value[q, t, rb], wide) for rb in range(2)], axis=0).astype(I16)
        for d in range(1, 4):
            for copy in y_copies(e, d):
                copy.start()

        @pl.when(core == 0)
        def _():
            for copy in y_copies(e, 0):
                copy.start()

        @pl.when(core == 1)
        def _():
            yget[4, 0] = ycode[4, y]
            ygets[4, 0, pl.ds(0, 1)] = yscale[4, pl.ds(0, 1)]

    def widened(code_ref, scale_row):
        code = code_ref[...].astype(jnp.int32).astype(F32)
        scale = spread(jnp.broadcast_to(scale_row, (8, 128)), 4)
        return [code[rb * 8 : (rb + 1) * 8] * scale for rb in range(2)]

    def homeward(e):
        @pl.when(e < 4)
        def _():
            for copy in y_copies(e, 0):
                copy.wait_recv()

        sums = [widened(yget.at[e, 0, t], ygets[e, 0, pl.ds(0, 1)]) for t in range(2)]
        for d in range(1, 4):
            for copy in y_copies(e, d):
                copy.wait_recv()
            for t in range(2):
                for rb, part in enumerate(widened(yget.at[e, d, t], ygets[e, d, pl.ds(0, 1)])):
                    sums[t][rb] += part
        upper = lax.broadcasted_iota(jnp.int32, (8, 512), 0) < 4
        rows = [
            [jnp.where(upper, sums[0][rb], pltpu.roll(sums[1][rb], 4, 0)) for rb in range(2)],
            [jnp.where(upper, pltpu.roll(sums[0][rb], 4, 0), sums[1][rb]) for rb in range(2)],
        ]
        top, wide = one_row([x for z in range(2) for rb in range(2) for x in lane_tiles(rows[z][rb])])
        hscale[e, pl.ds(0, 1)] = top * (1.0 / TOP)
        wide = spread(wide, 4)
        for z in range(2):
            hcode[e, z] = jnp.concatenate([coded(rows[z][rb], wide) for rb in range(2)], axis=0).astype(I16)
        for copy in h_copies(e):
            copy.start()

    def relay(slot):
        quarter(slot, y).wait_recv()
        for d in range(1, 4):
            forward(slot, d).start()

    def spread_slot(slot):
        for d in range(1, 4):
            quarter(slot, y_peer(d)).wait_recv()
        to_partner(slot, tbuf.at[slot]).start()

    def step(i, carry):
        @pl.when(jnp.logical_and(core == 1, i == 0))
        def _():
            to_partner(4, mine).wait_recv()
            for c in range(2):
                near(c).start()
            relay(1)
            relay(0)
            spread_slot(1)
            relay(3)
            relay(2)
            spread_slot(0)

        @pl.when(jnp.logical_and(core == 1, i == 1))
        def _():
            spread_slot(2)
            spread_slot(3)

        @pl.when(core == 0)
        def _():
            for k in range(2):
                to_partner(2 * i + k, mine).wait_recv()

        solve((i * 2 + (1 - i) * (1 + 3 * core), i * 3 + (1 - i) * core))

        @pl.when(core == 0)
        def _():
            def combine(k, inner):
                slot = 2 * i + k

                @pl.when(slot > 0)
                def _():
                    to_other(slot).wait_recv()

                over_y(slot, terms[slot] + other[slot])
                return inner

            lax.fori_loop(0, 2, combine, 0)

        @pl.when(jnp.logical_and(core == 1, i == 0))
        def _():
            to_other(1).start()
            over_y(4, terms[4])

        @pl.when(jnp.logical_and(core == 1, i == 1))
        def _():
            to_other(2).start()
            to_other(3).start()

        return carry

    lax.fori_loop(0, 2, step, 0)

    for r in range(2):
        res_out[r] = restored([res_acc[r, rb] for rb in range(2)], perm_ref)

    def send_home(j, carry):
        homeward(lax.rem(j + 4, 5))
        return carry

    @pl.when(core == 1)
    def _():
        lax.fori_loop(0, 5, send_home, 0)

    def from_home(at):
        return (
            remote(hcode.at[0, 0], hget.at[at], h_send.at[0, 0], h_recv.at[at], partner),
            remote(hscale.at[0, pl.ds(0, 1)], hgets.at[at, pl.ds(0, 1)], hs_send.at[0, 0], hs_recv.at[at], partner),
        )

    def take(at):
        for rb, part in enumerate(widened(hget.at[at], hgets[at, pl.ds(0, 1)])):
            total[rb] += part

    total[...] = jnp.zeros_like(total)
    for at in range(2, 6):
        for copy in from_home(at):
            copy.wait_recv()
        take(at)

    @pl.when(core == 0)
    def _():
        for at in range(2):
            for copy in from_home(at):
                copy.wait_recv()
            take(at)

    trav_out[...] = restored([total[rb] for rb in range(2)], perm_ref).reshape(2, 4, 1024)

    far.wait_send()
    for d in range(1, 4):
        for copy in y_copies(4 * core, d):
            copy.wait_send()

    @pl.when(core == 0)
    def _():
        to_partner(4, mine).wait_send()
        for e in range(4):
            for d in range(4):
                if e == 0 and d > 0:
                    continue
                for copy in y_copies(e, d):
                    copy.wait_send()

    @pl.when(core == 1)
    def _():
        for c in range(2):
            near(c).wait_send()
        for slot in range(4):
            for d in range(1, 4):
                forward(slot, d).wait_send()
            to_partner(slot, mine).wait_send()
            if slot:
                to_other(slot).wait_send()
        for e in range(5):
            for copy in h_copies(e):
                copy.wait_send()


def store(res_ref, trav_ref, res_out, trav_out, sem):
    copies = [
        pltpu.make_async_copy(res_ref, res_out, sem.at[0]),
        pltpu.make_async_copy(trav_ref, trav_out, sem.at[1]),
    ]
    for copy in copies:
        copy.start()
    for copy in copies:
        copy.wait()


def local(residents, travellers, pair_list):
    consts = tables(32)
    hbm = pl.BlockSpec(memory_space=pltpu.HBM)
    vmem = pl.BlockSpec(memory_space=pltpu.VMEM)
    dma = pltpu.SemaphoreType.DMA
    done = pl.pallas_call(
        kernel,
        out_shape=(pltpu.VMEM((2, 32, 1024), F32), pltpu.VMEM((2, 4, 1024), F32)),
        in_specs=[hbm] * 7,
        out_specs=(vmem, vmem),
        scratch_shapes=[
            pltpu.VMEM((2, 32, 1024), BF16),
            pltpu.VMEM((2, 32, 1024), BF16),
            pltpu.SMEM((1, 3, 2, 4), jnp.int32),
            pltpu.VMEM((4, 256, 256), BF16),
            pltpu.VMEM((2, 4, 2, 256, 256), BF16),
            pltpu.VMEM((128, 384), BF16),
            pltpu.VMEM((4, 32, 256), F32),
            dma((7,)),
            pltpu.VMEM((4, 2, 16, 512), BF16),
            pltpu.VMEM((5, 4, 2, 16, 512), BF16),
            pltpu.VMEM((2, 2, 32, 512), F32),
            pltpu.VMEM((2, 2, 32, 512), F32),
            pltpu.VMEM((5, 4, 2, 2, 8, 512), F32),
            pltpu.VMEM((5, 4, 2, 2, 8, 512), F32),
            pltpu.VMEM((5, 4, 2, 16, 512), I16),
            pltpu.VMEM((5, 8, 128), F32),
            pltpu.VMEM((5, 4, 2, 16, 512), I16),
            pltpu.VMEM((5, 4, 8, 128), F32),
            pltpu.VMEM((5, 2, 16, 512), I16),
            pltpu.VMEM((5, 8, 128), F32),
            pltpu.VMEM((6, 16, 512), I16),
            pltpu.VMEM((6, 8, 128), F32),
            pltpu.VMEM((2, 8, 512), F32),
            dma((3,)),
            dma((4, 3)),
            dma((4, 4)),
            dma((5,)),
            dma((5,)),
            dma((4,)),
            dma((4,)),
            dma((5, 4)),
            dma((5, 4)),
            dma((5, 4)),
            dma((5, 4)),
            dma((5, 2)),
            dma((5, 2)),
            dma((6,)),
            dma((6,)),
        ],
        compiler_params=pltpu.CompilerParams(
            collective_id=0, has_side_effects=True
        ),
    )(residents, travellers, pair_list.transpose(0, 3, 2, 1), *[jnp.asarray(c) for c in consts])
    return pl.pallas_call(
        store,
        out_shape=(
            jax.ShapeDtypeStruct((2, 32, 1024), F32),
            jax.ShapeDtypeStruct((2, 4, 1024), F32),
        ),
        in_specs=[vmem] * 2,
        out_specs=(hbm, hbm),
        scratch_shapes=[dma((2,))],
        compiler_params=pltpu.CompilerParams(vmem_limit_bytes=2**20),
    )(*done)


def solution(mesh):
    return jax.shard_map(
        local,
        mesh=mesh,
        in_specs=(
            P(("blk", "grp"), None, None),
            P("blk", None, None),
            P(("blk", "grp"), None, None, None),
        ),
        out_specs=(P(("blk", "grp"), None, None), P("blk", "grp", None)),
        check_vma=False,
    )
```

```python
import functools

import jax
import jax.numpy as jnp
import numpy as np
from jax import lax
from jax.experimental import pallas as pl
from jax.experimental.pallas import tpu as pltpu
from jax.sharding import PartitionSpec as P

MESH = pl.DeviceIdType.MESH
F32, BF16, I16 = jnp.float32, jnp.bfloat16, jnp.int16
TOP = 32767.0


def tables(edge):
    half = edge // 2
    index = np.arange(edge, dtype=np.float64) + 1.0
    sine = np.sqrt(2.0 / (edge + 1)) * np.sin(np.pi * np.outer(index, index) / (edge + 1))
    eigen = 2.0 - 2.0 * np.cos(np.pi * index / (edge + 1))
    perm = np.zeros((2, 256, 256))
    for b8 in range(8):
        for c in range(edge):
            rc, cc = (0, c) if c < half else (1, edge - 1 - c)
            perm[0, b8 * edge + c, rc * 128 + b8 * half + cc] = 1.0
            perm[1, b8 * edge + c, rc * 128 + (7 - b8) * half + cc] = 1.0
    perms = np.concatenate([perm, perm.transpose(0, 2, 1)])
    planes, scales = [], []
    for pb in range(2):
        for pc in range(2):
            planes.append(np.kron(sine[pb::2, :half].T, sine[pc::2, :half].T))
            scales.append(
                1.0
                / (
                    eigen[:, None, None]
                    + eigen[None, pb::2, None]
                    + eigen[None, None, pc::2]
                ).reshape(edge, half * half)
            )
    planes = np.stack(planes)
    both = np.stack([planes, planes.transpose(0, 2, 1)]).astype(np.float32)
    high = both.astype(jnp.bfloat16)
    low = (both - high.astype(np.float32)).astype(jnp.bfloat16)
    weights = np.stack([high, low], axis=2)
    small = np.kron(np.eye(4), sine).astype(np.float32)
    small_high = small.astype(jnp.bfloat16)
    small_low = (small - small_high.astype(np.float32)).astype(jnp.bfloat16)
    rows = np.concatenate([np.concatenate([small_high, small_low], axis=1), np.zeros((128, 256), jnp.bfloat16)])
    return (
        perms.astype(jnp.bfloat16),
        np.concatenate([weights.reshape(16, 256, 256), rows[None]]),
        np.stack(scales).astype(np.float32),
    )


def dot(a, b):
    return jnp.dot(a, b, preferred_element_type=F32)


def split(x):
    high = x.astype(BF16)
    return high, (x - high.astype(F32)).astype(BF16)


def permuted(x, perm_ref):
    halves = []
    for rb in range(2):
        parts = [[None, None], [None, None]]
        for n in range(2):
            m = n if rb == 0 else 3 - n
            y = dot(x[:, m * 256 : (m + 1) * 256], perm_ref[rb])
            parts[0][n], parts[1][n] = y[:, :128], y[:, 128:]
        halves.append(jnp.concatenate(parts[0] + parts[1], axis=1))
    return halves


def restored(halves, perm_ref):
    rows = halves[0].shape[0]
    groups = [None] * 4
    for rb in range(2):
        for n in range(2):
            m = n if rb == 0 else 3 - n
            x = jnp.concatenate(
                [
                    halves[rb][:, n * 128 : (n + 1) * 128],
                    halves[rb][:, 256 + n * 128 : 256 + (n + 1) * 128],
                ],
                axis=1,
            )
            y = dot(jnp.concatenate(split(x), axis=0), perm_ref[2 + rb])
            groups[m] = y[:rows] + y[rows:]
    return jnp.concatenate(groups, axis=1)


def plane(g, weight_ref, way):
    out = []
    for p in range(4):
        high, low = split(g[p])
        rows = high.shape[0]
        a = dot(jnp.concatenate([high, low], axis=0), weight_ref[way * 8 + p * 2])
        out.append(a[:rows] + a[rows:] + dot(high, weight_ref[way * 8 + p * 2 + 1]))
    return out


def along_rows(g, rows):
    out = []
    for p in range(4):
        high, low = split(g[p])
        out.append(dot(rows, jnp.concatenate([high, low, high], axis=0)))
    return out


def peak(tiles):
    tiles = [jnp.abs(t) for t in tiles]
    while len(tiles) > 1:
        tiles = [
            jnp.maximum(tiles[i], tiles[i + 1]) if i + 1 < len(tiles) else tiles[i]
            for i in range(0, len(tiles), 2)
        ]
    return jnp.maximum(tiles[0], 1e-30)


def lane_tiles(x):
    return [x[:, j * 128 : (j + 1) * 128] for j in range(x.shape[1] // 128)]


def coded(x, wide):
    return jnp.round(x * wide).astype(jnp.int32)


def spread(tile, times):
    return jnp.concatenate([tile] * times, axis=1)


def kernel(
    res_hbm,
    trav_hbm,
    pair_hbm,
    perm_hbm,
    weight_hbm,
    scale_hbm,
    res_out,
    trav_out,
    res_in,
    trav_in,
    pair_ref,
    perm_ref,
    weight_ref,
    scale_ref,
    load_sem,
    mine,
    tbuf,
    ubuf,
    res_acc,
    terms,
    other,
    ycode,
    yscale,
    ysent,
    yget,
    ygets,
    hcode,
    hscale,
    hget,
    hgets,
    total,
    z_send,
    z_recv,
    f_send,
    f_recv,
    x_send,
    x_recv,
    c_send,
    c_recv,
    y_send,
    ys_send,
    y_recv,
    ys_recv,
    h_send,
    hs_send,
    h_recv,
    hs_recv,
):
    n_blk = lax.axis_size("blk")
    blk, grp = lax.axis_index("blk"), lax.axis_index("grp")
    core = lax.rem(blk, 2)
    first = blk - core
    y, lo = grp // 2, lax.rem(grp, 2)
    partner = (first + 1 - core, grp)
    across_z = y * 2 + 1 - lo

    def around(b):
        return lax.rem(b + n_blk, n_blk)

    def y_peer(d):
        return lax.rem(y + d, 4)

    def remote(src, dst, send, recv, to):
        return pltpu.make_async_remote_copy(
            src_ref=src, dst_ref=dst, send_sem=send, recv_sem=recv, device_id=to, device_id_type=MESH
        )

    def came(ref, sem):
        remote(ref, ref, sem, sem, partner).wait_recv()

    def left(ref, sem):
        remote(ref, ref, sem, sem, partner).wait_send()

    loads = [
        pltpu.make_async_copy(src, dst, load_sem.at[j])
        for j, (src, dst) in enumerate(
            (
                (trav_hbm, trav_in),
                (perm_hbm, perm_ref),
                (res_hbm, res_in),
                (pair_hbm, pair_ref),
                (scale_hbm, scale_ref),
                (weight_hbm, weight_ref),
            )
        )
    ]
    for load in loads:
        load.start()

    barrier = pltpu.get_barrier_semaphore()

    def arrive(to):
        pl.semaphore_signal(barrier, inc=1, device_id=to, device_id_type=MESH)

    arrive(partner)
    arrive((blk, across_z))

    @pl.when(core == 1)
    def _():
        for c in range(2):
            arrive((around(first - 4 + c), across_z))
            arrive((around(first - 2 + c), grp))
            for d in range(1, 4):
                arrive((first + c, y_peer(d) * 2 + lo))

    loads[0].wait()
    loads[1].wait()
    own = [h.reshape(2, 4, 8, 512) for h in permuted(trav_in[...].reshape(64, 1024), perm_ref)]
    for q in range(4):
        for t in range(2):
            mine[q, t] = jnp.concatenate([own[0][t, q], own[1][t, q]], axis=0).astype(BF16)

    pl.semaphore_wait(barrier, 7)

    far = remote(mine.at[y], tbuf.at[core, y], z_send, z_recv.at[core], (around(first + 5), across_z))
    far.start()

    def near(c):
        src = mine.at[y] if c else tbuf.at[4, y]
        return remote(src, tbuf.at[2 + c, y], z_send, z_recv.at[2 + c], (around(first + 3), grp))

    def to_partner(slot, src):
        return remote(src, tbuf.at[slot], x_send, x_recv.at[slot // 2 % 2], partner)

    @pl.when(core == 0)
    def _():
        to_partner(4, mine).start()

    loads[2].wait()
    for rb, h in enumerate(permuted(res_in[...].reshape(64, 1024), perm_ref)):
        for r in range(2):
            ubuf[r, rb] = h[r * 32 : (r + 1) * 32]
    res_acc[...] = jnp.zeros_like(res_acc)

    other[0] = jnp.zeros((4, 2, 2, 8, 512), F32)

    def forward(slot, d):
        return remote(
            tbuf.at[slot, y],
            tbuf.at[slot, y],
            f_send,
            f_recv.at[slot],
            (blk, y_peer(d) * 2 + lo),
        )

    for load in loads[3:]:
        load.wait()

    def to_other(slot):
        return remote(terms.at[slot], other.at[slot], c_send, c_recv.at[slot // 2], partner)

    def y_copies(e, d):
        to = (first + 1, y_peer(d) * 2 + lo)
        return (
            remote(ycode.at[e, y_peer(d)], yget.at[e, d], y_send, y_recv.at[e], to),
            remote(yscale.at[pl.ds(e, 1)], ygets.at[e, pl.ds(d, 1)], ys_send, ys_recv.at[e], to),
        )

    def h_copies(e):
        at = (5 - e) // 2 * 2 + lo
        copies = []
        for z in range(2):
            to = (around(first - 4 + e), y * 2 + z)
            copies += [
                remote(hcode.at[e, z], hget.at[at], h_send, h_recv, to),
                remote(hscale.at[pl.ds(e, 1)], hgets.at[pl.ds(at, 1)], hs_send, hs_recv, to),
            ]
        return copies

    def solve(slots):
        u, w, factors = [], [], []
        for slot in slots:
            s = lax.rem(3 - slot + core, 4)
            both = []
            for t in range(2):
                wide = tbuf[slot, :, t].astype(F32).reshape(4, 2, 8, 512)
                both.append([wide[:, rb].reshape(32, 512) for rb in range(2)])
            for p in range(2):
                r, t, active = (pair_ref[0, e, p, s] for e in range(3))
                u.append([ubuf[r, rb] for rb in range(2)])
                w.append([jnp.where(t == 1, both[1][rb], both[0][rb]) for rb in range(2)])
                factors.append([[jnp.where(e == j, active, 0).astype(F32) for j in range(2)] for e in (r, t)])
        d = [jnp.concatenate([u[f][rb] * w[f][rb] for f in range(4)], axis=0) for rb in range(2)]
        g = []
        for e in (d[0] + d[1], d[0] - d[1]):
            g += [e[:, :256] + e[:, 256:], e[:, :256] - e[:, 256:]]
        high, low = weight_ref[16, :128, :128], weight_ref[16, :128, 128:]
        rows = jnp.concatenate([high, high, low], axis=1)
        g = along_rows(plane(g, weight_ref, 0), rows)
        g = [
            (m.reshape(4, 32, 256) * scale_ref[p][None]).reshape(128, 256)
            for p, m in enumerate(g)
        ]
        g = plane(along_rows(g, rows), weight_ref, 1)
        pot = []
        for e, o in (
            (g[0] + g[2], g[1] + g[3]),
            (g[0] - g[2], g[1] - g[3]),
        ):
            pot.append(jnp.concatenate([e + o, e - o], axis=1))
        for rb in range(2):
            v = [pot[rb][f * 32 : (f + 1) * 32] for f in range(4)]
            vw = [v[f] * w[f][rb] for f in range(4)]
            vu = [v[f] * u[f][rb] for f in range(4)]
            for j in range(2):
                ours = [vw[f] * factors[f][0][j] for f in range(4)]
                res_acc[j, rb] += (ours[0] + ours[1]) + (ours[2] + ours[3])
                for k, slot in enumerate(slots):
                    f = 2 * k
                    theirs = vu[f] * factors[f][1][j] + vu[f + 1] * factors[f + 1][1][j]
                    terms[slot, :, j, rb] = theirs.reshape(4, 8, 512)

    def one_row(tiles):
        top = jnp.max(peak(tiles), axis=0, keepdims=True)
        return top, jnp.broadcast_to(TOP / top, (8, 128))

    def over_y(e, value):
        parts = [(q, t, rb) for q in range(4) for t in range(2) for rb in range(2)]
        top, wide = one_row([x for at in parts for x in lane_tiles(value[at])])
        yscale[pl.ds(e, 1)] = top * (1.0 / TOP)
        wide = spread(wide, 4)
        for q in range(4):
            for t in range(2):
                ycode[e, q, t] = jnp.concatenate([coded(value[q, t, rb], wide) for rb in range(2)], axis=0).astype(I16)
        for d in range(1, 4):
            for copy in y_copies(e, d):
                copy.start()

        @pl.when(core == 0)
        def _():
            for copy in y_copies(e, 0):
                copy.start()

        @pl.when(core == 1)
        def _():
            yget[4, 0] = ycode[4, y]
            ygets[4, pl.ds(0, 1)] = yscale[pl.ds(4, 1)]

    def widened(code_ref, scale_row):
        code = code_ref[...].astype(jnp.int32).astype(F32)
        scale = spread(jnp.broadcast_to(scale_row, (8, 128)), 4)
        return [code[rb * 8 : (rb + 1) * 8] * scale for rb in range(2)]

    def homeward(e):
        @pl.when(e < 4)
        def _():
            came(yget.at[e], y_recv.at[e])
            came(ygets.at[e, pl.ds(0, 4)], ys_recv.at[e])

        @pl.when(e == 4)
        def _():
            came(yget.at[4, pl.ds(1, 3)], y_recv.at[4])
            came(ygets.at[4, pl.ds(1, 3)], ys_recv.at[4])

        sums = [[0.0, 0.0], [0.0, 0.0]]
        for d in range(4):
            for t in range(2):
                for rb, part in enumerate(widened(yget.at[e, d, t], ygets[e, pl.ds(d, 1)])):
                    sums[t][rb] += part
        upper = lax.broadcasted_iota(jnp.int32, (8, 512), 0) < 4
        rows = [
            [jnp.where(upper, sums[0][rb], pltpu.roll(sums[1][rb], 4, 0)) for rb in range(2)],
            [jnp.where(upper, pltpu.roll(sums[0][rb], 4, 0), sums[1][rb]) for rb in range(2)],
        ]
        top, wide = one_row([x for z in range(2) for rb in range(2) for x in lane_tiles(rows[z][rb])])
        hscale[pl.ds(e, 1)] = top * (1.0 / TOP)
        wide = spread(wide, 4)
        for z in range(2):
            hcode[e, z] = jnp.concatenate([coded(rows[z][rb], wide) for rb in range(2)], axis=0).astype(I16)
        for copy in h_copies(e):
            copy.start()

    def relay(slot):
        came(tbuf.at[slot, y], z_recv.at[slot])
        for d in range(1, 4):
            forward(slot, d).start()

    def spread_slot(slot):
        came(tbuf.at[slot, pl.ds(0, 3)], f_recv.at[slot])
        to_partner(slot, tbuf.at[slot]).start()

    def step(i, carry):
        @pl.when(jnp.logical_and(core == 1, i == 0))
        def _():
            came(tbuf.at[4], x_recv.at[0])
            for c in range(2):
                near(c).start()
            for slot in (1, 0, 3, 2):
                relay(slot)
            spread_slot(1)
            spread_slot(0)

        @pl.when(jnp.logical_and(core == 1, i == 1))
        def _():
            spread_slot(2)
            spread_slot(3)

        @pl.when(core == 0)
        def _():
            came(tbuf.at[pl.ds(2 * i, 2)], x_recv.at[i])

        solve((i * 2 + (1 - i) * (1 + 3 * core), i * 3 + (1 - i) * core))

        @pl.when(core == 0)
        def _():
            def combine(k, inner):
                slot = 2 * i + k

                @pl.when(slot == 1)
                def _():
                    came(other.at[1], c_recv.at[0])

                @pl.when(slot == 2)
                def _():
                    came(other.at[pl.ds(2, 2)], c_recv.at[1])

                over_y(slot, terms[slot] + other[slot])
                return inner

            lax.fori_loop(0, 2, combine, 0)

        @pl.when(jnp.logical_and(core == 1, i == 0))
        def _():
            to_other(1).start()
            over_y(4, terms[4])

        @pl.when(jnp.logical_and(core == 1, i == 1))
        def _():
            to_other(2).start()
            to_other(3).start()

        return carry

    lax.fori_loop(0, 2, step, 0)

    for r in range(2):
        res_out[r] = restored([res_acc[r, rb] for rb in range(2)], perm_ref)

    def send_home(j, carry):
        homeward(lax.rem(j + 4, 5))
        return carry

    @pl.when(core == 1)
    def _():
        lax.fori_loop(0, 5, send_home, 0)

    def take(at):
        for rb, part in enumerate(widened(hget.at[at], hgets[pl.ds(at, 1)])):
            total[rb] += part

    total[...] = jnp.zeros_like(total)

    @pl.when(core == 1)
    def _():
        came(hget.at[pl.ds(2, 4)], h_recv)
        came(hgets.at[pl.ds(2, 4)], hs_recv)

    @pl.when(core == 0)
    def _():
        came(hget, h_recv)
        came(hgets.at[pl.ds(0, 6)], hs_recv)
        for at in range(2):
            take(at)

    for at in range(2, 6):
        take(at)

    trav_out[...] = restored([total[rb] for rb in range(2)], perm_ref).reshape(2, 4, 1024)

    @pl.when(core == 0)
    def _():
        left(mine.at[0], z_send)
        left(mine, x_send)
        left(ycode.at[pl.ds(0, 4)], y_send)
        left(ysent, ys_send)

    @pl.when(core == 1)
    def _():
        left(mine.at[pl.ds(0, 3)], z_send)
        left(tbuf.at[pl.ds(0, 3)], f_send)
        left(tbuf.at[pl.ds(0, 4)], x_send)
        left(terms.at[pl.ds(1, 3)], c_send)
        left(ycode.at[4, pl.ds(0, 3)], y_send)
        left(ysent.at[pl.ds(0, 3)], ys_send)
        left(hcode, h_send)
        left(ysent.at[pl.ds(0, 10)], hs_send)


def store(res_ref, trav_ref, res_out, trav_out, sem):
    copies = [
        pltpu.make_async_copy(res_ref, res_out, sem.at[0]),
        pltpu.make_async_copy(trav_ref, trav_out, sem.at[1]),
    ]
    for copy in copies:
        copy.start()
    for copy in copies:
        copy.wait()


def local(residents, travellers, pair_list):
    consts = tables(32)
    hbm = pl.BlockSpec(memory_space=pltpu.HBM)
    vmem = pl.BlockSpec(memory_space=pltpu.VMEM)
    dma = pltpu.SemaphoreType.DMA
    done = pl.pallas_call(
        kernel,
        out_shape=(pltpu.VMEM((2, 32, 1024), F32), pltpu.VMEM((2, 4, 1024), F32)),
        in_specs=[hbm] * 6,
        out_specs=(vmem, vmem),
        scratch_shapes=[
            pltpu.VMEM((2, 32, 1024), BF16),
            pltpu.VMEM((2, 32, 1024), BF16),
            pltpu.SMEM((1, 3, 2, 4), jnp.int32),
            pltpu.VMEM((4, 256, 256), BF16),
            pltpu.VMEM((17, 256, 256), BF16),
            pltpu.VMEM((4, 32, 256), F32),
            dma((6,)),
            pltpu.VMEM((4, 2, 16, 512), BF16),
            pltpu.VMEM((5, 4, 2, 16, 512), BF16),
            pltpu.VMEM((2, 2, 32, 512), F32),
            pltpu.VMEM((2, 2, 32, 512), F32),
            pltpu.VMEM((5, 4, 2, 2, 8, 512), F32),
            pltpu.VMEM((5, 4, 2, 2, 8, 512), F32),
            pltpu.VMEM((5, 4, 2, 16, 512), I16),
            pltpu.VMEM((8, 128), F32),
            pltpu.VMEM((16, 128), F32),
            pltpu.VMEM((5, 4, 2, 16, 512), I16),
            pltpu.VMEM((5, 8, 128), F32),
            pltpu.VMEM((5, 2, 16, 512), I16),
            pltpu.VMEM((8, 128), F32),
            pltpu.VMEM((6, 16, 512), I16),
            pltpu.VMEM((8, 128), F32),
            pltpu.VMEM((2, 8, 512), F32),
            dma,
            dma((4,)),
            dma,
            dma((4,)),
            dma,
            dma((2,)),
            dma,
            dma((2,)),
            dma,
            dma,
            dma((5,)),
            dma((5,)),
            dma,
            dma,
            dma,
            dma,
        ],
        compiler_params=pltpu.CompilerParams(
            collective_id=0, has_side_effects=True
        ),
    )(residents, travellers, pair_list.transpose(0, 3, 2, 1), *[jnp.asarray(c) for c in consts])
    return pl.pallas_call(
        store,
        out_shape=(
            jax.ShapeDtypeStruct((2, 32, 1024), F32),
            jax.ShapeDtypeStruct((2, 4, 1024), F32),
        ),
        in_specs=[vmem] * 2,
        out_specs=(hbm, hbm),
        scratch_shapes=[dma((2,))],
        compiler_params=pltpu.CompilerParams(vmem_limit_bytes=2**20),
    )(*done)


def solution(mesh):
    return jax.shard_map(
        local,
        mesh=mesh,
        in_specs=(
            P(("blk", "grp"), None, None),
            P("blk", None, None),
            P(("blk", "grp"), None, None, None),
        ),
        out_specs=(P(("blk", "grp"), None, None), P("blk", "grp", None)),
        check_vma=False,
    )
```

```python
import functools

import jax
import jax.numpy as jnp
import numpy as np
from jax import lax
from jax.experimental import pallas as pl
from jax.experimental.pallas import tpu as pltpu
from jax.sharding import PartitionSpec as P

MESH = pl.DeviceIdType.MESH
F32, BF16, I16 = jnp.float32, jnp.bfloat16, jnp.int16
TOP = 32767.0


def tables(edge):
    half = edge // 2
    index = np.arange(edge, dtype=np.float64) + 1.0
    sine = np.sqrt(2.0 / (edge + 1)) * np.sin(np.pi * np.outer(index, index) / (edge + 1))
    eigen = 2.0 - 2.0 * np.cos(np.pi * index / (edge + 1))
    perm = np.zeros((2, 256, 256))
    for b8 in range(8):
        for c in range(edge):
            rc, cc = (0, c) if c < half else (1, edge - 1 - c)
            perm[0, b8 * edge + c, rc * 128 + b8 * half + cc] = 1.0
            perm[1, b8 * edge + c, rc * 128 + (7 - b8) * half + cc] = 1.0
    perms = np.concatenate([perm, perm.transpose(0, 2, 1)])
    planes, scales = [], []
    for pb in range(2):
        for pc in range(2):
            planes.append(np.kron(sine[pb::2, :half].T, sine[pc::2, :half].T))
            scales.append(
                1.0
                / (
                    eigen[:, None, None]
                    + eigen[None, pb::2, None]
                    + eigen[None, None, pc::2]
                ).reshape(edge, half * half)
            )
    planes = np.stack(planes)
    both = np.stack([planes, planes.transpose(0, 2, 1)]).astype(np.float32)
    high = both.astype(jnp.bfloat16)
    low = (both - high.astype(np.float32)).astype(jnp.bfloat16)
    weights = np.stack([high, low], axis=2)
    small = np.kron(np.eye(4), sine).astype(np.float32)
    small_high = small.astype(jnp.bfloat16)
    small_low = (small - small_high.astype(np.float32)).astype(jnp.bfloat16)
    rows = np.block([[small_high, small_high], [small_low, small_low]])
    return (
        perms.astype(jnp.bfloat16),
        np.concatenate([weights.reshape(16, 256, 256), rows[None]]),
        np.stack(scales).astype(np.float32),
    )


def dot(a, b):
    return jnp.dot(a, b, preferred_element_type=F32)


def split(x):
    high = x.astype(BF16)
    return high, (x - high.astype(F32)).astype(BF16)


def permuted(x, perm_ref):
    halves = []
    for rb in range(2):
        parts = [[None, None], [None, None]]
        for n in range(2):
            m = n if rb == 0 else 3 - n
            y = dot(x[:, m * 256 : (m + 1) * 256], perm_ref[rb])
            parts[0][n], parts[1][n] = y[:, :128], y[:, 128:]
        halves.append(jnp.concatenate(parts[0] + parts[1], axis=1))
    return halves


def restored(halves, perm_ref):
    rows = halves[0].shape[0]
    groups = [None] * 4
    for rb in range(2):
        for n in range(2):
            m = n if rb == 0 else 3 - n
            x = jnp.concatenate(
                [
                    halves[rb][:, n * 128 : (n + 1) * 128],
                    halves[rb][:, 256 + n * 128 : 256 + (n + 1) * 128],
                ],
                axis=1,
            )
            y = dot(jnp.concatenate(split(x), axis=0), perm_ref[2 + rb])
            groups[m] = y[:rows] + y[rows:]
    return jnp.concatenate(groups, axis=1)


def plane(g, weight_ref, way):
    out = []
    for p in range(4):
        high, low = split(g[p])
        rows = high.shape[0]
        a = dot(jnp.concatenate([high, low], axis=0), weight_ref[way * 8 + p * 2])
        out.append(a[:rows] + a[rows:] + dot(high, weight_ref[way * 8 + p * 2 + 1]))
    return out


def along_rows(g, rows):
    out = []
    for p in range(4):
        both = dot(rows, jnp.concatenate(split(g[p]), axis=0))
        half = both.shape[0] // 2
        out.append(both[:half] + both[half:])
    return out


def peak(tiles):
    tiles = [jnp.abs(t) for t in tiles]
    while len(tiles) > 1:
        tiles = [
            jnp.maximum(tiles[i], tiles[i + 1]) if i + 1 < len(tiles) else tiles[i]
            for i in range(0, len(tiles), 2)
        ]
    return jnp.maximum(tiles[0], 1e-30)


def lane_tiles(x):
    return [x[:, j * 128 : (j + 1) * 128] for j in range(x.shape[1] // 128)]


def coded(x, wide):
    return jnp.round(x * wide).astype(jnp.int32)


def spread(tile, times):
    return jnp.concatenate([tile] * times, axis=1)


def kernel(
    res_hbm,
    trav_hbm,
    pair_hbm,
    perm_hbm,
    weight_hbm,
    scale_hbm,
    res_out,
    trav_out,
    res_in,
    trav_in,
    pair_ref,
    perm_ref,
    weight_ref,
    scale_ref,
    load_sem,
    mine,
    tbuf,
    ubuf,
    res_acc,
    terms,
    other,
    ycode,
    yscale,
    ysent,
    yget,
    ygets,
    hcode,
    hscale,
    hget,
    hgets,
    total,
    z_send,
    z_recv,
    f_send,
    f_recv,
    x_send,
    x_recv,
    c_send,
    c_recv,
    y_send,
    ys_send,
    y_recv,
    ys_recv,
    h_send,
    hs_send,
    h_recv,
    hs_recv,
):
    n_blk = lax.axis_size("blk")
    blk, grp = lax.axis_index("blk"), lax.axis_index("grp")
    core = lax.rem(blk, 2)
    first = blk - core
    y, lo = grp // 2, lax.rem(grp, 2)
    partner = (first + 1 - core, grp)
    across_z = y * 2 + 1 - lo

    def around(b):
        return lax.rem(b + n_blk, n_blk)

    def y_peer(d):
        return lax.rem(y + d, 4)

    def remote(src, dst, send, recv, to):
        return pltpu.make_async_remote_copy(
            src_ref=src, dst_ref=dst, send_sem=send, recv_sem=recv, device_id=to, device_id_type=MESH
        )

    def came(ref, sem):
        remote(ref, ref, sem, sem, partner).wait_recv()

    def left(ref, sem):
        remote(ref, ref, sem, sem, partner).wait_send()

    loads = [
        pltpu.make_async_copy(src, dst, load_sem.at[j])
        for j, (src, dst) in enumerate(
            (
                (trav_hbm, trav_in),
                (perm_hbm, perm_ref),
                (res_hbm, res_in),
                (pair_hbm, pair_ref),
                (scale_hbm, scale_ref),
                (weight_hbm, weight_ref),
            )
        )
    ]
    for load in loads:
        load.start()

    barrier = pltpu.get_barrier_semaphore()

    def arrive(to):
        pl.semaphore_signal(barrier, inc=1, device_id=to, device_id_type=MESH)

    arrive(partner)
    arrive((blk, across_z))

    @pl.when(core == 1)
    def _():
        for c in range(2):
            arrive((around(first - 4 + c), across_z))
            arrive((around(first - 2 + c), grp))
            for d in range(1, 4):
                arrive((first + c, y_peer(d) * 2 + lo))

    loads[0].wait()
    loads[1].wait()
    own = [h.reshape(2, 4, 8, 512) for h in permuted(trav_in[...].reshape(64, 1024), perm_ref)]
    for q in range(4):
        for t in range(2):
            mine[q, t] = jnp.concatenate([own[0][t, q], own[1][t, q]], axis=0).astype(BF16)

    pl.semaphore_wait(barrier, 7)

    far = remote(mine.at[y], tbuf.at[core, y], z_send, z_recv.at[core], (around(first + 5), across_z))
    far.start()

    def near(c):
        src = mine.at[y] if c else tbuf.at[4, y]
        return remote(src, tbuf.at[2 + c, y], z_send, z_recv.at[2 + c], (around(first + 3), grp))

    def to_partner(slot, src):
        return remote(src, tbuf.at[slot], x_send, x_recv.at[slot // 2 % 2], partner)

    @pl.when(core == 0)
    def _():
        to_partner(4, mine).start()

    loads[2].wait()
    for rb, h in enumerate(permuted(res_in[...].reshape(64, 1024), perm_ref)):
        for r in range(2):
            ubuf[r, rb] = h[r * 32 : (r + 1) * 32]
    res_acc[...] = jnp.zeros_like(res_acc)

    other[0] = jnp.zeros((4, 2, 2, 8, 512), F32)

    def forward(slot, d):
        return remote(
            tbuf.at[slot, y],
            tbuf.at[slot, y],
            f_send,
            f_recv.at[slot],
            (blk, y_peer(d) * 2 + lo),
        )

    for load in loads[3:]:
        load.wait()

    def to_other(slot):
        return remote(terms.at[slot], other.at[slot], c_send, c_recv.at[slot - 1], partner)

    def y_copies(e, d):
        to = (first + 1, y_peer(d) * 2 + lo)
        return (
            remote(ycode.at[e, y_peer(d)], yget.at[e, d], y_send, y_recv.at[e], to),
            remote(yscale.at[pl.ds(e, 1)], ygets.at[e, pl.ds(d, 1)], ys_send, ys_recv.at[e], to),
        )

    def h_copies(e):
        at = (5 - e) // 2 * 2 + lo
        copies = []
        for z in range(2):
            to = (around(first - 4 + e), y * 2 + z)
            copies += [
                remote(hcode.at[e, z], hget.at[at], h_send, h_recv, to),
                remote(hscale.at[pl.ds(e, 1)], hgets.at[pl.ds(at, 1)], hs_send, hs_recv, to),
            ]
        return copies

    def solve(slots):
        u, w, factors = [], [], []
        for slot in slots:
            s = lax.rem(3 - slot + core, 4)
            both = []
            for t in range(2):
                wide = tbuf[slot, :, t].astype(F32).reshape(4, 2, 8, 512)
                both.append([wide[:, rb].reshape(32, 512) for rb in range(2)])
            for p in range(2):
                r, t, active = (pair_ref[0, e, p, s] for e in range(3))
                u.append([ubuf[r, rb] for rb in range(2)])
                w.append([jnp.where(t == 1, both[1][rb], both[0][rb]) for rb in range(2)])
                factors.append([[jnp.where(e == j, active, 0).astype(F32) for j in range(2)] for e in (r, t)])
        d = [jnp.concatenate([u[f][rb] * w[f][rb] for f in range(4)], axis=0) for rb in range(2)]
        g = []
        for e in (d[0] + d[1], d[0] - d[1]):
            g += [e[:, :256] + e[:, 256:], e[:, :256] - e[:, 256:]]
        rows = weight_ref[16]
        g = along_rows(plane(g, weight_ref, 0), rows)
        g = [
            (m.reshape(4, 32, 256) * scale_ref[p][None]).reshape(128, 256)
            for p, m in enumerate(g)
        ]
        g = plane(along_rows(g, rows), weight_ref, 1)
        pot = []
        for e, o in (
            (g[0] + g[2], g[1] + g[3]),
            (g[0] - g[2], g[1] - g[3]),
        ):
            pot.append(jnp.concatenate([e + o, e - o], axis=1))
        for rb in range(2):
            v = [pot[rb][f * 32 : (f + 1) * 32] for f in range(4)]
            vw = [v[f] * w[f][rb] for f in range(4)]
            vu = [v[f] * u[f][rb] for f in range(4)]
            for j in range(2):
                ours = [vw[f] * factors[f][0][j] for f in range(4)]
                res_acc[j, rb] += (ours[0] + ours[1]) + (ours[2] + ours[3])
                for k, slot in enumerate(slots):
                    f = 2 * k
                    theirs = vu[f] * factors[f][1][j] + vu[f + 1] * factors[f + 1][1][j]
                    terms[slot, :, j, rb] = theirs.reshape(4, 8, 512)

    def one_row(tiles):
        top = jnp.max(peak(tiles), axis=0, keepdims=True)
        return top, jnp.broadcast_to(TOP / top, (8, 128))

    def over_y(e, value):
        parts = [(q, t, rb) for q in range(4) for t in range(2) for rb in range(2)]
        top, wide = one_row([x for at in parts for x in lane_tiles(value[at])])
        yscale[pl.ds(e, 1)] = top * (1.0 / TOP)
        wide = spread(wide, 4)
        for q in range(4):
            for t in range(2):
                ycode[e, q, t] = jnp.concatenate([coded(value[q, t, rb], wide) for rb in range(2)], axis=0).astype(I16)
        for d in (2, 1, 3):
            for copy in y_copies(e, d):
                copy.start()

        @pl.when(core == 0)
        def _():
            for copy in y_copies(e, 0):
                copy.start()

        @pl.when(core == 1)
        def _():
            yget[4, 0] = ycode[4, y]
            ygets[4, pl.ds(0, 1)] = yscale[pl.ds(4, 1)]

    def widened(code_ref, scale_row):
        code = code_ref[...].astype(jnp.int32).astype(F32)
        scale = spread(jnp.broadcast_to(scale_row, (8, 128)), 4)
        return [code[rb * 8 : (rb + 1) * 8] * scale for rb in range(2)]

    def homeward(e):
        @pl.when(e < 4)
        def _():
            came(yget.at[e], y_recv.at[e])
            came(ygets.at[e, pl.ds(0, 4)], ys_recv.at[e])

        @pl.when(e == 4)
        def _():
            came(yget.at[4, pl.ds(1, 3)], y_recv.at[4])
            came(ygets.at[4, pl.ds(1, 3)], ys_recv.at[4])

        sums = [[0.0, 0.0], [0.0, 0.0]]
        for d in range(4):
            for t in range(2):
                for rb, part in enumerate(widened(yget.at[e, d, t], ygets[e, pl.ds(d, 1)])):
                    sums[t][rb] += part
        upper = lax.broadcasted_iota(jnp.int32, (8, 512), 0) < 4
        rows = [
            [jnp.where(upper, sums[0][rb], pltpu.roll(sums[1][rb], 4, 0)) for rb in range(2)],
            [jnp.where(upper, pltpu.roll(sums[0][rb], 4, 0), sums[1][rb]) for rb in range(2)],
        ]
        top, wide = one_row([x for z in range(2) for rb in range(2) for x in lane_tiles(rows[z][rb])])
        hscale[pl.ds(e, 1)] = top * (1.0 / TOP)
        wide = spread(wide, 4)
        for z in range(2):
            hcode[e, z] = jnp.concatenate([coded(rows[z][rb], wide) for rb in range(2)], axis=0).astype(I16)
        for copy in h_copies(e):
            copy.start()

    def relay(slot):
        came(tbuf.at[slot, y], z_recv.at[slot])
        for d in (2, 1, 3):
            forward(slot, d).start()

    def spread_slot(slot):
        came(tbuf.at[slot, pl.ds(0, 3)], f_recv.at[slot])
        to_partner(slot, tbuf.at[slot]).start()

    def step(i, carry):
        @pl.when(jnp.logical_and(core == 1, i == 0))
        def _():
            came(tbuf.at[4], x_recv.at[0])
            for c in range(2):
                near(c).start()
            for slot in (1, 0, 3, 2):
                relay(slot)
            spread_slot(1)
            spread_slot(0)

        @pl.when(jnp.logical_and(core == 1, i == 1))
        def _():
            spread_slot(2)
            spread_slot(3)

        @pl.when(core == 0)
        def _():
            came(tbuf.at[pl.ds(2 * i, 2)], x_recv.at[i])

        solve((i * 2 + (1 - i) * (1 + 3 * core), i * 3 + (1 - i) * core))

        @pl.when(core == 0)
        def _():
            def combine(k, inner):
                slot = 2 * i + k

                @pl.when(slot > 0)
                def _():
                    to_other(slot).wait_recv()

                over_y(slot, terms[slot] + other[slot])
                return inner

            lax.fori_loop(0, 2, combine, 0)

        @pl.when(jnp.logical_and(core == 1, i == 0))
        def _():
            to_other(1).start()
            over_y(4, terms[4])

        @pl.when(jnp.logical_and(core == 1, i == 1))
        def _():
            to_other(2).start()
            to_other(3).start()

        return carry

    lax.fori_loop(0, 2, step, 0)

    for r in range(2):
        res_out[r] = restored([res_acc[r, rb] for rb in range(2)], perm_ref)

    def send_home(j, carry):
        homeward(lax.rem(j + 4, 5))
        return carry

    @pl.when(core == 1)
    def _():
        lax.fori_loop(0, 5, send_home, 0)

    def take(at):
        for rb, part in enumerate(widened(hget.at[at], hgets[pl.ds(at, 1)])):
            total[rb] += part

    total[...] = jnp.zeros_like(total)

    @pl.when(core == 1)
    def _():
        came(hget.at[pl.ds(2, 4)], h_recv)
        came(hgets.at[pl.ds(2, 4)], hs_recv)

    @pl.when(core == 0)
    def _():
        came(hget, h_recv)
        came(hgets.at[pl.ds(0, 6)], hs_recv)
        for at in range(2):
            take(at)

    for at in range(2, 6):
        take(at)

    trav_out[...] = restored([total[rb] for rb in range(2)], perm_ref).reshape(2, 4, 1024)

    @pl.when(core == 0)
    def _():
        left(mine.at[0], z_send)
        left(mine, x_send)
        left(ycode.at[pl.ds(0, 4)], y_send)
        left(ysent, ys_send)

    @pl.when(core == 1)
    def _():
        left(mine.at[pl.ds(0, 3)], z_send)
        left(tbuf.at[pl.ds(0, 3)], f_send)
        left(tbuf.at[pl.ds(0, 4)], x_send)
        left(terms.at[pl.ds(1, 3)], c_send)
        left(ycode.at[4, pl.ds(0, 3)], y_send)
        left(ysent.at[pl.ds(0, 3)], ys_send)
        left(hcode, h_send)
        left(ysent.at[pl.ds(0, 10)], hs_send)


def store(res_ref, trav_ref, res_out, trav_out, sem):
    copies = [
        pltpu.make_async_copy(res_ref, res_out, sem.at[0]),
        pltpu.make_async_copy(trav_ref, trav_out, sem.at[1]),
    ]
    for copy in copies:
        copy.start()
    for copy in copies:
        copy.wait()


def local(residents, travellers, pair_list):
    consts = tables(32)
    hbm = pl.BlockSpec(memory_space=pltpu.HBM)
    vmem = pl.BlockSpec(memory_space=pltpu.VMEM)
    dma = pltpu.SemaphoreType.DMA
    done = pl.pallas_call(
        kernel,
        out_shape=(pltpu.VMEM((2, 32, 1024), F32), pltpu.VMEM((2, 4, 1024), F32)),
        in_specs=[hbm] * 6,
        out_specs=(vmem, vmem),
        scratch_shapes=[
            pltpu.VMEM((2, 32, 1024), BF16),
            pltpu.VMEM((2, 32, 1024), BF16),
            pltpu.SMEM((1, 3, 2, 4), jnp.int32),
            pltpu.VMEM((4, 256, 256), BF16),
            pltpu.VMEM((17, 256, 256), BF16),
            pltpu.VMEM((4, 32, 256), F32),
            dma((6,)),
            pltpu.VMEM((4, 2, 16, 512), BF16),
            pltpu.VMEM((5, 4, 2, 16, 512), BF16),
            pltpu.VMEM((2, 2, 32, 512), F32),
            pltpu.VMEM((2, 2, 32, 512), F32),
            pltpu.VMEM((5, 4, 2, 2, 8, 512), F32),
            pltpu.VMEM((5, 4, 2, 2, 8, 512), F32),
            pltpu.VMEM((5, 4, 2, 16, 512), I16),
            pltpu.VMEM((8, 128), F32),
            pltpu.VMEM((16, 128), F32),
            pltpu.VMEM((5, 4, 2, 16, 512), I16),
            pltpu.VMEM((5, 8, 128), F32),
            pltpu.VMEM((5, 2, 16, 512), I16),
            pltpu.VMEM((8, 128), F32),
            pltpu.VMEM((6, 16, 512), I16),
            pltpu.VMEM((8, 128), F32),
            pltpu.VMEM((2, 8, 512), F32),
            dma,
            dma((4,)),
            dma,
            dma((4,)),
            dma,
            dma((2,)),
            dma,
            dma((3,)),
            dma,
            dma,
            dma((5,)),
            dma((5,)),
            dma,
            dma,
            dma,
            dma,
        ],
        compiler_params=pltpu.CompilerParams(
            collective_id=0, has_side_effects=True
        ),
    )(residents, travellers, pair_list.transpose(0, 3, 2, 1), *[jnp.asarray(c) for c in consts])
    return pl.pallas_call(
        store,
        out_shape=(
            jax.ShapeDtypeStruct((2, 32, 1024), F32),
            jax.ShapeDtypeStruct((2, 4, 1024), F32),
        ),
        in_specs=[vmem] * 2,
        out_specs=(hbm, hbm),
        scratch_shapes=[dma((2,))],
        compiler_params=pltpu.CompilerParams(vmem_limit_bytes=2**20),
    )(*done)


def solution(mesh):
    return jax.shard_map(
        local,
        mesh=mesh,
        in_specs=(
            P(("blk", "grp"), None, None),
            P("blk", None, None),
            P(("blk", "grp"), None, None, None),
        ),
        out_specs=(P(("blk", "grp"), None, None), P("blk", "grp", None)),
        check_vma=False,
    )
```

```python
import functools

import jax
import jax.numpy as jnp
import numpy as np
from jax import lax
from jax.experimental import pallas as pl
from jax.experimental.pallas import tpu as pltpu
from jax.sharding import PartitionSpec as P

MESH = pl.DeviceIdType.MESH
F32, BF16, I16 = jnp.float32, jnp.bfloat16, jnp.int16
TOP = 32767.0


def tables(edge):
    half = edge // 2
    index = np.arange(edge, dtype=np.float64) + 1.0
    sine = np.sqrt(2.0 / (edge + 1)) * np.sin(np.pi * np.outer(index, index) / (edge + 1))
    eigen = 2.0 - 2.0 * np.cos(np.pi * index / (edge + 1))
    perm = np.zeros((2, 256, 256))
    for b8 in range(8):
        for c in range(edge):
            rc, cc = (0, c) if c < half else (1, edge - 1 - c)
            perm[0, b8 * edge + c, rc * 128 + b8 * half + cc] = 1.0
            perm[1, b8 * edge + c, rc * 128 + (7 - b8) * half + cc] = 1.0
    perms = np.concatenate([perm, perm.transpose(0, 2, 1)])
    planes, scales = [], []
    for pb in range(2):
        for pc in range(2):
            planes.append(np.kron(sine[pb::2, :half].T, sine[pc::2, :half].T))
            scales.append(
                1.0
                / (
                    eigen[:, None, None]
                    + eigen[None, pb::2, None]
                    + eigen[None, None, pc::2]
                ).reshape(edge, half * half)
            )
    planes = np.stack(planes)
    both = np.stack([planes, planes.transpose(0, 2, 1)]).astype(np.float32)
    high = both.astype(jnp.bfloat16)
    low = (both - high.astype(np.float32)).astype(jnp.bfloat16)
    weights = np.stack([high, low], axis=2)
    small = np.kron(np.eye(4), sine).astype(np.float32)
    small_high = small.astype(jnp.bfloat16)
    small_low = (small - small_high.astype(np.float32)).astype(jnp.bfloat16)
    rows = np.block([[small_high, small_high], [small_low, small_low]])
    return (
        perms.astype(jnp.bfloat16),
        np.concatenate([weights.reshape(16, 256, 256), rows[None]]),
        np.stack(scales).astype(np.float32),
    )


def dot(a, b):
    return jnp.dot(a, b, preferred_element_type=F32)


def split(x):
    high = x.astype(BF16)
    return high, (x - high.astype(F32)).astype(BF16)


def permuted(x, perm_ref):
    halves = []
    for rb in range(2):
        parts = [[None, None], [None, None]]
        for n in range(2):
            m = n if rb == 0 else 3 - n
            y = dot(x[:, m * 256 : (m + 1) * 256], perm_ref[rb])
            parts[0][n], parts[1][n] = y[:, :128], y[:, 128:]
        halves.append(jnp.concatenate(parts[0] + parts[1], axis=1))
    return halves


def restored(halves, perm_ref):
    rows = halves[0].shape[0]
    groups = [None] * 4
    for rb in range(2):
        for n in range(2):
            m = n if rb == 0 else 3 - n
            x = jnp.concatenate(
                [
                    halves[rb][:, n * 128 : (n + 1) * 128],
                    halves[rb][:, 256 + n * 128 : 256 + (n + 1) * 128],
                ],
                axis=1,
            )
            y = dot(jnp.concatenate(split(x), axis=0), perm_ref[2 + rb])
            groups[m] = y[:rows] + y[rows:]
    return jnp.concatenate(groups, axis=1)


def plane(g, weight_ref, way):
    out = []
    for p in range(4):
        high, low = split(g[p])
        rows = high.shape[0]
        a = dot(jnp.concatenate([high, low], axis=0), weight_ref[way * 8 + p * 2])
        out.append(a[:rows] + a[rows:] + dot(high, weight_ref[way * 8 + p * 2 + 1]))
    return out


def along_rows(g, rows):
    out = []
    for p in range(4):
        both = dot(rows, jnp.concatenate(split(g[p]), axis=0))
        half = both.shape[0] // 2
        out.append(both[:half] + both[half:])
    return out


def peak(tiles):
    tiles = [jnp.abs(t) for t in tiles]
    while len(tiles) > 1:
        tiles = [
            jnp.maximum(tiles[i], tiles[i + 1]) if i + 1 < len(tiles) else tiles[i]
            for i in range(0, len(tiles), 2)
        ]
    return jnp.maximum(tiles[0], 1e-30)


def lane_tiles(x):
    return [x[:, j * 128 : (j + 1) * 128] for j in range(x.shape[1] // 128)]


def coded(x, wide):
    return jnp.round(x * wide).astype(jnp.int32)


def spread(tile, times):
    return jnp.concatenate([tile] * times, axis=1)


def kernel(
    res_hbm,
    trav_hbm,
    pair_hbm,
    perm_hbm,
    weight_hbm,
    scale_hbm,
    res_out,
    trav_out,
    res_in,
    trav_in,
    pair_ref,
    perm_ref,
    weight_ref,
    scale_ref,
    load_sem,
    tbuf,
    ubuf,
    table,
    res_acc,
    res_got,
    terms,
    ycode,
    yscale,
    ysent,
    yget,
    ygets,
    hcode,
    hscale,
    hget,
    hgets,
    total,
    z_send,
    z_recv,
    f_send,
    f_recv,
    u_send,
    u_recv,
    p_send,
    p_recv,
    r_send,
    r_recv,
    y_send,
    ys_send,
    y_recv,
    ys_recv,
    h_send,
    hs_send,
    h_recv,
    hs_recv,
):
    n_blk = lax.axis_size("blk")
    blk, grp = lax.axis_index("blk"), lax.axis_index("grp")
    core = lax.rem(blk, 2)
    first = blk - core
    y, lo = grp // 2, lax.rem(grp, 2)
    partner = (first + 1 - core, grp)
    across_z = y * 2 + 1 - lo

    def around(b):
        return lax.rem(b + n_blk, n_blk)

    def y_peer(d):
        return lax.rem(y + d, 4)

    def remote(src, dst, send, recv, to):
        return pltpu.make_async_remote_copy(
            src_ref=src, dst_ref=dst, send_sem=send, recv_sem=recv, device_id=to, device_id_type=MESH
        )

    def came(ref, sem):
        remote(ref, ref, sem, sem, partner).wait_recv()

    def left(ref, sem):
        remote(ref, ref, sem, sem, partner).wait_send()

    loads = [
        pltpu.make_async_copy(src, dst, load_sem.at[j])
        for j, (src, dst) in enumerate(
            (
                (trav_hbm, trav_in),
                (perm_hbm, perm_ref),
                (res_hbm, res_in),
                (pair_hbm, pair_ref),
                (scale_hbm, scale_ref),
                (weight_hbm, weight_ref),
            )
        )
    ]
    for load in loads:
        load.start()

    barrier = pltpu.get_barrier_semaphore()

    def arrive(to):
        pl.semaphore_signal(barrier, inc=1, device_id=to, device_id_type=MESH)

    arrive((around(blk - 4), across_z))
    arrive((around(blk - 2), grp))
    for d in range(1, 4):
        arrive((blk, y_peer(d) * 2 + lo))
    arrive((blk, across_z))
    arrive(partner)

    @pl.when(core == 1)
    def _():
        for d in range(1, 4):
            arrive((first, y_peer(d) * 2 + lo))

    loads[0].wait()
    loads[1].wait()
    own = [h.reshape(2, 4, 8, 512) for h in permuted(trav_in[...].reshape(64, 1024), perm_ref)]
    for q in range(4):
        for t in range(2):
            tbuf[16 + q, t] = jnp.concatenate([own[0][t, q], own[1][t, q]], axis=0).astype(BF16)

    pl.semaphore_wait(barrier, 7 + 3 * (1 - core))

    def onward(near):
        to = (around(blk + 2), grp) if near else (around(blk + 4), across_z)
        return remote(tbuf.at[16 + y], tbuf.at[4 * (2 * near + core) + y], z_send, z_recv.at[near], to)

    onward(0).start()

    loads[2].wait()
    for rb, h in enumerate(permuted(res_in[...].reshape(64, 1024), perm_ref)):
        for r in range(2):
            ubuf[0, r, rb] = h[r * 32 : (r + 1) * 32].reshape(4, 8, 512)
    loads[3].wait()
    for s in range(4):
        for e in range(3):
            for p in range(2):
                table[0, s, 2 * e + p] = jnp.full((8, 128), pair_ref[0, e, p, s].astype(F32))
    shares = [
        remote(ubuf.at[0], ubuf.at[1], u_send, u_recv, partner),
        remote(table.at[0], table.at[1], p_send, p_recv, partner),
    ]
    for share in shares:
        share.start()
    res_acc[...] = jnp.zeros_like(res_acc)
    for load in loads[4:]:
        load.wait()
    for share in shares:
        share.wait_recv()
    onward(1).start()

    def forward(near, d):
        at = 4 * (2 * near + core) + y
        return remote(tbuf.at[at], tbuf.at[at], f_send, f_recv.at[near], (blk, y_peer(d) * 2 + lo))

    def y_copies(e, d):
        to = (first + 1, y_peer(d) * 2 + lo)
        return (
            remote(ycode.at[4 * e + y_peer(d)], yget.at[e, d], y_send, y_recv.at[e], to),
            remote(yscale.at[pl.ds(e, 1)], ygets.at[e, pl.ds(d, 1)], ys_send, ys_recv.at[e], to),
        )

    def h_copies(e):
        at = (5 - e) // 2 * 2 + lo
        copies = []
        for z in range(2):
            to = (around(first - 4 + e), y * 2 + z)
            copies += [
                remote(hcode.at[e, z], hget.at[at], h_send, h_recv, to),
                remote(hscale.at[pl.ds(e, 1)], hgets.at[pl.ds(at, 1)], hs_send, hs_recv, to),
            ]
        return copies

    def solve(slots):
        u, w, factors = [], [], []
        for owner, slot in enumerate(slots):
            s = (core if owner == 0 else 1 - core) + 3 - slot
            both = []
            for t in range(2):
                wide = tbuf[pl.ds(4 * slot, 4), t].astype(F32).reshape(4, 2, 8, 512)
                both.append([wide[:, rb] for rb in range(2)])
            for p in range(2):
                r, t, active = (spread(table[owner, s, 2 * e + p], 4)[None] for e in range(3))
                u.append([jnp.where(r > 0.5, ubuf[owner, 1, rb], ubuf[owner, 0, rb]) for rb in range(2)])
                w.append([jnp.where(t > 0.5, both[1][rb], both[0][rb]) for rb in range(2)])
                factors.append([[active - active * e, active * e] for e in (r, t)])
        d = [
            jnp.concatenate([(u[f][rb] * w[f][rb]).reshape(32, 512) for f in range(4)], axis=0)
            for rb in range(2)
        ]
        g = []
        for e in (d[0] + d[1], d[0] - d[1]):
            g += [e[:, :256] + e[:, 256:], e[:, :256] - e[:, 256:]]
        rows = weight_ref[16]
        g = along_rows(plane(g, weight_ref, 0), rows)
        g = [
            (m.reshape(4, 32, 256) * scale_ref[p][None]).reshape(128, 256)
            for p, m in enumerate(g)
        ]
        g = plane(along_rows(g, rows), weight_ref, 1)
        pot = []
        for e, o in (
            (g[0] + g[2], g[1] + g[3]),
            (g[0] - g[2], g[1] - g[3]),
        ):
            pot.append(jnp.concatenate([e + o, e - o], axis=1))
        for rb in range(2):
            v = [pot[rb][f * 32 : (f + 1) * 32].reshape(4, 8, 512) for f in range(4)]
            for owner in range(2):
                f, f1 = 2 * owner, 2 * owner + 1
                vw, vw1 = v[f] * w[f][rb], v[f1] * w[f1][rb]
                vu, vu1 = v[f] * u[f][rb], v[f1] * u[f1][rb]
                for j in range(2):
                    res_acc[owner, j, rb] += vw * factors[f][0][j] + vw1 * factors[f1][0][j]
                    terms[owner, :, j, rb] = vu * factors[f][1][j] + vu1 * factors[f1][1][j]

    def one_row(tiles):
        top = jnp.max(peak(tiles), axis=0, keepdims=True)
        return top, jnp.broadcast_to(TOP / top, (8, 128))

    def over_y(e, value):
        parts = [(q, t, rb) for q in range(4) for t in range(2) for rb in range(2)]
        top, wide = one_row([x for at in parts for x in lane_tiles(value[at])])
        yscale[pl.ds(e, 1)] = top * (1.0 / TOP)
        wide = spread(wide, 4)
        for q in range(4):
            for t in range(2):
                ycode[4 * e + q, t] = jnp.concatenate([coded(value[q, t, rb], wide) for rb in range(2)], axis=0).astype(I16)
        for d in (2, 1, 3):
            for copy in y_copies(e, d):
                copy.start()

        @pl.when(core == 0)
        def _():
            for copy in y_copies(e, 0):
                copy.start()

        @pl.when(core == 1)
        def _():
            yget[e, 0] = ycode[4 * e + y]
            ygets[e, pl.ds(0, 1)] = yscale[pl.ds(e, 1)]

    def widened(code_ref, scale_row):
        code = code_ref[...].astype(jnp.int32).astype(F32)
        scale = spread(jnp.broadcast_to(scale_row, (8, 128)), 4)
        return [code[rb * 8 : (rb + 1) * 8] * scale for rb in range(2)]

    def homeward(e):
        @pl.when(lax.rem(e, 2) == 0)
        def _():
            came(yget.at[e], y_recv.at[e])
            came(ygets.at[e, pl.ds(0, 4)], ys_recv.at[e])

        @pl.when(lax.rem(e, 2) == 1)
        def _():
            came(yget.at[e, pl.ds(1, 3)], y_recv.at[e])
            came(ygets.at[e, pl.ds(1, 3)], ys_recv.at[e])

        sums = [[0.0, 0.0], [0.0, 0.0]]
        for d in range(4):
            for t in range(2):
                for rb, part in enumerate(widened(yget.at[e, d, t], ygets[e, pl.ds(d, 1)])):
                    sums[t][rb] += part
        upper = lax.broadcasted_iota(jnp.int32, (8, 512), 0) < 4
        rows = [
            [jnp.where(upper, sums[0][rb], pltpu.roll(sums[1][rb], 4, 0)) for rb in range(2)],
            [jnp.where(upper, pltpu.roll(sums[0][rb], 4, 0), sums[1][rb]) for rb in range(2)],
        ]
        top, wide = one_row([x for z in range(2) for rb in range(2) for x in lane_tiles(rows[z][rb])])
        hscale[pl.ds(e, 1)] = top * (1.0 / TOP)
        wide = spread(wide, 4)
        for z in range(2):
            hcode[e, z] = jnp.concatenate([coded(rows[z][rb], wide) for rb in range(2)], axis=0).astype(I16)
        for copy in h_copies(e):
            copy.start()

    def step(i, carry):
        @pl.when(i == 0)
        def _():
            for near in range(2):
                came(tbuf.at[4 * (2 * near + core) + y], z_recv.at[near])
                for d in (2, 1, 3):
                    forward(near, d).start()

        came(tbuf.at[pl.ds(0, 3)], f_recv.at[i])
        slot = 2 * i + core
        apart = (1 - core) * (1 - i)
        solve((slot, slot + 4 * apart))

        @pl.when(apart == 0)
        def _():
            terms[0] += terms[1]

        def send(k, inner):
            over_y(slot + 4 * k, terms[k])
            return inner

        lax.fori_loop(0, 1 + apart, send, 0)
        return carry

    lax.fori_loop(0, 2, step, 0)

    back = remote(res_acc.at[1], res_got, r_send, r_recv, partner)
    back.start()

    def send_home(j, carry):
        even = (j + 3) // 5
        homeward((1 - even) * (2 * j + 1) + even * lax.rem(4 * j + 4, 6))
        return carry

    @pl.when(core == 1)
    def _():
        lax.fori_loop(0, 5, send_home, 0)

    back.wait_recv()
    for r in range(2):
        res_out[r] = restored([(res_acc[0, r, rb] + res_got[r, rb]).reshape(32, 512) for rb in range(2)], perm_ref)

    def take(at):
        for rb, part in enumerate(widened(hget.at[at], hgets[pl.ds(at, 1)])):
            total[rb] += part

    total[...] = jnp.zeros_like(total)

    @pl.when(core == 1)
    def _():
        came(hget.at[pl.ds(2, 4)], h_recv)
        came(hgets.at[pl.ds(2, 4)], hs_recv)

    @pl.when(core == 0)
    def _():
        came(hget, h_recv)
        came(hgets.at[pl.ds(0, 6)], hs_recv)
        for at in range(2):
            take(at)

    for at in range(2, 6):
        take(at)

    trav_out[...] = restored([total[rb] for rb in range(2)], perm_ref).reshape(2, 4, 1024)

    left(tbuf.at[pl.ds(0, 2)], z_send)
    left(tbuf.at[pl.ds(0, 6)], f_send)
    for share in shares:
        share.wait_send()
    back.wait_send()

    @pl.when(core == 0)
    def _():
        left(ycode.at[pl.ds(0, 12)], y_send)
        left(ysent.at[pl.ds(0, 12)], ys_send)

    @pl.when(core == 1)
    def _():
        left(ycode.at[pl.ds(0, 6)], y_send)
        left(ysent.at[pl.ds(0, 6)], ys_send)
        left(hcode, h_send)
        left(ysent.at[pl.ds(0, 10)], hs_send)


def store(res_ref, trav_ref, res_out, trav_out, sem):
    copies = [
        pltpu.make_async_copy(res_ref, res_out, sem.at[0]),
        pltpu.make_async_copy(trav_ref, trav_out, sem.at[1]),
    ]
    for copy in copies:
        copy.start()
    for copy in copies:
        copy.wait()


def local(residents, travellers, pair_list):
    consts = tables(32)
    hbm = pl.BlockSpec(memory_space=pltpu.HBM)
    vmem = pl.BlockSpec(memory_space=pltpu.VMEM)
    dma = pltpu.SemaphoreType.DMA
    done = pl.pallas_call(
        kernel,
        out_shape=(pltpu.VMEM((2, 32, 1024), F32), pltpu.VMEM((2, 4, 1024), F32)),
        in_specs=[hbm] * 6,
        out_specs=(vmem, vmem),
        scratch_shapes=[
            pltpu.VMEM((2, 32, 1024), BF16),
            pltpu.VMEM((2, 32, 1024), BF16),
            pltpu.SMEM((1, 3, 2, 4), jnp.int32),
            pltpu.VMEM((4, 256, 256), BF16),
            pltpu.VMEM((17, 256, 256), BF16),
            pltpu.VMEM((4, 32, 256), F32),
            dma((6,)),
            pltpu.VMEM((20, 2, 16, 512), BF16),
            pltpu.VMEM((2, 2, 2, 4, 8, 512), F32),
            pltpu.VMEM((2, 4, 6, 8, 128), F32),
            pltpu.VMEM((2, 2, 2, 4, 8, 512), F32),
            pltpu.VMEM((2, 2, 4, 8, 512), F32),
            pltpu.VMEM((2, 4, 2, 2, 8, 512), F32),
            pltpu.VMEM((20, 2, 16, 512), I16),
            pltpu.VMEM((8, 128), F32),
            pltpu.VMEM((16, 128), F32),
            pltpu.VMEM((5, 4, 2, 16, 512), I16),
            pltpu.VMEM((5, 8, 128), F32),
            pltpu.VMEM((5, 2, 16, 512), I16),
            pltpu.VMEM((8, 128), F32),
            pltpu.VMEM((6, 16, 512), I16),
            pltpu.VMEM((8, 128), F32),
            pltpu.VMEM((2, 8, 512), F32),
            dma,
            dma((2,)),
            dma,
            dma((2,)),
            dma,
            dma,
            dma,
            dma,
            dma,
            dma,
            dma,
            dma,
            dma((5,)),
            dma((5,)),
            dma,
            dma,
            dma,
            dma,
        ],
        compiler_params=pltpu.CompilerParams(
            collective_id=0, has_side_effects=True
        ),
    )(residents, travellers, pair_list.transpose(0, 3, 2, 1), *[jnp.asarray(c) for c in consts])
    return pl.pallas_call(
        store,
        out_shape=(
            jax.ShapeDtypeStruct((2, 32, 1024), F32),
            jax.ShapeDtypeStruct((2, 4, 1024), F32),
        ),
        in_specs=[vmem] * 2,
        out_specs=(hbm, hbm),
        scratch_shapes=[dma((2,))],
        compiler_params=pltpu.CompilerParams(vmem_limit_bytes=2**20),
    )(*done)


def solution(mesh):
    return jax.shard_map(
        local,
        mesh=mesh,
        in_specs=(
            P(("blk", "grp"), None, None),
            P("blk", None, None),
            P(("blk", "grp"), None, None, None),
        ),
        out_specs=(P(("blk", "grp"), None, None), P("blk", "grp", None)),
        check_vma=False,
    )
```

```python
import functools

import jax
import jax.numpy as jnp
import numpy as np
from jax import lax
from jax.experimental import pallas as pl
from jax.experimental.pallas import tpu as pltpu
from jax.sharding import PartitionSpec as P

MESH = pl.DeviceIdType.MESH
F32, BF16, I16 = jnp.float32, jnp.bfloat16, jnp.int16
TOP = 32767.0


def tables(edge):
    half = edge // 2
    index = np.arange(edge, dtype=np.float64) + 1.0
    sine = np.sqrt(2.0 / (edge + 1)) * np.sin(np.pi * np.outer(index, index) / (edge + 1))
    eigen = 2.0 - 2.0 * np.cos(np.pi * index / (edge + 1))
    perm = np.zeros((2, 256, 256))
    for b8 in range(8):
        for c in range(edge):
            rc, cc = (0, c) if c < half else (1, edge - 1 - c)
            perm[0, b8 * edge + c, rc * 128 + b8 * half + cc] = 1.0
            perm[1, b8 * edge + c, rc * 128 + (7 - b8) * half + cc] = 1.0
    perms = np.concatenate([perm, perm.transpose(0, 2, 1)])
    planes, scales = [], []
    for pb in range(2):
        for pc in range(2):
            planes.append(np.kron(sine[pb::2, :half].T, sine[pc::2, :half].T))
            scales.append(
                1.0
                / (
                    eigen[:, None, None]
                    + eigen[None, pb::2, None]
                    + eigen[None, None, pc::2]
                ).reshape(edge, half * half)
            )
    planes = np.stack(planes)
    both = np.stack([planes, planes.transpose(0, 2, 1)]).astype(np.float32)
    high = both.astype(jnp.bfloat16)
    low = (both - high.astype(np.float32)).astype(jnp.bfloat16)
    weights = np.stack([high, low], axis=2)
    small = np.kron(np.eye(4), sine).astype(np.float32)
    small_high = small.astype(jnp.bfloat16)
    small_low = (small - small_high.astype(np.float32)).astype(jnp.bfloat16)
    rows = np.block([[small_high, small_high], [small_low, small_low]])
    pair = np.zeros((256, 256), jnp.bfloat16)
    pair[:128, :128] = np.block([[t[:64, :64]] * 2 for t in (small_high, small_low)])
    return (
        perms.astype(jnp.bfloat16),
        np.concatenate([weights.reshape(16, 256, 256), rows[None], pair[None]]),
        np.stack(scales).astype(np.float32),
    )


def dot(a, b):
    return jnp.dot(a, b, preferred_element_type=F32)


def split(x):
    high = x.astype(BF16)
    return high, (x - high.astype(F32)).astype(BF16)


def permuted(x, perm_ref):
    halves = []
    for rb in range(2):
        parts = [[None, None], [None, None]]
        for n in range(2):
            m = n if rb == 0 else 3 - n
            y = dot(x[:, m * 256 : (m + 1) * 256], perm_ref[rb])
            parts[0][n], parts[1][n] = y[:, :128], y[:, 128:]
        halves.append(jnp.concatenate(parts[0] + parts[1], axis=1))
    return halves


def restored(halves, perm_ref):
    rows = halves[0].shape[0]
    groups = [None] * 4
    for rb in range(2):
        for n in range(2):
            m = n if rb == 0 else 3 - n
            x = jnp.concatenate(
                [
                    halves[rb][:, n * 128 : (n + 1) * 128],
                    halves[rb][:, 256 + n * 128 : 256 + (n + 1) * 128],
                ],
                axis=1,
            )
            y = dot(jnp.concatenate(split(x), axis=0), perm_ref[2 + rb])
            groups[m] = y[:rows] + y[rows:]
    return jnp.concatenate(groups, axis=1)


def plane(g, weight_ref, way):
    out = []
    for p in range(4):
        high, low = split(g[p])
        rows = high.shape[0]
        a = dot(jnp.concatenate([high, low], axis=0), weight_ref[way * 8 + p * 2])
        out.append(a[:rows] + a[rows:] + dot(high, weight_ref[way * 8 + p * 2 + 1]))
    return out


def along_rows(g, rows):
    out = []
    for p in range(4):
        both = dot(rows, jnp.concatenate(split(g[p]), axis=0))
        half = both.shape[0] // 2
        out.append(both[:half] + both[half:])
    return out


def peak(tiles):
    tiles = [jnp.abs(t) for t in tiles]
    while len(tiles) > 1:
        tiles = [
            jnp.maximum(tiles[i], tiles[i + 1]) if i + 1 < len(tiles) else tiles[i]
            for i in range(0, len(tiles), 2)
        ]
    return jnp.maximum(tiles[0], 1e-30)


def lane_tiles(x):
    return [x[:, j * 128 : (j + 1) * 128] for j in range(x.shape[1] // 128)]


def coded(x, wide):
    return jnp.round(x * wide).astype(jnp.int32)


def spread(tile, times):
    return jnp.concatenate([tile] * times, axis=1)


def kernel(
    res_hbm,
    trav_hbm,
    pair_hbm,
    perm_hbm,
    weight_hbm,
    scale_hbm,
    res_out,
    trav_out,
    res_in,
    trav_in,
    pair_ref,
    perm_ref,
    weight_ref,
    scale_ref,
    load_sem,
    tbuf,
    ubuf,
    table,
    res_acc,
    res_got,
    terms,
    ycode,
    yscale,
    ysent,
    yget,
    ygets,
    hcode,
    hscale,
    hget,
    hgets,
    total,
    z_send,
    z_recv,
    f_send,
    f_recv,
    w_send,
    w_recv,
    u_send,
    u_recv,
    p_send,
    p_recv,
    r_send,
    r_recv,
    y_send,
    ys_send,
    y_recv,
    ys_recv,
    h_send,
    hs_send,
    h_recv,
    hs_recv,
):
    n_blk = lax.axis_size("blk")
    blk, grp = lax.axis_index("blk"), lax.axis_index("grp")
    core = lax.rem(blk, 2)
    first = blk - core
    y, lo = grp // 2, lax.rem(grp, 2)
    partner = (first + 1 - core, grp)
    across_z = y * 2 + 1 - lo

    def around(b):
        return lax.rem(b + n_blk, n_blk)

    def y_peer(d):
        return lax.rem(y + d, 4)

    def remote(src, dst, send, recv, to):
        return pltpu.make_async_remote_copy(
            src_ref=src, dst_ref=dst, send_sem=send, recv_sem=recv, device_id=to, device_id_type=MESH
        )

    def came(ref, sem):
        remote(ref, ref, sem, sem, partner).wait_recv()

    def left(ref, sem):
        remote(ref, ref, sem, sem, partner).wait_send()

    loads = [
        pltpu.make_async_copy(src, dst, load_sem.at[j])
        for j, (src, dst) in enumerate(
            (
                (trav_hbm, trav_in),
                (perm_hbm, perm_ref),
                (res_hbm, res_in),
                (pair_hbm, pair_ref),
                (scale_hbm, scale_ref),
                (weight_hbm, weight_ref),
            )
        )
    ]
    for load in loads:
        load.start()

    barrier = pltpu.get_barrier_semaphore()

    def arrive(to):
        pl.semaphore_signal(barrier, inc=1, device_id=to, device_id_type=MESH)

    arrive((around(blk - 4), across_z))
    arrive((around(blk - 2), grp))
    for d in range(1, 4):
        arrive((blk, y_peer(d) * 2 + lo))
    arrive((blk, across_z))
    arrive(partner)

    @pl.when(core == 1)
    def _():
        for d in range(1, 4):
            arrive((first, y_peer(d) * 2 + lo))

    loads[0].wait()
    loads[1].wait()
    own = [h.reshape(2, 4, 8, 512) for h in permuted(trav_in[...].reshape(64, 1024), perm_ref)]
    for q in range(4):
        for t in range(2):
            tbuf[16 + q, t] = jnp.concatenate([own[0][t, q], own[1][t, q]], axis=0).astype(BF16)

    pl.semaphore_wait(barrier, 7 + 3 * (1 - core))

    def onward(near):
        to = (around(blk + 2), grp) if near else (around(blk + 4), across_z)
        return remote(tbuf.at[16 + y], tbuf.at[4 * (2 * near + core) + y], z_send, z_recv.at[near], to)

    onward(0).start()
    whole = remote(tbuf.at[pl.ds(16, 4)], tbuf.at[pl.ds(20, 4)], w_send, w_recv, partner)

    @pl.when(core == 0)
    def _():
        whole.start()

    loads[2].wait()
    for rb, h in enumerate(permuted(res_in[...].reshape(64, 1024), perm_ref)):
        for r in range(2):
            ubuf[0, r, rb] = h[r * 32 : (r + 1) * 32].reshape(4, 8, 512)
    loads[3].wait()
    for s in range(4):
        for e in range(3):
            for p in range(2):
                table[0, s, 2 * e + p] = jnp.full((8, 128), pair_ref[0, e, p, s].astype(F32))
    shares = [
        remote(ubuf.at[0], ubuf.at[1], u_send, u_recv, partner),
        remote(table.at[0], table.at[1], p_send, p_recv, partner),
    ]
    for share in shares:
        share.start()
    res_acc[...] = jnp.zeros_like(res_acc)
    for load in loads[4:]:
        load.wait()
    onward(1).start()

    def forward(near, d):
        at = 4 * (2 * near + core) + y
        return remote(tbuf.at[at], tbuf.at[at], f_send, f_recv.at[near], (blk, y_peer(d) * 2 + lo))

    def y_copies(e, d):
        to = (first + 1, y_peer(d) * 2 + lo)
        return (
            remote(ycode.at[4 * e + y_peer(d)], yget.at[e, d], y_send, y_recv.at[e], to),
            remote(yscale.at[pl.ds(e, 1)], ygets.at[e, pl.ds(d, 1)], ys_send, ys_recv.at[e], to),
        )

    def h_copies(e):
        at = (5 - e) // 2 * 2 + lo
        copies = []
        for z in range(2):
            to = (around(first - 4 + e), y * 2 + z)
            copies += [
                remote(hcode.at[e, z], hget.at[at], h_send, h_recv, to),
                remote(hscale.at[pl.ds(e, 1)], hgets.at[pl.ds(at, 1)], hs_send, hs_recv, to),
            ]
        return copies

    def solve(places):
        u, w, factors = [], [], []
        for owner, (entry, place) in enumerate(places):
            s = (core if owner == 0 else 1 - core) + 3 - entry
            both = []
            for t in range(2):
                wide = tbuf[pl.ds(place, 4), t].astype(F32).reshape(4, 2, 8, 512)
                both.append([wide[:, rb] for rb in range(2)])
            for p in range(2):
                r, t, active = (spread(table[owner, s, 2 * e + p], 4)[None] for e in range(3))
                u.append([jnp.where(r > 0.5, ubuf[owner, 1, rb], ubuf[owner, 0, rb]) for rb in range(2)])
                w.append([jnp.where(t > 0.5, both[1][rb], both[0][rb]) for rb in range(2)])
                factors.append([[active - active * e, active * e] for e in (r, t)])
        fields = 2 * len(places)
        d = [
            jnp.concatenate([(u[f][rb] * w[f][rb]).reshape(32, 512) for f in range(fields)], axis=0)
            for rb in range(2)
        ]
        g = []
        for e in (d[0] + d[1], d[0] - d[1]):
            g += [e[:, :256] + e[:, 256:], e[:, :256] - e[:, 256:]]
        rows = weight_ref[16] if fields == 4 else weight_ref[17, :128, :128]
        g = along_rows(plane(g, weight_ref, 0), rows)
        g = [
            (m.reshape(fields, 32, 256) * scale_ref[p][None]).reshape(fields * 32, 256)
            for p, m in enumerate(g)
        ]
        g = plane(along_rows(g, rows), weight_ref, 1)
        pot = []
        for e, o in (
            (g[0] + g[2], g[1] + g[3]),
            (g[0] - g[2], g[1] - g[3]),
        ):
            pot.append(jnp.concatenate([e + o, e - o], axis=1))
        for rb in range(2):
            v = [pot[rb][f * 32 : (f + 1) * 32].reshape(4, 8, 512) for f in range(fields)]
            theirs = [[], []]
            for f in range(0, fields, 2):
                vw, vw1 = v[f] * w[f][rb], v[f + 1] * w[f + 1][rb]
                vu, vu1 = v[f] * u[f][rb], v[f + 1] * u[f + 1][rb]
                for j in range(2):
                    res_acc[f // 2, j, rb] += vw * factors[f][0][j] + vw1 * factors[f + 1][0][j]
                    theirs[j].append(vu * factors[f][1][j] + vu1 * factors[f + 1][1][j])
            for j in range(2):
                terms[:, j, rb] = sum(theirs[j][1:], theirs[j][0])

    def one_row(tiles):
        top = jnp.max(peak(tiles), axis=0, keepdims=True)
        return top, jnp.broadcast_to(TOP / top, (8, 128))

    def over_y(e, value):
        parts = [(q, t, rb) for q in range(4) for t in range(2) for rb in range(2)]
        top, wide = one_row([x for at in parts for x in lane_tiles(value[at])])
        yscale[pl.ds(e, 1)] = top * (1.0 / TOP)
        wide = spread(wide, 4)
        for q in range(4):
            for t in range(2):
                ycode[4 * e + q, t] = jnp.concatenate([coded(value[q, t, rb], wide) for rb in range(2)], axis=0).astype(I16)
        for d in (2, 1, 3):
            for copy in y_copies(e, d):
                copy.start()

        @pl.when(core == 0)
        def _():
            for copy in y_copies(e, 0):
                copy.start()

        @pl.when(core == 1)
        def _():
            yget[e, 0] = ycode[4 * e + y]
            ygets[e, pl.ds(0, 1)] = yscale[pl.ds(e, 1)]

    def widened(code_ref, scale_row):
        code = code_ref[...].astype(jnp.int32).astype(F32)
        scale = spread(jnp.broadcast_to(scale_row, (8, 128)), 4)
        return [code[rb * 8 : (rb + 1) * 8] * scale for rb in range(2)]

    def homeward(e):
        from_0 = jnp.logical_or(e == 0, e == 2)

        @pl.when(from_0)
        def _():
            came(yget.at[e], y_recv.at[e])
            came(ygets.at[e, pl.ds(0, 4)], ys_recv.at[e])

        @pl.when(jnp.logical_not(from_0))
        def _():
            came(yget.at[e, pl.ds(1, 3)], y_recv.at[e])
            came(ygets.at[e, pl.ds(1, 3)], ys_recv.at[e])

        sums = [[0.0, 0.0], [0.0, 0.0]]
        for d in range(4):
            for t in range(2):
                for rb, part in enumerate(widened(yget.at[e, d, t], ygets[e, pl.ds(d, 1)])):
                    sums[t][rb] += part
        upper = lax.broadcasted_iota(jnp.int32, (8, 512), 0) < 4
        rows = [
            [jnp.where(upper, sums[0][rb], pltpu.roll(sums[1][rb], 4, 0)) for rb in range(2)],
            [jnp.where(upper, pltpu.roll(sums[0][rb], 4, 0), sums[1][rb]) for rb in range(2)],
        ]
        top, wide = one_row([x for z in range(2) for rb in range(2) for x in lane_tiles(rows[z][rb])])
        hscale[pl.ds(e, 1)] = top * (1.0 / TOP)
        wide = spread(wide, 4)
        for z in range(2):
            hcode[e, z] = jnp.concatenate([coded(rows[z][rb], wide) for rb in range(2)], axis=0).astype(I16)
        for copy in h_copies(e):
            copy.start()

    def step(i, carry):
        @pl.when(jnp.logical_and(i == 0, core == 1))
        def _():
            whole.wait_recv()

        @pl.when(i == 1)
        def _():
            for near in range(2):
                came(tbuf.at[4 * (2 * near + core) + y], z_recv.at[near])
                for d in (2, 1, 3):
                    forward(near, d).start()
            for share in shares:
                share.wait_recv()

        @pl.when(i > 0)
        def _():
            came(tbuf.at[pl.ds(0, 3)], f_recv.at[i - 1])

        alone = i + core == 1

        @pl.when(alone)
        def _():
            solve(((4 * core, 20 * core),))

        slot = 2 * (i - 1) + core

        @pl.when(i + core >= 2)
        def _():
            solve(((slot, 4 * slot), (slot, 4 * slot)))

        @pl.when(i + core >= 1)
        def _():
            one = (1 - (i + core) // 2) * (i + core)
            over_y(one * 4 * core + (1 - one) * slot, terms[...])

        return carry

    lax.fori_loop(0, 3, step, 0)

    back = remote(res_acc.at[1], res_got, r_send, r_recv, partner)
    back.start()

    def send_home(j, carry):
        homeward(lax.rem(4 + 2 * j, 5))
        return carry

    @pl.when(core == 1)
    def _():
        lax.fori_loop(0, 5, send_home, 0)

    back.wait_recv()
    for r in range(2):
        res_out[r] = restored([(res_acc[0, r, rb] + res_got[r, rb]).reshape(32, 512) for rb in range(2)], perm_ref)

    def take(at):
        for rb, part in enumerate(widened(hget.at[at], hgets[pl.ds(at, 1)])):
            total[rb] += part

    total[...] = jnp.zeros_like(total)

    @pl.when(core == 1)
    def _():
        came(hget.at[pl.ds(2, 4)], h_recv)
        came(hgets.at[pl.ds(2, 4)], hs_recv)

    @pl.when(core == 0)
    def _():
        came(hget, h_recv)
        came(hgets.at[pl.ds(0, 6)], hs_recv)
        for at in range(2):
            take(at)

    for at in range(2, 6):
        take(at)

    trav_out[...] = restored([total[rb] for rb in range(2)], perm_ref).reshape(2, 4, 1024)

    left(tbuf.at[pl.ds(0, 2)], z_send)
    left(tbuf.at[pl.ds(0, 6)], f_send)
    for share in shares:
        share.wait_send()
    back.wait_send()

    @pl.when(core == 0)
    def _():
        whole.wait_send()
        left(ycode.at[pl.ds(0, 8)], y_send)
        left(ysent.at[pl.ds(0, 8)], ys_send)

    @pl.when(core == 1)
    def _():
        left(ycode.at[pl.ds(0, 9)], y_send)
        left(ysent.at[pl.ds(0, 9)], ys_send)
        left(hcode, h_send)
        left(ysent.at[pl.ds(0, 10)], hs_send)


def store(res_ref, trav_ref, res_out, trav_out, sem):
    copies = [
        pltpu.make_async_copy(res_ref, res_out, sem.at[0]),
        pltpu.make_async_copy(trav_ref, trav_out, sem.at[1]),
    ]
    for copy in copies:
        copy.start()
    for copy in copies:
        copy.wait()


def local(residents, travellers, pair_list):
    consts = tables(32)
    hbm = pl.BlockSpec(memory_space=pltpu.HBM)
    vmem = pl.BlockSpec(memory_space=pltpu.VMEM)
    dma = pltpu.SemaphoreType.DMA
    done = pl.pallas_call(
        kernel,
        out_shape=(pltpu.VMEM((2, 32, 1024), F32), pltpu.VMEM((2, 4, 1024), F32)),
        in_specs=[hbm] * 6,
        out_specs=(vmem, vmem),
        scratch_shapes=[
            pltpu.VMEM((2, 32, 1024), BF16),
            pltpu.VMEM((2, 32, 1024), BF16),
            pltpu.SMEM((1, 3, 2, 4), jnp.int32),
            pltpu.VMEM((4, 256, 256), BF16),
            pltpu.VMEM((18, 256, 256), BF16),
            pltpu.VMEM((4, 32, 256), F32),
            dma((6,)),
            pltpu.VMEM((24, 2, 16, 512), BF16),
            pltpu.VMEM((2, 2, 2, 4, 8, 512), F32),
            pltpu.VMEM((2, 4, 6, 8, 128), F32),
            pltpu.VMEM((2, 2, 2, 4, 8, 512), F32),
            pltpu.VMEM((2, 2, 4, 8, 512), F32),
            pltpu.VMEM((4, 2, 2, 8, 512), F32),
            pltpu.VMEM((20, 2, 16, 512), I16),
            pltpu.VMEM((8, 128), F32),
            pltpu.VMEM((16, 128), F32),
            pltpu.VMEM((5, 4, 2, 16, 512), I16),
            pltpu.VMEM((5, 8, 128), F32),
            pltpu.VMEM((5, 2, 16, 512), I16),
            pltpu.VMEM((8, 128), F32),
            pltpu.VMEM((6, 16, 512), I16),
            pltpu.VMEM((8, 128), F32),
            pltpu.VMEM((2, 8, 512), F32),
            dma,
            dma((2,)),
            dma,
            dma((2,)),
            dma,
            dma,
            dma,
            dma,
            dma,
            dma,
            dma,
            dma,
            dma,
            dma,
            dma((5,)),
            dma((5,)),
            dma,
            dma,
            dma,
            dma,
        ],
        compiler_params=pltpu.CompilerParams(
            collective_id=0, has_side_effects=True
        ),
    )(residents, travellers, pair_list.transpose(0, 3, 2, 1), *[jnp.asarray(c) for c in consts])
    return pl.pallas_call(
        store,
        out_shape=(
            jax.ShapeDtypeStruct((2, 32, 1024), F32),
            jax.ShapeDtypeStruct((2, 4, 1024), F32),
        ),
        in_specs=[vmem] * 2,
        out_specs=(hbm, hbm),
        scratch_shapes=[dma((2,))],
        compiler_params=pltpu.CompilerParams(vmem_limit_bytes=2**20),
    )(*done)


def solution(mesh):
    return jax.shard_map(
        local,
        mesh=mesh,
        in_specs=(
            P(("blk", "grp"), None, None),
            P("blk", None, None),
            P(("blk", "grp"), None, None, None),
        ),
        out_specs=(P(("blk", "grp"), None, None), P("blk", "grp", None)),
        check_vma=False,
    )
```

```python
import functools

import jax
import jax.numpy as jnp
import numpy as np
from jax import lax
from jax.experimental import pallas as pl
from jax.experimental.pallas import tpu as pltpu
from jax.sharding import PartitionSpec as P

MESH = pl.DeviceIdType.MESH
F32, BF16, I16 = jnp.float32, jnp.bfloat16, jnp.int16
TOP = 32767.0


def tables(edge):
    half = edge // 2
    index = np.arange(edge, dtype=np.float64) + 1.0
    sine = np.sqrt(2.0 / (edge + 1)) * np.sin(np.pi * np.outer(index, index) / (edge + 1))
    eigen = 2.0 - 2.0 * np.cos(np.pi * index / (edge + 1))
    perm = np.zeros((2, 256, 256))
    for b8 in range(8):
        for c in range(edge):
            rc, cc = (0, c) if c < half else (1, edge - 1 - c)
            perm[0, b8 * edge + c, rc * 128 + b8 * half + cc] = 1.0
            perm[1, b8 * edge + c, rc * 128 + (7 - b8) * half + cc] = 1.0
    perms = np.concatenate([perm, perm.transpose(0, 2, 1)])
    planes, scales = [], []
    for pb in range(2):
        for pc in range(2):
            planes.append(np.kron(sine[pb::2, :half].T, sine[pc::2, :half].T))
            scales.append(
                1.0
                / (
                    eigen[:, None, None]
                    + eigen[None, pb::2, None]
                    + eigen[None, None, pc::2]
                ).reshape(edge, half * half)
            )
    planes = np.stack(planes)
    both = np.stack([planes, planes.transpose(0, 2, 1)]).astype(np.float32)
    high = both.astype(jnp.bfloat16)
    low = (both - high.astype(np.float32)).astype(jnp.bfloat16)
    weights = np.stack([high, low], axis=2)
    small = np.kron(np.eye(4), sine).astype(np.float32)
    small_high = small.astype(jnp.bfloat16)
    small_low = (small - small_high.astype(np.float32)).astype(jnp.bfloat16)
    rows = np.block([[small_high, small_high], [small_low, small_low]])
    pair = np.zeros((256, 256), jnp.bfloat16)
    pair[:128, :128] = np.block([[t[:64, :64]] * 2 for t in (small_high, small_low)])
    return (
        perms.astype(jnp.bfloat16),
        np.concatenate([weights.reshape(16, 256, 256), rows[None], pair[None]]),
        np.stack(scales).astype(np.float32),
    )


def dot(a, b):
    return jnp.dot(a, b, preferred_element_type=F32)


def split(x):
    high = x.astype(BF16)
    return high, (x - high.astype(F32)).astype(BF16)


def permuted(x, perm_ref):
    halves = []
    for rb in range(2):
        parts = [[None, None], [None, None]]
        for n in range(2):
            m = n if rb == 0 else 3 - n
            y = dot(x[:, m * 256 : (m + 1) * 256], perm_ref[rb])
            parts[0][n], parts[1][n] = y[:, :128], y[:, 128:]
        halves.append(jnp.concatenate(parts[0] + parts[1], axis=1))
    return halves


def restored(halves, perm_ref):
    rows = halves[0].shape[0]
    groups = [None] * 4
    for rb in range(2):
        for n in range(2):
            m = n if rb == 0 else 3 - n
            x = jnp.concatenate(
                [
                    halves[rb][:, n * 128 : (n + 1) * 128],
                    halves[rb][:, 256 + n * 128 : 256 + (n + 1) * 128],
                ],
                axis=1,
            )
            y = dot(jnp.concatenate(split(x), axis=0), perm_ref[2 + rb])
            groups[m] = y[:rows] + y[rows:]
    return jnp.concatenate(groups, axis=1)


def plane(g, weight_ref, way):
    out = []
    for p in range(4):
        high, low = split(g[p])
        rows = high.shape[0]
        a = dot(jnp.concatenate([high, low], axis=0), weight_ref[way * 8 + p * 2])
        out.append(a[:rows] + a[rows:] + dot(high, weight_ref[way * 8 + p * 2 + 1]))
    return out


def along_rows(g, rows):
    out = []
    for p in range(4):
        both = dot(rows, jnp.concatenate(split(g[p]), axis=0))
        half = both.shape[0] // 2
        out.append(both[:half] + both[half:])
    return out


def peak(tiles):
    tiles = [jnp.abs(t) for t in tiles]
    while len(tiles) > 1:
        tiles = [
            jnp.maximum(tiles[i], tiles[i + 1]) if i + 1 < len(tiles) else tiles[i]
            for i in range(0, len(tiles), 2)
        ]
    return jnp.maximum(tiles[0], 1e-30)


def lane_tiles(x):
    return [x[:, j * 128 : (j + 1) * 128] for j in range(x.shape[1] // 128)]


def coded(x, wide):
    return jnp.round(x * wide).astype(jnp.int32)


def spread(tile, times):
    return jnp.concatenate([tile] * times, axis=1)


def kernel(
    res_hbm,
    trav_hbm,
    pair_hbm,
    perm_hbm,
    weight_hbm,
    scale_hbm,
    res_out,
    trav_out,
    res_in,
    trav_in,
    pair_ref,
    perm_ref,
    weight_ref,
    scale_ref,
    load_sem,
    tbuf,
    ubuf,
    table,
    res_acc,
    res_got,
    terms,
    ycode,
    yscale,
    ysent,
    yget,
    ygets,
    hcode,
    hscale,
    hget,
    hgets,
    total,
    z_send,
    z_recv,
    f_send,
    f_recv,
    u_send,
    u_recv,
    p_send,
    p_recv,
    r_send,
    r_recv,
    y_send,
    ys_send,
    y_recv,
    ys_recv,
    h_send,
    hs_send,
    h_recv,
    hs_recv,
):
    n_blk = lax.axis_size("blk")
    blk, grp = lax.axis_index("blk"), lax.axis_index("grp")
    core = lax.rem(blk, 2)
    first = blk - core
    y, lo = grp // 2, lax.rem(grp, 2)
    partner = (first + 1 - core, grp)
    across_z = y * 2 + 1 - lo

    def around(b):
        return lax.rem(b + n_blk, n_blk)

    def y_peer(d):
        return lax.rem(y + d, 4)

    def remote(src, dst, send, recv, to):
        return pltpu.make_async_remote_copy(
            src_ref=src, dst_ref=dst, send_sem=send, recv_sem=recv, device_id=to, device_id_type=MESH
        )

    def came(ref, sem):
        remote(ref, ref, sem, sem, partner).wait_recv()

    def left(ref, sem):
        remote(ref, ref, sem, sem, partner).wait_send()

    loads = [
        pltpu.make_async_copy(src, dst, load_sem.at[j])
        for j, (src, dst) in enumerate(
            (
                (trav_hbm, trav_in),
                (perm_hbm, perm_ref),
                (res_hbm, res_in),
                (pair_hbm, pair_ref),
                (scale_hbm, scale_ref),
                (weight_hbm, weight_ref),
            )
        )
    ]
    for load in loads:
        load.start()

    barrier = pltpu.get_barrier_semaphore()

    def arrive(to):
        pl.semaphore_signal(barrier, inc=1, device_id=to, device_id_type=MESH)

    arrive((around(blk - 2), grp))
    for d in range(1, 4):
        arrive((blk, y_peer(d) * 2 + lo))
    arrive((blk, across_z))
    arrive(partner)

    @pl.when(core == 1)
    def _():
        for c in range(2):
            arrive((around(first - 4 + c), across_z))
        for d in range(1, 4):
            arrive((first, y_peer(d) * 2 + lo))

    loads[0].wait()
    loads[1].wait()
    own = [h.reshape(2, 4, 8, 512) for h in permuted(trav_in[...].reshape(64, 1024), perm_ref)]
    for q in range(4):
        for t in range(2):
            tbuf[16 + q, t] = jnp.concatenate([own[0][t, q], own[1][t, q]], axis=0).astype(BF16)

    pl.semaphore_wait(barrier, 7 + 3 * (1 - core))

    def onward(near):
        to = (around(blk + 2), grp) if near else (around(first + 5), across_z)
        slot = 2 * near + core
        return remote(tbuf.at[16 + y], tbuf.at[4 * slot + y], z_send, z_recv.at[slot], to)

    onward(0).start()

    loads[2].wait()
    for rb, h in enumerate(permuted(res_in[...].reshape(64, 1024), perm_ref)):
        for r in range(2):
            ubuf[0, r, rb] = h[r * 32 : (r + 1) * 32].reshape(4, 8, 512)
    loads[3].wait()
    for s in range(4):
        for e in range(3):
            for p in range(2):
                table[0, s, 2 * e + p] = jnp.full((8, 128), pair_ref[0, e, p, s].astype(F32))
    shares = [
        remote(ubuf.at[0], ubuf.at[1], u_send, u_recv, partner),
        remote(table.at[0], table.at[1], p_send, p_recv, partner),
    ]
    for share in shares:
        share.start()
    res_acc[...] = jnp.zeros_like(res_acc)
    for load in loads[4:]:
        load.wait()
    onward(1).start()

    def relay(slot):
        at = 4 * slot + y
        came(tbuf.at[at], z_recv.at[slot])
        for d in (2, 1, 3):
            remote(tbuf.at[at], tbuf.at[at], f_send, f_recv.at[slot], (blk, y_peer(d) * 2 + lo)).start()

    def y_copies(e, d):
        to = (first + 1, y_peer(d) * 2 + lo)
        return (
            remote(ycode.at[4 * e + y_peer(d)], yget.at[e, d], y_send, y_recv.at[e], to),
            remote(yscale.at[pl.ds(e, 1)], ygets.at[e, pl.ds(d, 1)], ys_send, ys_recv.at[e], to),
        )

    def h_copies(e):
        at = (5 - e) // 2 * 2 + lo
        copies = []
        for z in range(2):
            to = (around(first - 4 + e), y * 2 + z)
            copies += [
                remote(hcode.at[e, z], hget.at[at], h_send, h_recv, to),
                remote(hscale.at[pl.ds(e, 1)], hgets.at[pl.ds(at, 1)], hs_send, hs_recv, to),
            ]
        return copies

    def solve(places):
        u, w, factors = [], [], []
        for owner, entry, place in places:
            s = (core if owner == 0 else 1 - core) + 3 - entry
            both = []
            for t in range(2):
                wide = tbuf[pl.ds(place, 4), t].astype(F32).reshape(4, 2, 8, 512)
                both.append([wide[:, rb] for rb in range(2)])
            for p in range(2):
                r, t, active = (spread(table[owner, s, 2 * e + p], 4)[None] for e in range(3))
                u.append([jnp.where(r > 0.5, ubuf[owner, 1, rb], ubuf[owner, 0, rb]) for rb in range(2)])
                w.append([jnp.where(t > 0.5, both[1][rb], both[0][rb]) for rb in range(2)])
                factors.append([[active - active * e, active * e] for e in (r, t)])
        fields = 2 * len(places)
        d = [
            jnp.concatenate([(u[f][rb] * w[f][rb]).reshape(32, 512) for f in range(fields)], axis=0)
            for rb in range(2)
        ]
        g = []
        for e in (d[0] + d[1], d[0] - d[1]):
            g += [e[:, :256] + e[:, 256:], e[:, :256] - e[:, 256:]]
        rows = weight_ref[16] if fields == 4 else weight_ref[17, :128, :128]
        g = along_rows(plane(g, weight_ref, 0), rows)
        g = [
            (m.reshape(fields, 32, 256) * scale_ref[p][None]).reshape(fields * 32, 256)
            for p, m in enumerate(g)
        ]
        g = plane(along_rows(g, rows), weight_ref, 1)
        pot = []
        for e, o in (
            (g[0] + g[2], g[1] + g[3]),
            (g[0] - g[2], g[1] - g[3]),
        ):
            pot.append(jnp.concatenate([e + o, e - o], axis=1))
        for rb in range(2):
            v = [pot[rb][f * 32 : (f + 1) * 32].reshape(4, 8, 512) for f in range(fields)]
            theirs = [[], []]
            for f in range(0, fields, 2):
                vw, vw1 = v[f] * w[f][rb], v[f + 1] * w[f + 1][rb]
                vu, vu1 = v[f] * u[f][rb], v[f + 1] * u[f + 1][rb]
                for j in range(2):
                    res_acc[places[f // 2][0], j, rb] += vw * factors[f][0][j] + vw1 * factors[f + 1][0][j]
                    theirs[j].append(vu * factors[f][1][j] + vu1 * factors[f + 1][1][j])
            for j in range(2):
                terms[:, j, rb] = sum(theirs[j][1:], theirs[j][0])

    def one_row(tiles):
        top = jnp.max(peak(tiles), axis=0, keepdims=True)
        return top, jnp.broadcast_to(TOP / top, (8, 128))

    def over_y(e, value):
        parts = [(q, t, rb) for q in range(4) for t in range(2) for rb in range(2)]
        top, wide = one_row([x for at in parts for x in lane_tiles(value[at])])
        yscale[pl.ds(e, 1)] = top * (1.0 / TOP)
        wide = spread(wide, 4)
        for q in range(4):
            for t in range(2):
                ycode[4 * e + q, t] = jnp.concatenate([coded(value[q, t, rb], wide) for rb in range(2)], axis=0).astype(I16)
        for d in (2, 1, 3):
            for copy in y_copies(e, d):
                copy.start()

        @pl.when(core == 0)
        def _():
            for copy in y_copies(e, 0):
                copy.start()

        @pl.when(core == 1)
        def _():
            yget[e, 0] = ycode[4 * e + y]
            ygets[e, pl.ds(0, 1)] = yscale[pl.ds(e, 1)]

    def widened(code_ref, scale_row):
        code = code_ref[...].astype(jnp.int32).astype(F32)
        scale = spread(jnp.broadcast_to(scale_row, (8, 128)), 4)
        return [code[rb * 8 : (rb + 1) * 8] * scale for rb in range(2)]

    def homeward(e):
        from_0 = jnp.logical_or(e == 4, e == 2)

        @pl.when(from_0)
        def _():
            came(yget.at[e], y_recv.at[e])
            came(ygets.at[e, pl.ds(0, 4)], ys_recv.at[e])

        @pl.when(jnp.logical_not(from_0))
        def _():
            came(yget.at[e, pl.ds(1, 3)], y_recv.at[e])
            came(ygets.at[e, pl.ds(1, 3)], ys_recv.at[e])

        sums = [[0.0, 0.0], [0.0, 0.0]]
        for d in range(4):
            for t in range(2):
                for rb, part in enumerate(widened(yget.at[e, d, t], ygets[e, pl.ds(d, 1)])):
                    sums[t][rb] += part
        upper = lax.broadcasted_iota(jnp.int32, (8, 512), 0) < 4
        rows = [
            [jnp.where(upper, sums[0][rb], pltpu.roll(sums[1][rb], 4, 0)) for rb in range(2)],
            [jnp.where(upper, pltpu.roll(sums[0][rb], 4, 0), sums[1][rb]) for rb in range(2)],
        ]
        top, wide = one_row([x for z in range(2) for rb in range(2) for x in lane_tiles(rows[z][rb])])
        hscale[pl.ds(e, 1)] = top * (1.0 / TOP)
        wide = spread(wide, 4)
        for z in range(2):
            hcode[e, z] = jnp.concatenate([coded(rows[z][rb], wide) for rb in range(2)], axis=0).astype(I16)
        for copy in h_copies(e):
            copy.start()

    def step(i, carry):
        @pl.when(jnp.logical_and(i == 0, core == 1))
        def _():
            for slot in (1, 3, 0):
                relay(slot)

        @pl.when(jnp.logical_and(i == 1, core == 0))
        def _():
            relay(2)

        @pl.when(i == 0)
        def _():
            for share in shares:
                share.wait_recv()

        entry = 2 * i + core
        alone = i == 2 * core
        one = 1 - ((i - 2 * core) * (i - 2 * core) + 3) // 4
        single = 4 * (1 - core)

        @pl.when(jnp.logical_and(alone, core == 1))
        def _():
            came(tbuf.at[pl.ds(0, 3)], f_recv.at[0])

        @pl.when(alone)
        def _():
            solve(((1, single, 4 * single),))

        full = jnp.logical_or(i == 1, jnp.logical_and(i == 0, core == 1))

        @pl.when(full)
        def _():
            came(tbuf.at[pl.ds(0, 3)], f_recv.at[entry])
            solve(((0, entry, 4 * entry), (1, entry, 4 * entry)))

        @pl.when(jnp.logical_or(full, alone))
        def _():
            over_y(one * single + (1 - one) * entry, terms[...])

        return carry

    lax.fori_loop(0, 3, step, 0)

    back = remote(res_acc.at[1], res_got, r_send, r_recv, partner)
    back.start()

    def send_home(j, carry):
        homeward(lax.rem(4 + 2 * j, 5))
        return carry

    @pl.when(core == 1)
    def _():
        lax.fori_loop(0, 5, send_home, 0)

    back.wait_recv()
    for r in range(2):
        res_out[r] = restored([(res_acc[0, r, rb] + res_got[r, rb]).reshape(32, 512) for rb in range(2)], perm_ref)

    def take(at):
        for rb, part in enumerate(widened(hget.at[at], hgets[pl.ds(at, 1)])):
            total[rb] += part

    total[...] = jnp.zeros_like(total)

    @pl.when(core == 1)
    def _():
        came(hget.at[pl.ds(2, 4)], h_recv)
        came(hgets.at[pl.ds(2, 4)], hs_recv)

    @pl.when(core == 0)
    def _():
        came(hget, h_recv)
        came(hgets.at[pl.ds(0, 6)], hs_recv)
        for at in range(2):
            take(at)

    for at in range(2, 6):
        take(at)

    trav_out[...] = restored([total[rb] for rb in range(2)], perm_ref).reshape(2, 4, 1024)

    left(tbuf.at[pl.ds(0, 2)], z_send)
    for share in shares:
        share.wait_send()
    back.wait_send()

    @pl.when(core == 0)
    def _():
        left(tbuf.at[pl.ds(0, 3)], f_send)
        left(ycode.at[pl.ds(0, 8)], y_send)
        left(ysent.at[pl.ds(0, 8)], ys_send)

    @pl.when(core == 1)
    def _():
        left(tbuf.at[pl.ds(0, 9)], f_send)
        left(ycode.at[pl.ds(0, 9)], y_send)
        left(ysent.at[pl.ds(0, 9)], ys_send)
        left(hcode, h_send)
        left(ysent.at[pl.ds(0, 10)], hs_send)


def store(res_ref, trav_ref, res_out, trav_out, sem):
    copies = [
        pltpu.make_async_copy(res_ref, res_out, sem.at[0]),
        pltpu.make_async_copy(trav_ref, trav_out, sem.at[1]),
    ]
    for copy in copies:
        copy.start()
    for copy in copies:
        copy.wait()


def local(residents, travellers, pair_list):
    consts = tables(32)
    hbm = pl.BlockSpec(memory_space=pltpu.HBM)
    vmem = pl.BlockSpec(memory_space=pltpu.VMEM)
    dma = pltpu.SemaphoreType.DMA
    done = pl.pallas_call(
        kernel,
        out_shape=(pltpu.VMEM((2, 32, 1024), F32), pltpu.VMEM((2, 4, 1024), F32)),
        in_specs=[hbm] * 6,
        out_specs=(vmem, vmem),
        scratch_shapes=[
            pltpu.VMEM((2, 32, 1024), BF16),
            pltpu.VMEM((2, 32, 1024), BF16),
            pltpu.SMEM((1, 3, 2, 4), jnp.int32),
            pltpu.VMEM((4, 256, 256), BF16),
            pltpu.VMEM((18, 256, 256), BF16),
            pltpu.VMEM((4, 32, 256), F32),
            dma((6,)),
            pltpu.VMEM((20, 2, 16, 512), BF16),
            pltpu.VMEM((2, 2, 2, 4, 8, 512), F32),
            pltpu.VMEM((2, 4, 6, 8, 128), F32),
            pltpu.VMEM((2, 2, 2, 4, 8, 512), F32),
            pltpu.VMEM((2, 2, 4, 8, 512), F32),
            pltpu.VMEM((4, 2, 2, 8, 512), F32),
            pltpu.VMEM((20, 2, 16, 512), I16),
            pltpu.VMEM((8, 128), F32),
            pltpu.VMEM((16, 128), F32),
            pltpu.VMEM((5, 4, 2, 16, 512), I16),
            pltpu.VMEM((5, 8, 128), F32),
            pltpu.VMEM((5, 2, 16, 512), I16),
            pltpu.VMEM((8, 128), F32),
            pltpu.VMEM((6, 16, 512), I16),
            pltpu.VMEM((8, 128), F32),
            pltpu.VMEM((2, 8, 512), F32),
            dma,
            dma((4,)),
            dma,
            dma((4,)),
            dma,
            dma,
            dma,
            dma,
            dma,
            dma,
            dma,
            dma,
            dma((5,)),
            dma((5,)),
            dma,
            dma,
            dma,
            dma,
        ],
        compiler_params=pltpu.CompilerParams(
            collective_id=0, has_side_effects=True
        ),
    )(residents, travellers, pair_list.transpose(0, 3, 2, 1), *[jnp.asarray(c) for c in consts])
    return pl.pallas_call(
        store,
        out_shape=(
            jax.ShapeDtypeStruct((2, 32, 1024), F32),
            jax.ShapeDtypeStruct((2, 4, 1024), F32),
        ),
        in_specs=[vmem] * 2,
        out_specs=(hbm, hbm),
        scratch_shapes=[dma((2,))],
        compiler_params=pltpu.CompilerParams(vmem_limit_bytes=2**20),
    )(*done)


def solution(mesh):
    return jax.shard_map(
        local,
        mesh=mesh,
        in_specs=(
            P(("blk", "grp"), None, None),
            P("blk", None, None),
            P(("blk", "grp"), None, None, None),
        ),
        out_specs=(P(("blk", "grp"), None, None), P("blk", "grp", None)),
        check_vma=False,
    )
```

```python
import functools

import jax
import jax.numpy as jnp
import numpy as np
from jax import lax
from jax.experimental import pallas as pl
from jax.experimental.pallas import tpu as pltpu
from jax.sharding import PartitionSpec as P

MESH = pl.DeviceIdType.MESH
F32, BF16, I16 = jnp.float32, jnp.bfloat16, jnp.int16
TOP = 32767.0


def tables(edge):
    half = edge // 2
    index = np.arange(edge, dtype=np.float64) + 1.0
    sine = np.sqrt(2.0 / (edge + 1)) * np.sin(np.pi * np.outer(index, index) / (edge + 1))
    eigen = 2.0 - 2.0 * np.cos(np.pi * index / (edge + 1))
    perm = np.zeros((2, 256, 256))
    for b8 in range(8):
        for c in range(edge):
            rc, cc = (0, c) if c < half else (1, edge - 1 - c)
            perm[0, b8 * edge + c, rc * 128 + b8 * half + cc] = 1.0
            perm[1, b8 * edge + c, rc * 128 + (7 - b8) * half + cc] = 1.0
    perms = np.concatenate([perm, perm.transpose(0, 2, 1)])
    planes, scales = [], []
    for pb in range(2):
        for pc in range(2):
            planes.append(np.kron(sine[pb::2, :half].T, sine[pc::2, :half].T))
            scales.append(
                1.0
                / (
                    eigen[:, None, None]
                    + eigen[None, pb::2, None]
                    + eigen[None, None, pc::2]
                ).reshape(edge, half * half)
            )
    planes = np.stack(planes)
    both = np.stack([planes, planes.transpose(0, 2, 1)]).astype(np.float32)
    high = both.astype(jnp.bfloat16)
    low = (both - high.astype(np.float32)).astype(jnp.bfloat16)
    weights = np.stack([high, low], axis=2)
    small = np.kron(np.eye(4), sine).astype(np.float32)
    small_high = small.astype(jnp.bfloat16)
    small_low = (small - small_high.astype(np.float32)).astype(jnp.bfloat16)
    rows = np.block([[small_high, small_high], [small_low, small_low]])
    pair = np.zeros((256, 256), jnp.bfloat16)
    pair[:128, :128] = np.block([[t[:64, :64]] * 2 for t in (small_high, small_low)])
    return (
        perms.astype(jnp.bfloat16),
        np.concatenate([weights.reshape(16, 256, 256), rows[None], pair[None]]),
        np.stack(scales).astype(np.float32),
    )


def dot(a, b):
    return jnp.dot(a, b, preferred_element_type=F32)


def split(x):
    high = x.astype(BF16)
    return high, (x - high.astype(F32)).astype(BF16)


def permuted(x, perm_ref):
    halves = []
    for rb in range(2):
        parts = [[None, None], [None, None]]
        for n in range(2):
            m = n if rb == 0 else 3 - n
            y = dot(x[:, m * 256 : (m + 1) * 256], perm_ref[rb])
            parts[0][n], parts[1][n] = y[:, :128], y[:, 128:]
        halves.append(jnp.concatenate(parts[0] + parts[1], axis=1))
    return halves


def restored(halves, perm_ref):
    rows = halves[0].shape[0]
    groups = [None] * 4
    for rb in range(2):
        for n in range(2):
            m = n if rb == 0 else 3 - n
            x = jnp.concatenate(
                [
                    halves[rb][:, n * 128 : (n + 1) * 128],
                    halves[rb][:, 256 + n * 128 : 256 + (n + 1) * 128],
                ],
                axis=1,
            )
            y = dot(jnp.concatenate(split(x), axis=0), perm_ref[2 + rb])
            groups[m] = y[:rows] + y[rows:]
    return jnp.concatenate(groups, axis=1)


def plane(g, weight_ref, way):
    out = []
    for p in range(4):
        high, low = split(g[p])
        rows = high.shape[0]
        a = dot(jnp.concatenate([high, low], axis=0), weight_ref[way * 8 + p * 2])
        out.append(a[:rows] + a[rows:] + dot(high, weight_ref[way * 8 + p * 2 + 1]))
    return out


def along_rows(g, rows):
    out = []
    for p in range(4):
        both = dot(rows, jnp.concatenate(split(g[p]), axis=0))
        half = both.shape[0] // 2
        out.append(both[:half] + both[half:])
    return out


def peak(tiles):
    tiles = [jnp.abs(t) for t in tiles]
    while len(tiles) > 1:
        tiles = [
            jnp.maximum(tiles[i], tiles[i + 1]) if i + 1 < len(tiles) else tiles[i]
            for i in range(0, len(tiles), 2)
        ]
    return jnp.maximum(tiles[0], 1e-30)


def lane_tiles(x):
    return [x[:, j * 128 : (j + 1) * 128] for j in range(x.shape[1] // 128)]


def coded(x, wide):
    return jnp.round(x * wide).astype(jnp.int32)


def spread(tile, times):
    return jnp.concatenate([tile] * times, axis=1)


def kernel(
    res_hbm,
    trav_hbm,
    pair_hbm,
    perm_hbm,
    weight_hbm,
    scale_hbm,
    res_out,
    trav_out,
    res_in,
    trav_in,
    pair_ref,
    perm_ref,
    weight_ref,
    scale_ref,
    load_sem,
    tbuf,
    ubuf,
    table,
    res_acc,
    res_got,
    terms,
    ycode,
    yscale,
    ysent,
    yget,
    ygets,
    hcode,
    hscale,
    hget,
    hgets,
    total,
    z_send,
    z_recv,
    f_send,
    f_recv,
    u_send,
    u_recv,
    p_send,
    p_recv,
    r_send,
    r_recv,
    y_send,
    ys_send,
    y_recv,
    ys_recv,
    h_send,
    hs_send,
    h_recv,
    hs_recv,
):
    n_blk = lax.axis_size("blk")
    blk, grp = lax.axis_index("blk"), lax.axis_index("grp")
    core = lax.rem(blk, 2)
    first = blk - core
    y, lo = grp // 2, lax.rem(grp, 2)
    partner = (first + 1 - core, grp)
    across_z = y * 2 + 1 - lo

    def around(b):
        return lax.rem(b + n_blk, n_blk)

    def y_peer(d):
        return lax.rem(y + d, 4)

    def remote(src, dst, send, recv, to):
        return pltpu.make_async_remote_copy(
            src_ref=src, dst_ref=dst, send_sem=send, recv_sem=recv, device_id=to, device_id_type=MESH
        )

    def came(ref, sem):
        remote(ref, ref, sem, sem, partner).wait_recv()

    def left(ref, sem):
        remote(ref, ref, sem, sem, partner).wait_send()

    loads = [
        pltpu.make_async_copy(src, dst, load_sem.at[j])
        for j, (src, dst) in enumerate(
            (
                (trav_hbm, trav_in),
                (perm_hbm, perm_ref),
                (res_hbm, res_in),
                (pair_hbm, pair_ref),
                (scale_hbm, scale_ref),
                (weight_hbm, weight_ref),
            )
        )
    ]
    for load in loads:
        load.start()

    barrier = pltpu.get_barrier_semaphore()

    def arrive(to):
        pl.semaphore_signal(barrier, inc=1, device_id=to, device_id_type=MESH)

    arrive((around(blk - 2), grp))
    arrive((first, across_z))
    for d in range(1, 4):
        arrive((first, y_peer(d) * 2 + lo))

    @pl.when(core == 1)
    def _():
        for c in range(2):
            arrive((around(first - 4 + c), across_z))
        arrive(partner)

    loads[0].wait()
    loads[1].wait()
    own = [h.reshape(2, 4, 8, 512) for h in permuted(trav_in[...].reshape(64, 1024), perm_ref)]
    for q in range(4):
        for t in range(2):
            tbuf[16 + q, t] = jnp.concatenate([own[0][t, q], own[1][t, q]], axis=0).astype(BF16)

    pl.semaphore_wait(barrier, 2 + 9 * (1 - core))

    def onward(near):
        to = (around(blk + 2), grp) if near else (around(first + 5), across_z)
        slot = 2 * near + core
        return remote(tbuf.at[16 + y], tbuf.at[4 * slot + y], z_send, z_recv.at[slot], to)

    onward(0).start()

    loads[2].wait()
    for rb, h in enumerate(permuted(res_in[...].reshape(64, 1024), perm_ref)):
        for r in range(2):
            ubuf[0, r, rb] = h[r * 32 : (r + 1) * 32].reshape(4, 8, 512)
    loads[3].wait()
    for s in range(4):
        for e in range(3):
            for p in range(2):
                table[0, s, 2 * e + p] = jnp.full((8, 128), pair_ref[0, e, p, s].astype(F32))
    shares = [
        remote(ubuf.at[0], ubuf.at[1], u_send, u_recv, partner),
        remote(table.at[0], table.at[1], p_send, p_recv, partner),
    ]

    @pl.when(core == 0)
    def _():
        for share in shares:
            share.start()

    res_acc[...] = jnp.zeros_like(res_acc)
    for load in loads[4:]:
        load.wait()
    onward(1).start()

    def relay(slot):
        at = 4 * slot + y
        came(tbuf.at[at], z_recv.at[slot])
        for d in (2, 1, 3):
            remote(tbuf.at[at], tbuf.at[at], f_send, f_recv.at[slot], (blk, y_peer(d) * 2 + lo)).start()

    def y_copies(e, d):
        to = (first + 1, y_peer(d) * 2 + lo)
        return (
            remote(ycode.at[4 * e + y_peer(d)], yget.at[e, d], y_send, y_recv.at[e], to),
            remote(yscale.at[pl.ds(e, 1)], ygets.at[e, pl.ds(d, 1)], ys_send, ys_recv.at[e], to),
        )

    def h_copies(e):
        at = (5 - e) // 2 * 2 + lo
        copies = []
        for z in range(2):
            to = (around(first - 4 + e), y * 2 + z)
            copies += [
                remote(hcode.at[e, z], hget.at[at], h_send, h_recv, to),
                remote(hscale.at[pl.ds(e, 1)], hgets.at[pl.ds(at, 1)], hs_send, hs_recv, to),
            ]
        return copies

    def solve(places):
        u, w, factors = [], [], []
        for owner, entry, place in places:
            s = (core if owner == 0 else 1 - core) + 3 - entry
            both = []
            for t in range(2):
                wide = tbuf[pl.ds(place, 4), t].astype(F32).reshape(4, 2, 8, 512)
                both.append([wide[:, rb] for rb in range(2)])
            for p in range(2):
                r, t, active = (spread(table[owner, s, 2 * e + p], 4)[None] for e in range(3))
                u.append([jnp.where(r > 0.5, ubuf[owner, 1, rb], ubuf[owner, 0, rb]) for rb in range(2)])
                w.append([jnp.where(t > 0.5, both[1][rb], both[0][rb]) for rb in range(2)])
                factors.append([[active - active * e, active * e] for e in (r, t)])
        fields = 2 * len(places)
        d = [
            jnp.concatenate([(u[f][rb] * w[f][rb]).reshape(32, 512) for f in range(fields)], axis=0)
            for rb in range(2)
        ]
        g = []
        for e in (d[0] + d[1], d[0] - d[1]):
            g += [e[:, :256] + e[:, 256:], e[:, :256] - e[:, 256:]]
        rows = weight_ref[16] if fields == 4 else weight_ref[17, :128, :128]
        g = along_rows(plane(g, weight_ref, 0), rows)
        g = [
            (m.reshape(fields, 32, 256) * scale_ref[p][None]).reshape(fields * 32, 256)
            for p, m in enumerate(g)
        ]
        g = plane(along_rows(g, rows), weight_ref, 1)
        pot = []
        for e, o in (
            (g[0] + g[2], g[1] + g[3]),
            (g[0] - g[2], g[1] - g[3]),
        ):
            pot.append(jnp.concatenate([e + o, e - o], axis=1))
        for rb in range(2):
            v = [pot[rb][f * 32 : (f + 1) * 32].reshape(4, 8, 512) for f in range(fields)]
            theirs = [[], []]
            for f in range(0, fields, 2):
                vw, vw1 = v[f] * w[f][rb], v[f + 1] * w[f + 1][rb]
                vu, vu1 = v[f] * u[f][rb], v[f + 1] * u[f + 1][rb]
                for j in range(2):
                    res_acc[places[f // 2][0], j, rb] += vw * factors[f][0][j] + vw1 * factors[f + 1][0][j]
                    theirs[j].append(vu * factors[f][1][j] + vu1 * factors[f + 1][1][j])
            for j in range(2):
                terms[:, j, rb] = sum(theirs[j][1:], theirs[j][0])

    def one_row(tiles):
        top = jnp.max(peak(tiles), axis=0, keepdims=True)
        return top, jnp.broadcast_to(TOP / top, (8, 128))

    def over_y(e, value):
        parts = [(q, t, rb) for q in range(4) for t in range(2) for rb in range(2)]
        top, wide = one_row([x for at in parts for x in lane_tiles(value[at])])
        yscale[pl.ds(e, 1)] = top * (1.0 / TOP)
        wide = spread(wide, 4)
        for q in range(4):
            for t in range(2):
                ycode[4 * e + q, t] = jnp.concatenate([coded(value[q, t, rb], wide) for rb in range(2)], axis=0).astype(I16)
        for d in (2, 1, 3):
            for copy in y_copies(e, d):
                copy.start()

        @pl.when(core == 0)
        def _():
            for copy in y_copies(e, 0):
                copy.start()

        @pl.when(core == 1)
        def _():
            yget[e, 0] = ycode[4 * e + y]
            ygets[e, pl.ds(0, 1)] = yscale[pl.ds(e, 1)]

    def widened(code_ref, scale_row):
        code = code_ref[...].astype(jnp.int32).astype(F32)
        scale = spread(jnp.broadcast_to(scale_row, (8, 128)), 4)
        return [code[rb * 8 : (rb + 1) * 8] * scale for rb in range(2)]

    def homeward(e):
        from_0 = jnp.logical_or(e == 4, e == 2)

        @pl.when(from_0)
        def _():
            came(yget.at[e], y_recv.at[e])
            came(ygets.at[e, pl.ds(0, 4)], ys_recv.at[e])

        @pl.when(jnp.logical_not(from_0))
        def _():
            came(yget.at[e, pl.ds(1, 3)], y_recv.at[e])
            came(ygets.at[e, pl.ds(1, 3)], ys_recv.at[e])

        sums = [[0.0, 0.0], [0.0, 0.0]]
        for d in range(4):
            for t in range(2):
                for rb, part in enumerate(widened(yget.at[e, d, t], ygets[e, pl.ds(d, 1)])):
                    sums[t][rb] += part
        upper = lax.broadcasted_iota(jnp.int32, (8, 512), 0) < 4
        rows = [
            [jnp.where(upper, sums[0][rb], pltpu.roll(sums[1][rb], 4, 0)) for rb in range(2)],
            [jnp.where(upper, pltpu.roll(sums[0][rb], 4, 0), sums[1][rb]) for rb in range(2)],
        ]
        top, wide = one_row([x for z in range(2) for rb in range(2) for x in lane_tiles(rows[z][rb])])
        hscale[pl.ds(e, 1)] = top * (1.0 / TOP)
        wide = spread(wide, 4)
        for z in range(2):
            hcode[e, z] = jnp.concatenate([coded(rows[z][rb], wide) for rb in range(2)], axis=0).astype(I16)
        for copy in h_copies(e):
            copy.start()

    def step(i, carry):
        @pl.when(jnp.logical_and(i == 0, core == 1))
        def _():
            for share in shares:
                share.wait_recv()
            for share in shares:
                share.start()
            for slot in (1, 3, 0):
                relay(slot)

        @pl.when(jnp.logical_and(i == 1, core == 0))
        def _():
            relay(2)

        @pl.when(jnp.logical_and(i == 0, core == 0))
        def _():
            for share in shares:
                share.wait_recv()

        entry = 2 * i + core
        alone = i == 2 * core
        one = 1 - ((i - 2 * core) * (i - 2 * core) + 3) // 4
        single = 4 * (1 - core)

        @pl.when(jnp.logical_and(alone, core == 1))
        def _():
            came(tbuf.at[pl.ds(0, 3)], f_recv.at[0])

        @pl.when(alone)
        def _():
            solve(((1, single, 4 * single),))

        full = jnp.logical_or(i == 1, jnp.logical_and(i == 0, core == 1))

        @pl.when(full)
        def _():
            came(tbuf.at[pl.ds(0, 3)], f_recv.at[entry])
            solve(((0, entry, 4 * entry), (1, entry, 4 * entry)))

        @pl.when(jnp.logical_or(full, alone))
        def _():
            over_y(one * single + (1 - one) * entry, terms[...])

        return carry

    lax.fori_loop(0, 3, step, 0)

    back = remote(res_acc.at[1], res_got, r_send, r_recv, partner)
    back.start()

    def send_home(j, carry):
        homeward(lax.rem(4 + 2 * j, 5))
        return carry

    @pl.when(core == 1)
    def _():
        lax.fori_loop(0, 5, send_home, 0)

    back.wait_recv()
    for r in range(2):
        res_out[r] = restored([(res_acc[0, r, rb] + res_got[r, rb]).reshape(32, 512) for rb in range(2)], perm_ref)

    def take(at):
        for rb, part in enumerate(widened(hget.at[at], hgets[pl.ds(at, 1)])):
            total[rb] += part

    total[...] = jnp.zeros_like(total)

    @pl.when(core == 1)
    def _():
        came(hget.at[pl.ds(2, 4)], h_recv)
        came(hgets.at[pl.ds(2, 4)], hs_recv)

    @pl.when(core == 0)
    def _():
        came(hget, h_recv)
        came(hgets.at[pl.ds(0, 6)], hs_recv)
        for at in range(2):
            take(at)

    for at in range(2, 6):
        take(at)

    trav_out[...] = restored([total[rb] for rb in range(2)], perm_ref).reshape(2, 4, 1024)

    left(tbuf.at[pl.ds(0, 2)], z_send)
    for share in shares:
        share.wait_send()
    back.wait_send()

    @pl.when(core == 0)
    def _():
        left(tbuf.at[pl.ds(0, 3)], f_send)
        left(ycode.at[pl.ds(0, 8)], y_send)
        left(ysent.at[pl.ds(0, 8)], ys_send)

    @pl.when(core == 1)
    def _():
        left(tbuf.at[pl.ds(0, 9)], f_send)
        left(ycode.at[pl.ds(0, 9)], y_send)
        left(ysent.at[pl.ds(0, 9)], ys_send)
        left(hcode, h_send)
        left(ysent.at[pl.ds(0, 10)], hs_send)


def store(res_ref, trav_ref, res_out, trav_out, sem):
    copies = [
        pltpu.make_async_copy(res_ref, res_out, sem.at[0]),
        pltpu.make_async_copy(trav_ref, trav_out, sem.at[1]),
    ]
    for copy in copies:
        copy.start()
    for copy in copies:
        copy.wait()


def local(residents, travellers, pair_list):
    consts = tables(32)
    hbm = pl.BlockSpec(memory_space=pltpu.HBM)
    vmem = pl.BlockSpec(memory_space=pltpu.VMEM)
    dma = pltpu.SemaphoreType.DMA
    done = pl.pallas_call(
        kernel,
        out_shape=(pltpu.VMEM((2, 32, 1024), F32), pltpu.VMEM((2, 4, 1024), F32)),
        in_specs=[hbm] * 6,
        out_specs=(vmem, vmem),
        scratch_shapes=[
            pltpu.VMEM((2, 32, 1024), BF16),
            pltpu.VMEM((2, 32, 1024), BF16),
            pltpu.SMEM((1, 3, 2, 4), jnp.int32),
            pltpu.VMEM((4, 256, 256), BF16),
            pltpu.VMEM((18, 256, 256), BF16),
            pltpu.VMEM((4, 32, 256), F32),
            dma((6,)),
            pltpu.VMEM((20, 2, 16, 512), BF16),
            pltpu.VMEM((2, 2, 2, 4, 8, 512), F32),
            pltpu.VMEM((2, 4, 6, 8, 128), F32),
            pltpu.VMEM((2, 2, 2, 4, 8, 512), F32),
            pltpu.VMEM((2, 2, 4, 8, 512), F32),
            pltpu.VMEM((4, 2, 2, 8, 512), F32),
            pltpu.VMEM((20, 2, 16, 512), I16),
            pltpu.VMEM((8, 128), F32),
            pltpu.VMEM((16, 128), F32),
            pltpu.VMEM((5, 4, 2, 16, 512), I16),
            pltpu.VMEM((5, 8, 128), F32),
            pltpu.VMEM((5, 2, 16, 512), I16),
            pltpu.VMEM((8, 128), F32),
            pltpu.VMEM((6, 16, 512), I16),
            pltpu.VMEM((8, 128), F32),
            pltpu.VMEM((2, 8, 512), F32),
            dma,
            dma((4,)),
            dma,
            dma((4,)),
            dma,
            dma,
            dma,
            dma,
            dma,
            dma,
            dma,
            dma,
            dma((5,)),
            dma((5,)),
            dma,
            dma,
            dma,
            dma,
        ],
        compiler_params=pltpu.CompilerParams(
            collective_id=0, has_side_effects=True
        ),
    )(residents, travellers, pair_list.transpose(0, 3, 2, 1), *[jnp.asarray(c) for c in consts])
    return pl.pallas_call(
        store,
        out_shape=(
            jax.ShapeDtypeStruct((2, 32, 1024), F32),
            jax.ShapeDtypeStruct((2, 4, 1024), F32),
        ),
        in_specs=[vmem] * 2,
        out_specs=(hbm, hbm),
        scratch_shapes=[dma((2,))],
        compiler_params=pltpu.CompilerParams(vmem_limit_bytes=2**20),
    )(*done)


def solution(mesh):
    return jax.shard_map(
        local,
        mesh=mesh,
        in_specs=(
            P(("blk", "grp"), None, None),
            P("blk", None, None),
            P(("blk", "grp"), None, None, None),
        ),
        out_specs=(P(("blk", "grp"), None, None), P("blk", "grp", None)),
        check_vma=False,
    )
```

```python
import functools

import jax
import jax.numpy as jnp
import numpy as np
from jax import lax
from jax.experimental import pallas as pl
from jax.experimental.pallas import tpu as pltpu
from jax.sharding import PartitionSpec as P

MESH = pl.DeviceIdType.MESH
F32, BF16, I16 = jnp.float32, jnp.bfloat16, jnp.int16
TOP = 32767.0


def tables(edge):
    half = edge // 2
    index = np.arange(edge, dtype=np.float64) + 1.0
    sine = np.sqrt(2.0 / (edge + 1)) * np.sin(np.pi * np.outer(index, index) / (edge + 1))
    eigen = 2.0 - 2.0 * np.cos(np.pi * index / (edge + 1))
    perm = np.zeros((2, 256, 256))
    for b8 in range(8):
        for c in range(edge):
            rc, cc = (0, c) if c < half else (1, edge - 1 - c)
            perm[0, b8 * edge + c, rc * 128 + b8 * half + cc] = 1.0
            perm[1, b8 * edge + c, rc * 128 + (7 - b8) * half + cc] = 1.0
    perms = np.concatenate([perm, perm.transpose(0, 2, 1)])
    planes, scales = [], []
    for pb in range(2):
        for pc in range(2):
            planes.append(np.kron(sine[pb::2, :half].T, sine[pc::2, :half].T))
            scales.append(
                1.0
                / (
                    eigen[:, None, None]
                    + eigen[None, pb::2, None]
                    + eigen[None, None, pc::2]
                ).reshape(edge, half * half)
            )
    planes = np.stack(planes)
    both = np.stack([planes, planes.transpose(0, 2, 1)]).astype(np.float32)
    high = both.astype(jnp.bfloat16)
    low = (both - high.astype(np.float32)).astype(jnp.bfloat16)
    weights = np.stack([high, low], axis=2)
    small = np.kron(np.eye(4), sine).astype(np.float32)
    small_high = small.astype(jnp.bfloat16)
    small_low = (small - small_high.astype(np.float32)).astype(jnp.bfloat16)
    rows = np.block([[small_high, small_high], [small_low, small_low]])
    pair = np.zeros((256, 256), jnp.bfloat16)
    pair[:128, :128] = np.block([[t[:64, :64]] * 2 for t in (small_high, small_low)])
    return (
        perms.astype(jnp.bfloat16),
        np.concatenate([weights.reshape(16, 256, 256), rows[None], pair[None]]),
        np.stack(scales).astype(np.float32),
    )


def dot(a, b):
    return jnp.dot(a, b, preferred_element_type=F32)


def split(x):
    high = x.astype(BF16)
    return high, (x - high.astype(F32)).astype(BF16)


def permuted(x, perm_ref):
    halves = []
    for rb in range(2):
        parts = [[None, None], [None, None]]
        for n in range(2):
            m = n if rb == 0 else 3 - n
            y = dot(x[:, m * 256 : (m + 1) * 256], perm_ref[rb])
            parts[0][n], parts[1][n] = y[:, :128], y[:, 128:]
        halves.append(jnp.concatenate(parts[0] + parts[1], axis=1))
    return halves


def restored(halves, perm_ref):
    rows = halves[0].shape[0]
    groups = [None] * 4
    for rb in range(2):
        for n in range(2):
            m = n if rb == 0 else 3 - n
            x = jnp.concatenate(
                [
                    halves[rb][:, n * 128 : (n + 1) * 128],
                    halves[rb][:, 256 + n * 128 : 256 + (n + 1) * 128],
                ],
                axis=1,
            )
            y = dot(jnp.concatenate(split(x), axis=0), perm_ref[2 + rb])
            groups[m] = y[:rows] + y[rows:]
    return jnp.concatenate(groups, axis=1)


def plane(g, weight_ref, way):
    out = []
    for p in range(4):
        high, low = split(g[p])
        rows = high.shape[0]
        a = dot(jnp.concatenate([high, low], axis=0), weight_ref[way * 8 + p * 2])
        out.append(a[:rows] + a[rows:] + dot(high, weight_ref[way * 8 + p * 2 + 1]))
    return out


def along_rows(g, rows):
    out = []
    for p in range(4):
        both = dot(rows, jnp.concatenate(split(g[p]), axis=0))
        half = both.shape[0] // 2
        out.append(both[:half] + both[half:])
    return out


def peak(tiles):
    tiles = [jnp.abs(t) for t in tiles]
    while len(tiles) > 1:
        tiles = [
            jnp.maximum(tiles[i], tiles[i + 1]) if i + 1 < len(tiles) else tiles[i]
            for i in range(0, len(tiles), 2)
        ]
    return jnp.maximum(tiles[0], 1e-30)


def lane_tiles(x):
    return [x[:, j * 128 : (j + 1) * 128] for j in range(x.shape[1] // 128)]


def coded(x, wide):
    return jnp.round(x * wide).astype(jnp.int32)


def spread(tile, times):
    return jnp.concatenate([tile] * times, axis=1)


def kernel(
    res_hbm,
    trav_hbm,
    pair_hbm,
    perm_hbm,
    weight_hbm,
    scale_hbm,
    res_out,
    trav_out,
    res_in,
    trav_in,
    pair_ref,
    perm_ref,
    weight_ref,
    scale_ref,
    load_sem,
    tbuf,
    ubuf,
    table,
    res_acc,
    res_got,
    ycode,
    yscale,
    ysent,
    yget,
    ygets,
    hcode,
    hscale,
    hget,
    hgets,
    total,
    z_send,
    z_recv,
    f_send,
    f_recv,
    u_send,
    u_recv,
    p_send,
    p_recv,
    r_send,
    r_recv,
    y_send,
    ys_send,
    y_recv,
    ys_recv,
    h_send,
    hs_send,
    h_recv,
    hs_recv,
):
    n_blk = lax.axis_size("blk")
    blk, grp = lax.axis_index("blk"), lax.axis_index("grp")
    core = lax.rem(blk, 2)
    first = blk - core
    y, lo = grp // 2, lax.rem(grp, 2)
    partner = (first + 1 - core, grp)
    across_z = y * 2 + 1 - lo

    def around(b):
        return lax.rem(b + n_blk, n_blk)

    def y_peer(d):
        return lax.rem(y + d, 4)

    def remote(src, dst, send, recv, to):
        return pltpu.make_async_remote_copy(
            src_ref=src, dst_ref=dst, send_sem=send, recv_sem=recv, device_id=to, device_id_type=MESH
        )

    def came(ref, sem):
        remote(ref, ref, sem, sem, partner).wait_recv()

    def left(ref, sem):
        remote(ref, ref, sem, sem, partner).wait_send()

    loads = [
        pltpu.make_async_copy(src, dst, load_sem.at[j])
        for j, (src, dst) in enumerate(
            (
                (trav_hbm, trav_in),
                (perm_hbm, perm_ref),
                (res_hbm, res_in),
                (pair_hbm, pair_ref),
                (scale_hbm, scale_ref),
                (weight_hbm, weight_ref),
            )
        )
    ]
    for load in loads:
        load.start()

    barrier = pltpu.get_barrier_semaphore()

    def arrive(to):
        pl.semaphore_signal(barrier, inc=1, device_id=to, device_id_type=MESH)

    arrive((around(blk - 2), grp))
    for d in range(1, 4):
        arrive((blk, y_peer(d) * 2 + lo))
    arrive((blk, across_z))
    arrive(partner)

    @pl.when(core == 1)
    def _():
        for c in range(2):
            arrive((around(first - 4 + c), across_z))
        for d in range(1, 4):
            arrive((first, y_peer(d) * 2 + lo))

    loads[0].wait()
    loads[1].wait()
    own = [h.reshape(2, 4, 8, 512) for h in permuted(trav_in[...].reshape(64, 1024), perm_ref)]
    for q in range(4):
        for t in range(2):
            tbuf[16 + q, t] = jnp.concatenate([own[0][t, q], own[1][t, q]], axis=0).astype(BF16)

    pl.semaphore_wait(barrier, 7 + 3 * (1 - core))

    def onward(near):
        to = (around(blk + 2), grp) if near else (around(first + 5), across_z)
        slot = 2 * near + core
        return remote(tbuf.at[16 + y], tbuf.at[4 * slot + y], z_send, z_recv.at[slot], to)

    onward(0).start()

    loads[2].wait()
    for rb, h in enumerate(permuted(res_in[...].reshape(64, 1024), perm_ref)):
        for r in range(2):
            ubuf[0, r, rb] = h[r * 32 : (r + 1) * 32].reshape(4, 8, 512)
    loads[3].wait()
    for s in range(4):
        for e in range(3):
            for p in range(2):
                table[0, s, 2 * e + p] = jnp.full((8, 128), pair_ref[0, e, p, s].astype(F32))
    shares = [
        remote(ubuf.at[0], ubuf.at[1], u_send, u_recv, partner),
        remote(table.at[0], table.at[1], p_send, p_recv, partner),
    ]
    for share in shares:
        share.start()
    res_acc[...] = jnp.zeros_like(res_acc)
    for load in loads[4:]:
        load.wait()
    onward(1).start()

    def relay(slot):
        at = 4 * slot + y
        came(tbuf.at[at], z_recv.at[slot])
        for d in (2, 1, 3):
            remote(tbuf.at[at], tbuf.at[at], f_send, f_recv.at[slot], (blk, y_peer(d) * 2 + lo)).start()

    def y_copies(e, d):
        to = (first + 1, y_peer(d) * 2 + lo)
        return (
            remote(ycode.at[4 * e + y_peer(d)], yget.at[e, d], y_send, y_recv.at[e], to),
            remote(yscale.at[pl.ds(e, 1)], ygets.at[e, pl.ds(d, 1)], ys_send, ys_recv.at[e], to),
        )

    def h_copies(e):
        at = (5 - e) // 2 * 2 + lo
        copies = []
        for z in range(2):
            to = (around(first - 4 + e), y * 2 + z)
            copies += [
                remote(hcode.at[e, z], hget.at[at], h_send, h_recv, to),
                remote(hscale.at[pl.ds(e, 1)], hgets.at[pl.ds(at, 1)], hs_send, hs_recv, to),
            ]
        return copies

    def solve(places):
        u, w, factors = [], [], []
        for owner, entry, place in places:
            s = (core if owner == 0 else 1 - core) + 3 - entry
            both = []
            for t in range(2):
                wide = tbuf[pl.ds(place, 4), t].astype(F32).reshape(4, 2, 8, 512)
                both.append([wide[:, rb] for rb in range(2)])
            for p in range(2):
                r, t, active = (spread(table[owner, s, 2 * e + p], 4)[None] for e in range(3))
                u.append([jnp.where(r > 0.5, ubuf[owner, 1, rb], ubuf[owner, 0, rb]) for rb in range(2)])
                w.append([jnp.where(t > 0.5, both[1][rb], both[0][rb]) for rb in range(2)])
                factors.append([[active - active * e, active * e] for e in (r, t)])
        fields = 2 * len(places)
        d = [
            jnp.concatenate([(u[f][rb] * w[f][rb]).reshape(32, 512) for f in range(fields)], axis=0)
            for rb in range(2)
        ]
        g = []
        for e in (d[0] + d[1], d[0] - d[1]):
            g += [e[:, :256] + e[:, 256:], e[:, :256] - e[:, 256:]]
        rows = weight_ref[16] if fields == 4 else weight_ref[17, :128, :128]
        g = along_rows(plane(g, weight_ref, 0), rows)
        g = [
            (m.reshape(fields, 32, 256) * scale_ref[p][None]).reshape(fields * 32, 256)
            for p, m in enumerate(g)
        ]
        g = plane(along_rows(g, rows), weight_ref, 1)
        pot = []
        for e, o in (
            (g[0] + g[2], g[1] + g[3]),
            (g[0] - g[2], g[1] - g[3]),
        ):
            pot.append(jnp.concatenate([e + o, e - o], axis=1))
        terms = [[], []]
        for rb in range(2):
            v = [pot[rb][f * 32 : (f + 1) * 32].reshape(4, 8, 512) for f in range(fields)]
            theirs = [[], []]
            for f in range(0, fields, 2):
                vw, vw1 = v[f] * w[f][rb], v[f + 1] * w[f + 1][rb]
                vu, vu1 = v[f] * u[f][rb], v[f + 1] * u[f + 1][rb]
                for j in range(2):
                    res_acc[places[f // 2][0], j, rb] += vw * factors[f][0][j] + vw1 * factors[f + 1][0][j]
                    theirs[j].append(vu * factors[f][1][j] + vu1 * factors[f + 1][1][j])
            for j in range(2):
                terms[j].append(sum(theirs[j][1:], theirs[j][0]))
        return terms

    def one_row(tiles):
        top = jnp.max(peak(tiles), axis=0, keepdims=True)
        return top, jnp.broadcast_to(TOP / top, (8, 128))

    def over_y(e, value):
        parts = [(q, t, rb) for q in range(4) for t in range(2) for rb in range(2)]
        top, wide = one_row([x for at in parts for x in lane_tiles(value[at[1]][at[2]][at[0]])])
        yscale[pl.ds(e, 1)] = top * (1.0 / TOP)
        wide = spread(wide, 4)
        for q in range(4):
            for t in range(2):
                ycode[4 * e + q, t] = jnp.concatenate([coded(value[t][rb][q], wide) for rb in range(2)], axis=0).astype(I16)
        for d in (2, 1, 3):
            for copy in y_copies(e, d):
                copy.start()

        @pl.when(core == 0)
        def _():
            for copy in y_copies(e, 0):
                copy.start()

        @pl.when(core == 1)
        def _():
            yget[e, 0] = ycode[4 * e + y]
            ygets[e, pl.ds(0, 1)] = yscale[pl.ds(e, 1)]

    def widened(code_ref, scale_row):
        code = code_ref[...].astype(jnp.int32).astype(F32)
        scale = spread(jnp.broadcast_to(scale_row, (8, 128)), 4)
        return [code[rb * 8 : (rb + 1) * 8] * scale for rb in range(2)]

    def homeward(e):
        from_0 = jnp.logical_or(e == 4, e == 2)

        @pl.when(from_0)
        def _():
            came(yget.at[e], y_recv.at[e])
            came(ygets.at[e, pl.ds(0, 4)], ys_recv.at[e])

        @pl.when(jnp.logical_not(from_0))
        def _():
            came(yget.at[e, pl.ds(1, 3)], y_recv.at[e])
            came(ygets.at[e, pl.ds(1, 3)], ys_recv.at[e])

        sums = [[0.0, 0.0], [0.0, 0.0]]
        for d in range(4):
            for t in range(2):
                for rb, part in enumerate(widened(yget.at[e, d, t], ygets[e, pl.ds(d, 1)])):
                    sums[t][rb] += part
        upper = lax.broadcasted_iota(jnp.int32, (8, 512), 0) < 4
        rows = [
            [jnp.where(upper, sums[0][rb], pltpu.roll(sums[1][rb], 4, 0)) for rb in range(2)],
            [jnp.where(upper, pltpu.roll(sums[0][rb], 4, 0), sums[1][rb]) for rb in range(2)],
        ]
        top, wide = one_row([x for z in range(2) for rb in range(2) for x in lane_tiles(rows[z][rb])])
        hscale[pl.ds(e, 1)] = top * (1.0 / TOP)
        wide = spread(wide, 4)
        for z in range(2):
            hcode[e, z] = jnp.concatenate([coded(rows[z][rb], wide) for rb in range(2)], axis=0).astype(I16)
        for copy in h_copies(e):
            copy.start()

    def step(i, carry):
        @pl.when(jnp.logical_and(i == 0, core == 1))
        def _():
            for slot in (1, 3, 0):
                relay(slot)

        @pl.when(jnp.logical_and(i == 1, core == 0))
        def _():
            relay(2)

        @pl.when(i == 0)
        def _():
            for share in shares:
                share.wait_recv()

        entry = 2 * i + core
        alone = i == 2 * core
        single = 4 * (1 - core)

        @pl.when(jnp.logical_and(alone, core == 1))
        def _():
            came(tbuf.at[pl.ds(0, 3)], f_recv.at[0])

        @pl.when(alone)
        def _():
            over_y(single, solve(((1, single, 4 * single),)))

        full = jnp.logical_or(i == 1, jnp.logical_and(i == 0, core == 1))

        @pl.when(full)
        def _():
            came(tbuf.at[pl.ds(0, 3)], f_recv.at[entry])
            over_y(entry, solve(((0, entry, 4 * entry), (1, entry, 4 * entry))))

        return carry

    lax.fori_loop(0, 3, step, 0)

    back = remote(res_acc.at[1], res_got, r_send, r_recv, partner)
    back.start()

    def send_home(j, carry):
        homeward(lax.rem(4 + 2 * j, 5))
        return carry

    @pl.when(core == 1)
    def _():
        lax.fori_loop(0, 5, send_home, 0)

    back.wait_recv()
    for r in range(2):
        res_out[r] = restored([(res_acc[0, r, rb] + res_got[r, rb]).reshape(32, 512) for rb in range(2)], perm_ref)

    def take(at):
        for rb, part in enumerate(widened(hget.at[at], hgets[pl.ds(at, 1)])):
            total[rb] += part

    total[...] = jnp.zeros_like(total)

    @pl.when(core == 1)
    def _():
        came(hget.at[pl.ds(2, 4)], h_recv)
        came(hgets.at[pl.ds(2, 4)], hs_recv)

    @pl.when(core == 0)
    def _():
        came(hget, h_recv)
        came(hgets.at[pl.ds(0, 6)], hs_recv)
        for at in range(2):
            take(at)

    for at in range(2, 6):
        take(at)

    trav_out[...] = restored([total[rb] for rb in range(2)], perm_ref).reshape(2, 4, 1024)

    left(tbuf.at[pl.ds(0, 2)], z_send)
    for share in shares:
        share.wait_send()
    back.wait_send()

    @pl.when(core == 0)
    def _():
        left(tbuf.at[pl.ds(0, 3)], f_send)
        left(ycode.at[pl.ds(0, 8)], y_send)
        left(ysent.at[pl.ds(0, 8)], ys_send)

    @pl.when(core == 1)
    def _():
        left(tbuf.at[pl.ds(0, 9)], f_send)
        left(ycode.at[pl.ds(0, 9)], y_send)
        left(ysent.at[pl.ds(0, 9)], ys_send)
        left(hcode, h_send)
        left(ysent.at[pl.ds(0, 10)], hs_send)


def store(res_ref, trav_ref, res_out, trav_out, sem):
    copies = [
        pltpu.make_async_copy(res_ref, res_out, sem.at[0]),
        pltpu.make_async_copy(trav_ref, trav_out, sem.at[1]),
    ]
    for copy in copies:
        copy.start()
    for copy in copies:
        copy.wait()


def local(residents, travellers, pair_list):
    consts = tables(32)
    hbm = pl.BlockSpec(memory_space=pltpu.HBM)
    vmem = pl.BlockSpec(memory_space=pltpu.VMEM)
    dma = pltpu.SemaphoreType.DMA
    done = pl.pallas_call(
        kernel,
        out_shape=(pltpu.VMEM((2, 32, 1024), F32), pltpu.VMEM((2, 4, 1024), F32)),
        in_specs=[hbm] * 6,
        out_specs=(vmem, vmem),
        scratch_shapes=[
            pltpu.VMEM((2, 32, 1024), BF16),
            pltpu.VMEM((2, 32, 1024), BF16),
            pltpu.SMEM((1, 3, 2, 4), jnp.int32),
            pltpu.VMEM((4, 256, 256), BF16),
            pltpu.VMEM((18, 256, 256), BF16),
            pltpu.VMEM((4, 32, 256), F32),
            dma((6,)),
            pltpu.VMEM((20, 2, 16, 512), BF16),
            pltpu.VMEM((2, 2, 2, 4, 8, 512), F32),
            pltpu.VMEM((2, 4, 6, 8, 128), F32),
            pltpu.VMEM((2, 2, 2, 4, 8, 512), F32),
            pltpu.VMEM((2, 2, 4, 8, 512), F32),
            pltpu.VMEM((20, 2, 16, 512), I16),
            pltpu.VMEM((8, 128), F32),
            pltpu.VMEM((16, 128), F32),
            pltpu.VMEM((5, 4, 2, 16, 512), I16),
            pltpu.VMEM((5, 8, 128), F32),
            pltpu.VMEM((5, 2, 16, 512), I16),
            pltpu.VMEM((8, 128), F32),
            pltpu.VMEM((6, 16, 512), I16),
            pltpu.VMEM((8, 128), F32),
            pltpu.VMEM((2, 8, 512), F32),
            dma,
            dma((4,)),
            dma,
            dma((4,)),
            dma,
            dma,
            dma,
            dma,
            dma,
            dma,
            dma,
            dma,
            dma((5,)),
            dma((5,)),
            dma,
            dma,
            dma,
            dma,
        ],
        compiler_params=pltpu.CompilerParams(
            collective_id=0, has_side_effects=True
        ),
    )(residents, travellers, pair_list.transpose(0, 3, 2, 1), *[jnp.asarray(c) for c in consts])
    return pl.pallas_call(
        store,
        out_shape=(
            jax.ShapeDtypeStruct((2, 32, 1024), F32),
            jax.ShapeDtypeStruct((2, 4, 1024), F32),
        ),
        in_specs=[vmem] * 2,
        out_specs=(hbm, hbm),
        scratch_shapes=[dma((2,))],
        compiler_params=pltpu.CompilerParams(vmem_limit_bytes=2**20),
    )(*done)


def solution(mesh):
    return jax.shard_map(
        local,
        mesh=mesh,
        in_specs=(
            P(("blk", "grp"), None, None),
            P("blk", None, None),
            P(("blk", "grp"), None, None, None),
        ),
        out_specs=(P(("blk", "grp"), None, None), P("blk", "grp", None)),
        check_vma=False,
    )
```

```python
import functools

import jax
import jax.numpy as jnp
import numpy as np
from jax import lax
from jax.experimental import pallas as pl
from jax.experimental.pallas import tpu as pltpu
from jax.sharding import PartitionSpec as P

MESH = pl.DeviceIdType.MESH
F32, BF16, I16 = jnp.float32, jnp.bfloat16, jnp.int16
TOP = 32767.0


def tables(edge):
    half = edge // 2
    index = np.arange(edge, dtype=np.float64) + 1.0
    sine = np.sqrt(2.0 / (edge + 1)) * np.sin(np.pi * np.outer(index, index) / (edge + 1))
    eigen = 2.0 - 2.0 * np.cos(np.pi * index / (edge + 1))
    perm = np.zeros((2, 256, 256))
    for b8 in range(8):
        for c in range(edge):
            rc, cc = (0, c) if c < half else (1, edge - 1 - c)
            perm[0, b8 * edge + c, rc * 128 + b8 * half + cc] = 1.0
            perm[1, b8 * edge + c, rc * 128 + (7 - b8) * half + cc] = 1.0
    perms = np.concatenate([perm, perm.transpose(0, 2, 1)])
    planes, scales = [], []
    for pb in range(2):
        for pc in range(2):
            planes.append(np.kron(sine[pb::2, :half].T, sine[pc::2, :half].T))
            scales.append(
                1.0
                / (
                    eigen[:, None, None]
                    + eigen[None, pb::2, None]
                    + eigen[None, None, pc::2]
                ).reshape(edge, half * half)
            )
    planes = np.stack(planes)
    both = np.stack([planes, planes.transpose(0, 2, 1)]).astype(np.float32)
    high = both.astype(jnp.bfloat16)
    low = (both - high.astype(np.float32)).astype(jnp.bfloat16)
    weights = np.stack([high, low], axis=2)
    small = np.kron(np.eye(4), sine).astype(np.float32)
    small_high = small.astype(jnp.bfloat16)
    small_low = (small - small_high.astype(np.float32)).astype(jnp.bfloat16)
    rows = np.block([[small_high, small_high], [small_low, small_low]])
    pair = np.zeros((256, 256), jnp.bfloat16)
    pair[:128, :128] = np.block([[t[:64, :64]] * 2 for t in (small_high, small_low)])
    return (
        perms.astype(jnp.bfloat16),
        np.concatenate([weights.reshape(16, 256, 256), rows[None], pair[None]]),
        np.stack(scales).astype(np.float32),
    )


def dot(a, b):
    return jnp.dot(a, b, preferred_element_type=F32)


def split(x):
    high = x.astype(BF16)
    return high, (x - high.astype(F32)).astype(BF16)


def permuted(x, perm_ref):
    halves = []
    for rb in range(2):
        parts = [[None, None], [None, None]]
        for n in range(2):
            m = n if rb == 0 else 3 - n
            y = dot(x[:, m * 256 : (m + 1) * 256], perm_ref[rb])
            parts[0][n], parts[1][n] = y[:, :128], y[:, 128:]
        halves.append(jnp.concatenate(parts[0] + parts[1], axis=1))
    return halves


def restored(halves, perm_ref):
    rows = halves[0].shape[0]
    groups = [None] * 4
    for rb in range(2):
        for n in range(2):
            m = n if rb == 0 else 3 - n
            x = jnp.concatenate(
                [
                    halves[rb][:, n * 128 : (n + 1) * 128],
                    halves[rb][:, 256 + n * 128 : 256 + (n + 1) * 128],
                ],
                axis=1,
            )
            y = dot(jnp.concatenate(split(x), axis=0), perm_ref[2 + rb])
            groups[m] = y[:rows] + y[rows:]
    return jnp.concatenate(groups, axis=1)


def plane(g, weight_ref, way):
    out = []
    for p in range(4):
        high, low = split(g[p])
        rows = high.shape[0]
        a = dot(jnp.concatenate([high, low], axis=0), weight_ref[way * 8 + p * 2])
        out.append(a[:rows] + a[rows:] + dot(high, weight_ref[way * 8 + p * 2 + 1]))
    return out


def along_rows(g, rows):
    out = []
    for p in range(4):
        both = dot(rows, jnp.concatenate(split(g[p]), axis=0))
        half = both.shape[0] // 2
        out.append(both[:half] + both[half:])
    return out


def peak(tiles):
    tiles = [jnp.abs(t) for t in tiles]
    while len(tiles) > 1:
        tiles = [
            jnp.maximum(tiles[i], tiles[i + 1]) if i + 1 < len(tiles) else tiles[i]
            for i in range(0, len(tiles), 2)
        ]
    return jnp.maximum(tiles[0], 1e-30)


def lane_tiles(x):
    return [x[:, j * 128 : (j + 1) * 128] for j in range(x.shape[1] // 128)]


def coded(x, wide):
    return jnp.round(x * wide).astype(jnp.int32)


def spread(tile, times):
    return jnp.concatenate([tile] * times, axis=1)


def kernel(
    res_hbm,
    trav_hbm,
    pair_hbm,
    perm_hbm,
    weight_hbm,
    scale_hbm,
    res_out,
    trav_out,
    res_in,
    trav_in,
    pair_ref,
    perm_ref,
    weight_ref,
    scale_ref,
    load_sem,
    tbuf,
    ubuf,
    table,
    res_acc,
    res_got,
    terms,
    ycode,
    yscale,
    ysent,
    yget,
    ygets,
    hcode,
    hscale,
    hget,
    hgets,
    total,
    z_send,
    z_recv,
    f_send,
    f_recv,
    u_send,
    u_recv,
    p_send,
    p_recv,
    r_send,
    r_recv,
    y_send,
    ys_send,
    y_recv,
    ys_recv,
    h_send,
    hs_send,
    h_recv,
    hs_recv,
):
    n_blk = lax.axis_size("blk")
    blk, grp = lax.axis_index("blk"), lax.axis_index("grp")
    core = lax.rem(blk, 2)
    first = blk - core
    y, lo = grp // 2, lax.rem(grp, 2)
    partner = (first + 1 - core, grp)
    across_z = y * 2 + 1 - lo

    def around(b):
        return lax.rem(b + n_blk, n_blk)

    def y_peer(d):
        return lax.rem(y + d, 4)

    def remote(src, dst, send, recv, to):
        return pltpu.make_async_remote_copy(
            src_ref=src, dst_ref=dst, send_sem=send, recv_sem=recv, device_id=to, device_id_type=MESH
        )

    def came(ref, sem):
        remote(ref, ref, sem, sem, partner).wait_recv()

    def left(ref, sem):
        remote(ref, ref, sem, sem, partner).wait_send()

    loads = [
        pltpu.make_async_copy(src, dst, load_sem.at[j])
        for j, (src, dst) in enumerate(
            (
                (trav_hbm, trav_in),
                (perm_hbm, perm_ref),
                (res_hbm, res_in),
                (pair_hbm, pair_ref),
                (scale_hbm, scale_ref),
                (weight_hbm, weight_ref),
            )
        )
    ]
    for load in loads:
        load.start()

    barrier = pltpu.get_barrier_semaphore()

    def arrive(to):
        pl.semaphore_signal(barrier, inc=1, device_id=to, device_id_type=MESH)

    arrive((around(blk - 2), grp))
    for d in range(1, 4):
        arrive((blk, y_peer(d) * 2 + lo))
    arrive((blk, across_z))
    arrive(partner)

    @pl.when(core == 1)
    def _():
        for c in range(2):
            arrive((around(first - 4 + c), across_z))
        for d in range(1, 4):
            arrive((first, y_peer(d) * 2 + lo))

    loads[0].wait()
    loads[1].wait()
    own = [h.reshape(2, 4, 8, 512) for h in permuted(trav_in[...].reshape(64, 1024), perm_ref)]
    for q in range(4):
        for t in range(2):
            tbuf[16 + q, t] = jnp.concatenate([own[0][t, q], own[1][t, q]], axis=0).astype(BF16)

    pl.semaphore_wait(barrier, 7 + 3 * (1 - core))

    def onward(near):
        to = (around(blk + 2), grp) if near else (around(first + 5), across_z)
        slot = 2 * near + core
        return remote(tbuf.at[16 + y], tbuf.at[4 * slot + y], z_send, z_recv.at[slot], to)

    onward(0).start()

    loads[2].wait()
    for rb, h in enumerate(permuted(res_in[...].reshape(64, 1024), perm_ref)):
        for r in range(2):
            ubuf[0, r, rb] = h[r * 32 : (r + 1) * 32].reshape(4, 8, 512)
    loads[3].wait()
    for s in range(4):
        for e in range(3):
            for p in range(2):
                table[0, s, 2 * e + p] = jnp.full((8, 128), pair_ref[0, e, p, s].astype(F32))
    shares = [
        remote(ubuf.at[0], ubuf.at[1], u_send, u_recv, partner),
        remote(table.at[0], table.at[1], p_send, p_recv, partner),
    ]
    for share in shares:
        share.start()
    res_acc[...] = jnp.zeros_like(res_acc)
    for load in loads[4:]:
        load.wait()

    @pl.when(core == 1)
    def _():
        onward(1).start()

    def relay(slot):
        at = 4 * slot + y
        came(tbuf.at[at], z_recv.at[slot])
        for d in (2, 1, 3):
            remote(tbuf.at[at], tbuf.at[at], f_send, f_recv.at[slot], (blk, y_peer(d) * 2 + lo)).start()

    def y_copies(e, d):
        to = (first + 1, y_peer(d) * 2 + lo)
        return (
            remote(ycode.at[4 * e + y_peer(d)], yget.at[e, d], y_send, y_recv.at[e], to),
            remote(yscale.at[pl.ds(e, 1)], ygets.at[e, pl.ds(d, 1)], ys_send, ys_recv.at[e], to),
        )

    def h_copies(e):
        at = (5 - e) // 2 * 2 + lo
        copies = []
        for z in range(2):
            to = (around(first - 4 + e), y * 2 + z)
            copies += [
                remote(hcode.at[e, z], hget.at[at], h_send, h_recv, to),
                remote(hscale.at[pl.ds(e, 1)], hgets.at[pl.ds(at, 1)], hs_send, hs_recv, to),
            ]
        return copies

    def solve(places):
        u, w, factors = [], [], []
        for owner, entry, place in places:
            s = (core if owner == 0 else 1 - core) + 3 - entry
            both = []
            for t in range(2):
                wide = tbuf[pl.ds(place, 4), t].astype(F32).reshape(4, 2, 8, 512)
                both.append([wide[:, rb] for rb in range(2)])
            for p in range(2):
                r, t, active = (spread(table[owner, s, 2 * e + p], 4)[None] for e in range(3))
                u.append([jnp.where(r > 0.5, ubuf[owner, 1, rb], ubuf[owner, 0, rb]) for rb in range(2)])
                w.append([jnp.where(t > 0.5, both[1][rb], both[0][rb]) for rb in range(2)])
                factors.append([[active - active * e, active * e] for e in (r, t)])
        fields = 2 * len(places)
        d = [
            jnp.concatenate([(u[f][rb] * w[f][rb]).reshape(32, 512) for f in range(fields)], axis=0)
            for rb in range(2)
        ]
        g = []
        for e in (d[0] + d[1], d[0] - d[1]):
            g += [e[:, :256] + e[:, 256:], e[:, :256] - e[:, 256:]]
        rows = weight_ref[16] if fields == 4 else weight_ref[17, :128, :128]
        g = along_rows(plane(g, weight_ref, 0), rows)
        g = [
            (m.reshape(fields, 32, 256) * scale_ref[p][None]).reshape(fields * 32, 256)
            for p, m in enumerate(g)
        ]
        g = plane(along_rows(g, rows), weight_ref, 1)
        pot = []
        for e, o in (
            (g[0] + g[2], g[1] + g[3]),
            (g[0] - g[2], g[1] - g[3]),
        ):
            pot.append(jnp.concatenate([e + o, e - o], axis=1))
        for rb in range(2):
            v = [pot[rb][f * 32 : (f + 1) * 32].reshape(4, 8, 512) for f in range(fields)]
            theirs = [[], []]
            for f in range(0, fields, 2):
                vw, vw1 = v[f] * w[f][rb], v[f + 1] * w[f + 1][rb]
                vu, vu1 = v[f] * u[f][rb], v[f + 1] * u[f + 1][rb]
                for j in range(2):
                    res_acc[places[f // 2][0], j, rb] += vw * factors[f][0][j] + vw1 * factors[f + 1][0][j]
                    theirs[j].append(vu * factors[f][1][j] + vu1 * factors[f + 1][1][j])
            for j in range(2):
                terms[:, j, rb] = sum(theirs[j][1:], theirs[j][0])

    def one_row(tiles):
        top = jnp.max(peak(tiles), axis=0, keepdims=True)
        return top, jnp.broadcast_to(TOP / top, (8, 128))

    def over_y(e, value):
        parts = [(q, t, rb) for q in range(4) for t in range(2) for rb in range(2)]
        top, wide = one_row([x for at in parts for x in lane_tiles(value[at])])
        yscale[pl.ds(e, 1)] = top * (1.0 / TOP)
        wide = spread(wide, 4)
        for q in range(4):
            for t in range(2):
                ycode[4 * e + q, t] = jnp.concatenate([coded(value[q, t, rb], wide) for rb in range(2)], axis=0).astype(I16)
        for d in (2, 1, 3):
            for copy in y_copies(e, d):
                copy.start()

        @pl.when(core == 0)
        def _():
            for copy in y_copies(e, 0):
                copy.start()

        @pl.when(core == 1)
        def _():
            yget[e, 0] = ycode[4 * e + y]
            ygets[e, pl.ds(0, 1)] = yscale[pl.ds(e, 1)]

    def widened(code_ref, scale_row):
        code = code_ref[...].astype(jnp.int32).astype(F32)
        scale = spread(jnp.broadcast_to(scale_row, (8, 128)), 4)
        return [code[rb * 8 : (rb + 1) * 8] * scale for rb in range(2)]

    def homeward(e):
        from_0 = jnp.logical_or(e == 4, e == 2)

        @pl.when(from_0)
        def _():
            came(yget.at[e], y_recv.at[e])
            came(ygets.at[e, pl.ds(0, 4)], ys_recv.at[e])

        @pl.when(jnp.logical_not(from_0))
        def _():
            came(yget.at[e, pl.ds(1, 3)], y_recv.at[e])
            came(ygets.at[e, pl.ds(1, 3)], ys_recv.at[e])

        sums = [[0.0, 0.0], [0.0, 0.0]]
        for d in range(4):
            for t in range(2):
                for rb, part in enumerate(widened(yget.at[e, d, t], ygets[e, pl.ds(d, 1)])):
                    sums[t][rb] += part
        upper = lax.broadcasted_iota(jnp.int32, (8, 512), 0) < 4
        rows = [
            [jnp.where(upper, sums[0][rb], pltpu.roll(sums[1][rb], 4, 0)) for rb in range(2)],
            [jnp.where(upper, pltpu.roll(sums[0][rb], 4, 0), sums[1][rb]) for rb in range(2)],
        ]
        top, wide = one_row([x for z in range(2) for rb in range(2) for x in lane_tiles(rows[z][rb])])
        hscale[pl.ds(e, 1)] = top * (1.0 / TOP)
        wide = spread(wide, 4)
        for z in range(2):
            hcode[e, z] = jnp.concatenate([coded(rows[z][rb], wide) for rb in range(2)], axis=0).astype(I16)
        for copy in h_copies(e):
            copy.start()

    def step(i, carry):
        @pl.when(jnp.logical_and(i == 0, core == 1))
        def _():
            for slot in (1, 3, 0):
                relay(slot)

        @pl.when(jnp.logical_and(i == 1, core == 0))
        def _():
            relay(2)

        @pl.when(i == 0)
        def _():
            for share in shares:
                share.wait_recv()

        @pl.when(jnp.logical_and(i == 0, core == 0))
        def _():
            onward(1).start()

        entry = 2 * i + core
        alone = i == 2 * core
        one = 1 - ((i - 2 * core) * (i - 2 * core) + 3) // 4
        single = 4 * (1 - core)

        @pl.when(jnp.logical_and(alone, core == 1))
        def _():
            came(tbuf.at[pl.ds(0, 3)], f_recv.at[0])

        @pl.when(alone)
        def _():
            solve(((1, single, 4 * single),))

        full = jnp.logical_or(i == 1, jnp.logical_and(i == 0, core == 1))

        @pl.when(full)
        def _():
            came(tbuf.at[pl.ds(0, 3)], f_recv.at[entry])
            solve(((0, entry, 4 * entry), (1, entry, 4 * entry)))

        @pl.when(jnp.logical_or(full, alone))
        def _():
            over_y(one * single + (1 - one) * entry, terms[...])

        return carry

    lax.fori_loop(0, 3, step, 0)

    back = remote(res_acc.at[1], res_got, r_send, r_recv, partner)
    back.start()

    def send_home(j, carry):
        homeward(lax.rem(4 + 2 * j, 5))
        return carry

    @pl.when(core == 1)
    def _():
        lax.fori_loop(0, 5, send_home, 0)

    back.wait_recv()
    for r in range(2):
        res_out[r] = restored([(res_acc[0, r, rb] + res_got[r, rb]).reshape(32, 512) for rb in range(2)], perm_ref)

    def take(at):
        for rb, part in enumerate(widened(hget.at[at], hgets[pl.ds(at, 1)])):
            total[rb] += part

    total[...] = jnp.zeros_like(total)

    @pl.when(core == 1)
    def _():
        came(hget.at[pl.ds(2, 4)], h_recv)
        came(hgets.at[pl.ds(2, 4)], hs_recv)

    @pl.when(core == 0)
    def _():
        came(hget, h_recv)
        came(hgets.at[pl.ds(0, 6)], hs_recv)
        for at in range(2):
            take(at)

    for at in range(2, 6):
        take(at)

    trav_out[...] = restored([total[rb] for rb in range(2)], perm_ref).reshape(2, 4, 1024)

    left(tbuf.at[pl.ds(0, 2)], z_send)
    for share in shares:
        share.wait_send()
    back.wait_send()

    @pl.when(core == 0)
    def _():
        left(tbuf.at[pl.ds(0, 3)], f_send)
        left(ycode.at[pl.ds(0, 8)], y_send)
        left(ysent.at[pl.ds(0, 8)], ys_send)

    @pl.when(core == 1)
    def _():
        left(tbuf.at[pl.ds(0, 9)], f_send)
        left(ycode.at[pl.ds(0, 9)], y_send)
        left(ysent.at[pl.ds(0, 9)], ys_send)
        left(hcode, h_send)
        left(ysent.at[pl.ds(0, 10)], hs_send)


def store(res_ref, trav_ref, res_out, trav_out, sem):
    copies = [
        pltpu.make_async_copy(res_ref, res_out, sem.at[0]),
        pltpu.make_async_copy(trav_ref, trav_out, sem.at[1]),
    ]
    for copy in copies:
        copy.start()
    for copy in copies:
        copy.wait()


def local(residents, travellers, pair_list):
    consts = tables(32)
    hbm = pl.BlockSpec(memory_space=pltpu.HBM)
    vmem = pl.BlockSpec(memory_space=pltpu.VMEM)
    dma = pltpu.SemaphoreType.DMA
    done = pl.pallas_call(
        kernel,
        out_shape=(pltpu.VMEM((2, 32, 1024), F32), pltpu.VMEM((2, 4, 1024), F32)),
        in_specs=[hbm] * 6,
        out_specs=(vmem, vmem),
        scratch_shapes=[
            pltpu.VMEM((2, 32, 1024), BF16),
            pltpu.VMEM((2, 32, 1024), BF16),
            pltpu.SMEM((1, 3, 2, 4), jnp.int32),
            pltpu.VMEM((4, 256, 256), BF16),
            pltpu.VMEM((18, 256, 256), BF16),
            pltpu.VMEM((4, 32, 256), F32),
            dma((6,)),
            pltpu.VMEM((20, 2, 16, 512), BF16),
            pltpu.VMEM((2, 2, 2, 4, 8, 512), F32),
            pltpu.VMEM((2, 4, 6, 8, 128), F32),
            pltpu.VMEM((2, 2, 2, 4, 8, 512), F32),
            pltpu.VMEM((2, 2, 4, 8, 512), F32),
            pltpu.VMEM((4, 2, 2, 8, 512), F32),
            pltpu.VMEM((20, 2, 16, 512), I16),
            pltpu.VMEM((8, 128), F32),
            pltpu.VMEM((16, 128), F32),
            pltpu.VMEM((5, 4, 2, 16, 512), I16),
            pltpu.VMEM((5, 8, 128), F32),
            pltpu.VMEM((5, 2, 16, 512), I16),
            pltpu.VMEM((8, 128), F32),
            pltpu.VMEM((6, 16, 512), I16),
            pltpu.VMEM((8, 128), F32),
            pltpu.VMEM((2, 8, 512), F32),
            dma,
            dma((4,)),
            dma,
            dma((4,)),
            dma,
            dma,
            dma,
            dma,
            dma,
            dma,
            dma,
            dma,
            dma((5,)),
            dma((5,)),
            dma,
            dma,
            dma,
            dma,
        ],
        compiler_params=pltpu.CompilerParams(
            collective_id=0, has_side_effects=True
        ),
    )(residents, travellers, pair_list.transpose(0, 3, 2, 1), *[jnp.asarray(c) for c in consts])
    return pl.pallas_call(
        store,
        out_shape=(
            jax.ShapeDtypeStruct((2, 32, 1024), F32),
            jax.ShapeDtypeStruct((2, 4, 1024), F32),
        ),
        in_specs=[vmem] * 2,
        out_specs=(hbm, hbm),
        scratch_shapes=[dma((2,))],
        compiler_params=pltpu.CompilerParams(vmem_limit_bytes=2**20),
    )(*done)


def solution(mesh):
    return jax.shard_map(
        local,
        mesh=mesh,
        in_specs=(
            P(("blk", "grp"), None, None),
            P("blk", None, None),
            P(("blk", "grp"), None, None, None),
        ),
        out_specs=(P(("blk", "grp"), None, None), P("blk", "grp", None)),
        check_vma=False,
    )
```
